128 devices in a mesh: dp: 1, yz: 16 (over z, y), x: 8 (over x, core).
Axes of the slice: x: 4, y: 4, z: 4, core: 2. Of those that a mesh axis runs over, the one named last changes fastest.
Arguments:
- x_in: bfloat16 [8192, 2816], P('dp', ('x', 'yz'))
- ln_gain: bfloat16 [2816], P(('x', 'yz'))
- w_qkv: bfloat16 [2816, 3072], P('x', 'yz')
- w_gate: bfloat16 [2816, 11264], P('x', 'yz')
- w_up: bfloat16 [2816, 11264], P('x', 'yz')
- w_attn_out: bfloat16 [2816, 2816], P('yz', 'x')
- w_mlp_out: bfloat16 [11264, 2816], P('yz', 'x')
- k_cache: bfloat16 [8192, 128, 128], P(('dp', 'x', 'yz'))
- v_cache: bfloat16 [8192, 128, 128], P(('dp', 'x', 'yz'))
- ctx_len: int32 [8192], P(('dp', 'x', 'yz'))
Outputs:
- output 1: bfloat16 [8192, 2816], P('dp', ('x', 'yz'))
- output 2: bfloat16 [8192, 128, 128], P(('dp', 'x', 'yz'))
- output 3: bfloat16 [8192, 128, 128], P(('dp', 'x', 'yz'))
All inputs are finite; a program needn't handle non-finite values.
Results may differ from the reference program's by a relative error of at most 0.00711414.
Values are sent between devices in bfloat16 or wider.
A program may use at most 1 GiB of HBM per device.

```python
import jax
import jax.numpy as jnp
from jax import lax

BATCH_SIZE = 8192
D_MODEL = 2816
NUM_HEADS = 22
HEAD_DIM = 128
FF_DIM = 11264
CACHE_LEN = 128


def setup_inputs(seed: int = 0, part: int = 0) -> dict:
    part_key = jax.random.fold_in(jax.random.key(seed), part)
    shared_key = jax.random.key(seed + 1)
    x_key, kc_key, vc_key, vm_key, len_key = jax.random.split(part_key, 5)
    g_key, qkv_key, gate_key, up_key, ao_key, mo_key = jax.random.split(shared_key, 6)
    qkv_cols = (NUM_HEADS + 2) * HEAD_DIM
    attn_cols = NUM_HEADS * HEAD_DIM
    x_in = jax.random.normal(x_key, (BATCH_SIZE, D_MODEL), jnp.float32)
    ln_gain = jax.random.uniform(g_key, (D_MODEL,), jnp.float32, 0.5, 1.5)
    w_qkv = jax.random.normal(qkv_key, (D_MODEL, qkv_cols), jnp.float32) * D_MODEL ** -0.5
    w_gate = jax.random.normal(gate_key, (D_MODEL, FF_DIM), jnp.float32) * D_MODEL ** -0.5
    w_up = jax.random.normal(up_key, (D_MODEL, FF_DIM), jnp.float32) * D_MODEL ** -0.5
    w_attn_out = jax.random.normal(ao_key, (attn_cols, D_MODEL), jnp.float32) * attn_cols ** -0.5
    w_mlp_out = jax.random.normal(mo_key, (FF_DIM, D_MODEL), jnp.float32) * FF_DIM ** -0.5
    k_cache = jax.random.normal(kc_key, (BATCH_SIZE, CACHE_LEN, HEAD_DIM), jnp.float32)
    v_mean = jax.random.normal(vm_key, (BATCH_SIZE, 1, HEAD_DIM), jnp.float32)
    v_cache = v_mean + 0.7 * jax.random.normal(vc_key, (BATCH_SIZE, CACHE_LEN, HEAD_DIM), jnp.float32)
    ctx_len = jax.random.randint(len_key, (BATCH_SIZE,), CACHE_LEN // 8, CACHE_LEN, jnp.int32)
    ctx_len = ctx_len.at[0].set(CACHE_LEN - 1).at[1].set(CACHE_LEN // 8)
    return {
        "x_in": x_in.astype(jnp.bfloat16),
        "ln_gain": ln_gain.astype(jnp.bfloat16),
        "w_qkv": w_qkv.astype(jnp.bfloat16),
        "w_gate": w_gate.astype(jnp.bfloat16),
        "w_up": w_up.astype(jnp.bfloat16),
        "w_attn_out": w_attn_out.astype(jnp.bfloat16),
        "w_mlp_out": w_mlp_out.astype(jnp.bfloat16),
        "k_cache": k_cache.astype(jnp.bfloat16),
        "v_cache": v_cache.astype(jnp.bfloat16),
        "ctx_len": ctx_len,
    }


def apply_rope(vecs, positions):
    half_dim = vecs.shape[-1] // 2
    inv_freq = 10000.0 ** (-jnp.arange(half_dim, dtype=jnp.float32) / half_dim)
    angles = positions.astype(jnp.float32)[..., None] * inv_freq
    cos_t = jnp.cos(angles)
    sin_t = jnp.sin(angles)
    first_half = vecs[..., :half_dim]
    second_half = vecs[..., half_dim:]
    return jnp.concatenate([first_half * cos_t - second_half * sin_t, second_half * cos_t + first_half * sin_t], axis=-1)


def layer_norm(x_in, ln_gain):
    x_f32 = x_in.astype(jnp.float32)
    row_mean = jnp.sum(x_f32, axis=-1, keepdims=True) / D_MODEL
    row_var = jnp.sum(x_f32 * x_f32, axis=-1, keepdims=True) / D_MODEL - row_mean * row_mean
    normed = (x_f32 - row_mean) * lax.rsqrt(row_var + 1e-6) * ln_gain.astype(jnp.float32)
    return normed.astype(jnp.bfloat16)


def reference(x_in, ln_gain, w_qkv, w_gate, w_up, w_attn_out, w_mlp_out, k_cache, v_cache, ctx_len):
    normed = layer_norm(x_in, ln_gain)
    qkv_proj = jnp.dot(normed, w_qkv, preferred_element_type=jnp.float32).astype(jnp.bfloat16)
    gate_proj = jnp.dot(normed, w_gate, preferred_element_type=jnp.float32).astype(jnp.bfloat16)
    up_proj = jnp.dot(normed, w_up, preferred_element_type=jnp.float32).astype(jnp.bfloat16)
    mlp_act = (jax.nn.silu(gate_proj.astype(jnp.float32)) * up_proj.astype(jnp.float32)).astype(jnp.bfloat16)
    attn_cols = NUM_HEADS * HEAD_DIM
    q_heads = qkv_proj[:, :attn_cols].reshape(BATCH_SIZE, NUM_HEADS, HEAD_DIM)
    k_new = qkv_proj[:, attn_cols:attn_cols + HEAD_DIM]
    v_new = qkv_proj[:, attn_cols + HEAD_DIM:]
    q_rot = apply_rope(q_heads.astype(jnp.float32), ctx_len[:, None]).astype(jnp.bfloat16)
    k_rot = apply_rope(k_new.astype(jnp.float32), ctx_len).astype(jnp.bfloat16)
    positions = jnp.arange(CACHE_LEN)
    new_slot = (positions[None, :] == ctx_len[:, None])[:, :, None]
    k_out = jnp.where(new_slot, k_rot[:, None, :], k_cache)
    v_out = jnp.where(new_slot, v_new[:, None, :], v_cache)
    block_rows = 8
    n_blocks = BATCH_SIZE // block_rows

    def attend(block_in):
        q_blk, k_blk, v_blk, len_blk = block_in
        scores = jnp.einsum("bhd,btd->bht", q_blk.astype(jnp.float32), k_blk.astype(jnp.float32)) * HEAD_DIM ** -0.5
        visible = (positions[None, :] <= len_blk[:, None])[:, None, :]
        scores = jnp.where(visible, scores, -1e30)
        attn_probs = jax.nn.softmax(scores, axis=-1).astype(jnp.bfloat16)
        return jnp.einsum("bht,btd->bhd", attn_probs.astype(jnp.float32), v_blk.astype(jnp.float32)).astype(jnp.bfloat16)

    attn_heads = lax.map(attend, (
        q_rot.reshape(n_blocks, block_rows, NUM_HEADS, HEAD_DIM),
        k_out.reshape(n_blocks, block_rows, CACHE_LEN, HEAD_DIM),
        v_out.reshape(n_blocks, block_rows, CACHE_LEN, HEAD_DIM),
        ctx_len.reshape(n_blocks, block_rows),
    ))
    attn_flat = attn_heads.reshape(BATCH_SIZE, attn_cols)
    z_sum = jnp.dot(attn_flat, w_attn_out, preferred_element_type=jnp.float32) + jnp.dot(mlp_act, w_mlp_out, preferred_element_type=jnp.float32)
    y_out = (x_in.astype(jnp.float32) + z_sum).astype(jnp.bfloat16)
    return (y_out, k_out, v_out)
```

```python
import jax
import jax.numpy as jnp
from jax import lax
from jax.sharding import PartitionSpec as P


def apply_rope(vecs, positions):
    half_dim = vecs.shape[-1] // 2
    inv_freq = 10000.0 ** (-jnp.arange(half_dim, dtype=jnp.float32) / half_dim)
    angles = positions.astype(jnp.float32)[..., None] * inv_freq
    cos_t = jnp.cos(angles)
    sin_t = jnp.sin(angles)
    first_half = vecs[..., :half_dim]
    second_half = vecs[..., half_dim:]
    return jnp.concatenate([first_half * cos_t - second_half * sin_t, second_half * cos_t + first_half * sin_t], axis=-1)


def attend_local(q_rot, k_all, v_all, ctx_len):
    head_dim = q_rot.shape[-1]
    positions = jnp.arange(k_all.shape[1])
    scores = jnp.einsum("bhd,btd->bht", q_rot, k_all, preferred_element_type=jnp.float32) * head_dim ** -0.5
    visible = (positions[None, :] <= ctx_len[:, None])[:, None, :]
    scores = jnp.where(visible, scores, -1e30)
    attn_probs = jax.nn.softmax(scores, axis=-1).astype(jnp.bfloat16)
    return jnp.einsum("bht,btd->bhd", attn_probs, v_all, preferred_element_type=jnp.float32).astype(jnp.bfloat16)


def solution(mesh):
    xs = mesh.shape["x"]
    yzs = mesh.shape["yz"]
    both_axes = ("x", "yz")
    row_spec = P("dp", both_axes)
    in_w_spec = P("x", "yz")
    out_w_spec = P("yz", "x")
    cache_spec = P(("dp", "x", "yz"), None, None)
    len_spec = P(("dp", "x", "yz"))

    def local_layer(x_loc, gain_loc, wqkv_loc, wgate_loc, wup_loc, wao_loc, wmo_loc, kc_loc, vc_loc, len_loc):
        n_rows, grp = x_loc.shape
        pad = -grp % 8
        gp = grp + pad
        d_model = grp * xs * yzs
        head_dim = kc_loc.shape[2]
        dev_rows = kc_loc.shape[0]
        rows = n_rows // xs
        attn_cols = wao_loc.shape[0] * yzs
        num_heads = attn_cols // head_dim
        f32, bf16 = jnp.float32, jnp.bfloat16

        w1_loc = jnp.concatenate([wqkv_loc, wgate_loc, wup_loc], axis=1)
        n1 = w1_loc.shape[1]
        w1_loc = jnp.pad(w1_loc.reshape(yzs, grp, n1), ((0, 0), (0, pad), (0, 0))).reshape(yzs * gp, n1)
        w1 = lax.all_gather(w1_loc, "x", axis=0, tiled=True)
        w2_loc = jnp.concatenate([wao_loc, wmo_loc], axis=0).T
        n2 = w2_loc.shape[1]
        w2_loc = jnp.pad(w2_loc.reshape(yzs, grp, n2), ((0, 0), (0, pad), (0, 0))).reshape(yzs * gp, n2)
        w2 = lax.all_gather(w2_loc, "x", axis=0, tiled=False)

        x_t = x_loc.T.reshape(grp, xs, rows).transpose(1, 0, 2)
        gain_row = jnp.broadcast_to(jnp.pad(gain_loc, (0, rows - grp)).reshape(1, 1, rows), (xs, 1, rows))
        x_pad = jnp.concatenate([x_t, gain_row, jnp.zeros((xs, pad - 1, rows), bf16)], axis=1)
        x_mine = lax.all_to_all(x_pad, "x", 0, 0, tiled=True)
        x_all = lax.all_gather(x_mine, "yz", axis=0, tiled=False)
        gain = x_all[:, :, grp, :grp].astype(f32)[..., None]
        x_f32 = x_all[:, :, :grp, :].astype(f32)
        row_mean = jnp.sum(x_f32, axis=(0, 1, 2), keepdims=True) / d_model
        row_var = jnp.sum(x_f32 * x_f32, axis=(0, 1, 2), keepdims=True) / d_model - row_mean * row_mean
        normed = ((x_f32 - row_mean) * lax.rsqrt(row_var + 1e-6) * gain).astype(bf16)
        normed = jnp.pad(normed, ((0, 0), (0, 0), (0, pad), (0, 0))).transpose(1, 0, 2, 3).reshape(xs * yzs * gp, rows)

        c_q = wqkv_loc.shape[1]
        c_f = wgate_loc.shape[1]
        cd = (((0,), (0,)), ((), ()))
        qkv = lax.dot_general(normed, w1[:, :c_q], cd, preferred_element_type=f32).astype(bf16)
        gate = lax.dot_general(w1[:, c_q:c_q + c_f], normed, cd, preferred_element_type=f32).astype(bf16)
        up = lax.dot_general(w1[:, c_q + c_f:], normed, cd, preferred_element_type=f32).astype(bf16)
        mlp_t = (jax.nn.silu(gate.astype(f32)) * up.astype(f32)).astype(bf16)

        qkv_dev = lax.all_to_all(qkv, "yz", 0, 1, tiled=True)
        q_heads = qkv_dev[:, :attn_cols].reshape(dev_rows, num_heads, head_dim)
        k_new = qkv_dev[:, attn_cols:attn_cols + head_dim]
        v_new = qkv_dev[:, attn_cols + head_dim:]
        q_rot = apply_rope(q_heads.astype(f32), len_loc[:, None]).astype(bf16)
        k_rot = apply_rope(k_new.astype(f32), len_loc).astype(bf16)
        new_slot = (jnp.arange(kc_loc.shape[1])[None, :] == len_loc[:, None])[:, :, None]
        k_all = jnp.where(new_slot, k_rot[:, None, :], kc_loc)
        v_all = jnp.where(new_slot, v_new[:, None, :], vc_loc)
        attn_dev = attend_local(q_rot, k_all, v_all, len_loc).reshape(dev_rows, attn_cols)
        attn_rows = lax.all_to_all(attn_dev, "yz", 1, 0, tiled=True)

        w2_p = w2.reshape(xs, yzs, gp, n2).transpose(1, 0, 2, 3).reshape(yzs * xs * gp, n2)
        c_a = wao_loc.shape[0]
        z_part = jnp.dot(w2_p[:, c_a:], mlp_t, preferred_element_type=f32)
        z_part = z_part + lax.dot_general(w2_p[:, :c_a], attn_rows, (((1,), (1,)), ((), ())), preferred_element_type=f32)
        z_loc = lax.psum_scatter(z_part, "yz", scatter_dimension=0, tiled=True)
        z_loc = z_loc.reshape(xs, gp, rows)
        y_mine = (x_mine.astype(f32) + z_loc).astype(bf16)
        y_back = lax.all_to_all(y_mine, "x", 0, 0, tiled=True)
        y_loc = y_back[:, :grp].transpose(1, 0, 2).reshape(grp, n_rows).T
        return y_loc, k_all, v_all

    in_specs = (row_spec, P(both_axes), in_w_spec, in_w_spec, in_w_spec, out_w_spec, out_w_spec, cache_spec, cache_spec, len_spec)
    out_specs = (row_spec, cache_spec, cache_spec)
    return jax.shard_map(local_layer, mesh=mesh, in_specs=in_specs, out_specs=out_specs, check_vma=False)
```

```python
import functools

import jax
import jax.numpy as jnp
from jax import lax
from jax.experimental import pallas as pl
from jax.experimental.pallas import tpu as pltpu
from jax.sharding import PartitionSpec as P

MESH = pl.DeviceIdType.MESH
RING = 4
VMEM_LIMIT = 62 * 1024 * 1024


def apply_rope(vecs, positions):
    half_dim = vecs.shape[-1] // 2
    inv_freq = 10000.0 ** (-jnp.arange(half_dim, dtype=jnp.float32) / half_dim)
    angles = positions.astype(jnp.float32)[..., None] * inv_freq
    cos_t = jnp.cos(angles)
    sin_t = jnp.sin(angles)
    first_half = vecs[..., :half_dim]
    second_half = vecs[..., half_dim:]
    return jnp.concatenate([first_half * cos_t - second_half * sin_t, second_half * cos_t + first_half * sin_t], axis=-1)


def attend_local(q_rot, k_all, v_all, ctx_len):
    head_dim = q_rot.shape[-1]
    positions = jnp.arange(k_all.shape[1])
    scores = jnp.einsum("bhd,btd->bht", q_rot, k_all, preferred_element_type=jnp.float32) * head_dim ** -0.5
    visible = (positions[None, :] <= ctx_len[:, None])[:, None, :]
    scores = jnp.where(visible, scores, -1e30)
    attn_probs = jax.nn.softmax(scores, axis=-1).astype(jnp.bfloat16)
    return jnp.einsum("bht,btd->bhd", attn_probs, v_all, preferred_element_type=jnp.float32).astype(jnp.bfloat16)


class Where:
    def __init__(self, xs):
        self.xs = xs
        self.dp = lax.axis_index("dp")
        self.x = lax.axis_index("x")
        self.j = lax.axis_index("yz")
        self.zz = self.j // RING
        self.yy = self.j % RING
        self.chip = self.x // 2
        self.core = self.x % 2

    def block(self, dz, dy):
        return ((self.zz + dz) % RING) * RING + (self.yy + dy) % RING

    def on_yz(self, j):
        return (self.dp, j, self.x)

    def on_x(self, x):
        return (self.dp, self.j, x)

    def axis_block(self, first, df, dg):
        return self.block(df, dg) if first == "z" else self.block(dg, df)

    def step(self, first, axis, d):
        return self.on_yz(self.axis_block(first, d, 0) if axis == 0 else self.axis_block(first, 0, d))

    def x_of(self, dc):
        return ((self.chip + dc) % RING) * 2 + self.core

    def x_other(self, dc):
        return ((self.chip + dc) % RING) * 2 + (1 - self.core)

    def greet(self):
        barrier = pltpu.get_barrier_semaphore()
        peers = [self.on_x((self.x + d) % self.xs) for d in range(1, self.xs)]
        peers += [self.on_yz(self.block(*d)) for d in ((1, 0), (3, 0), (0, 1), (0, 3))]
        for peer in peers:
            pl.semaphore_signal(barrier, inc=1, device_id=peer, device_id_type=MESH)
        pl.semaphore_wait(barrier, len(peers))


def remote(src, dst, send, recv, peer):
    return pltpu.make_async_remote_copy(src_ref=src, dst_ref=dst, send_sem=send, recv_sem=recv, device_id=peer, device_id_type=MESH)


def gather_kernel(xs, x_ref, w_ref, xg_ref, wg_ref, loc_sem, xsend, xrecv, gsend, grecv, wsend, wrecv):
    at = Where(xs)
    half = xs // 2
    quarter = half // 2
    at.greet()
    started = []

    def send(src, dst, sems, idx, peer):
        copy = remote(src, dst, sems[0].at[idx], sems[1].at[idx], peer)
        copy.start()
        started.append(copy)

    def arrived(region, sems, idx):
        remote(region, region, sems[0].at[idx], sems[1].at[idx], at.on_yz(at.block(0, 1))).wait_recv()

    xsem, wsem = (xsend, xrecv), (wsend, wrecv)
    own_x = pltpu.make_async_copy(x_ref.at[at.x], xg_ref.at[at.x, at.j], loc_sem.at[0])
    own_x.start()
    for d in range(1, xs):
        to = (at.x + d) % xs
        send(x_ref.at[to], xg_ref.at[at.x, at.j], xsem, d - 1, at.on_x(to))
    own_w = pltpu.make_async_copy(w_ref, wg_ref.at[at.x], loc_sem.at[1])
    own_w.start()
    send(w_ref, wg_ref.at[at.x], wsem, 0, at.on_x(at.x_of(1)))
    send(w_ref, wg_ref.at[at.x], wsem, 1, at.on_x(at.x_of(3)))
    send(w_ref, wg_ref.at[at.x], wsem, 2, at.on_x(at.x_other(0)))
    own_x.wait()
    for d in range(1, xs):
        arrived(xg_ref.at[(at.x + xs - d) % xs, at.j], xsem, d - 1)

    order = ("y", "z")

    def region(h, df, dg, lo=0, n=half):
        return xg_ref.at[pl.ds(h * half + lo, n), at.axis_block(order[h], df, dg)]

    def gsend_block(h, df, dg, axis, d, slot, lo=0, n=half):
        r = region(h, df, dg, lo, n)
        send(r, r, (gsend.at[h], grecv.at[h]), slot, at.step(order[h], axis, d))

    def garrived(h, df, dg, slot, lo=0, n=half):
        arrived(region(h, df, dg, lo, n), (gsend.at[h], grecv.at[h]), slot)

    for h in range(2):
        gsend_block(h, 0, 0, 0, 1, 0)
        gsend_block(h, 0, 0, 0, 3, 1)
        gsend_block(h, 0, 0, 1, 1, 4)
        gsend_block(h, 0, 0, 1, 3, 8)
    for h in range(2):
        garrived(h, 3, 0, 0)
        gsend_block(h, 3, 0, 0, 1, 2, 0, quarter)
        garrived(h, 1, 0, 1)
        gsend_block(h, 1, 0, 0, 3, 3, quarter, quarter)
        gsend_block(h, 3, 0, 1, 1, 4 + 3)
        gsend_block(h, 3, 0, 1, 3, 8 + 3)
        gsend_block(h, 1, 0, 1, 1, 4 + 1)
        gsend_block(h, 1, 0, 1, 3, 8 + 1)
    for h in range(2):
        garrived(h, 2, 0, 2, 0, quarter)
        garrived(h, 2, 0, 3, quarter, quarter)
        gsend_block(h, 2, 0, 1, 1, 4 + 2)
        gsend_block(h, 2, 0, 1, 3, 8 + 2)
    for h in range(2):
        for df in (0, 3):
            garrived(h, df, 3, 4 + df)
            gsend_block(h, df, 3, 1, 1, 12 + df)
    wrows = w_ref.shape[0] // 2

    def wregion(x, lo=None):
        return wg_ref.at[x] if lo is None else wg_ref.at[x, pl.ds(lo * wrows, wrows)]

    def wsend_block(r, slot, x):
        send(r, r, wsem, slot, at.on_x(x))

    arrived(wregion(at.x_of(3)), wsem, 0)
    wsend_block(wregion(at.x_of(3), 0), 3, at.x_of(1))
    arrived(wregion(at.x_of(1)), wsem, 1)
    wsend_block(wregion(at.x_of(1), 1), 4, at.x_of(3))
    wsend_block(wregion(at.x_of(3)), 5, at.x_other(0))
    wsend_block(wregion(at.x_of(1)), 6, at.x_other(0))
    for h in range(2):
        for df in (1, 2):
            garrived(h, df, 1, 8 + df)
            gsend_block(h, df, 1, 1, 3, 12 + df)
    arrived(wregion(at.x_of(2), 0), wsem, 3)
    wsend_block(wregion(at.x_of(2), 0), 7, at.x_other(0))
    arrived(wregion(at.x_of(2), 1), wsem, 4)
    wsend_block(wregion(at.x_of(2), 1), 8, at.x_other(0))
    for h in range(2):
        for df in (1, 2):
            garrived(h, df, 3, 4 + df)
        for df in (0, 3):
            garrived(h, df, 1, 8 + df)
        for df in range(4):
            garrived(h, df, 2, 12 + df)
    arrived(wregion(at.x_other(0)), wsem, 2)
    arrived(wregion(at.x_other(3)), wsem, 5)
    arrived(wregion(at.x_other(1)), wsem, 6)
    arrived(wregion(at.x_other(2), 0), wsem, 7)
    arrived(wregion(at.x_other(2), 1), wsem, 8)
    own_w.wait()
    for copy in started:
        copy.wait_send()


def gather_inputs(x_pad, w_loc, xs, yzs):
    _, gp, rows = x_pad.shape
    dma = pltpu.SemaphoreType.DMA
    return pl.pallas_call(
        functools.partial(gather_kernel, xs),
        out_shape=(
            jax.ShapeDtypeStruct((xs, yzs, gp, rows), x_pad.dtype),
            jax.ShapeDtypeStruct((xs,) + w_loc.shape, w_loc.dtype),
        ),
        in_specs=[pl.BlockSpec(memory_space=pltpu.VMEM)] * 2,
        out_specs=(pl.BlockSpec(memory_space=pl.ANY), pl.BlockSpec(memory_space=pl.ANY)),
        scratch_shapes=[dma((2,)), dma((xs - 1,)), dma((xs - 1,)), dma((2, 16)), dma((2, 16)), dma((9,)), dma((9,))],
        compiler_params=pltpu.CompilerParams(collective_id=0, has_side_effects=True, vmem_limit_bytes=VMEM_LIMIT),
        name="gather_inputs",
    )(x_pad, w_loc)


def scatter_kernel(xs, c_a, w_ref, a_ref, o_ref, xg_ref, y_ref, zb, r1, r2, r3, r4, xv, yv, loc_sem, s1, q1, s2, q2, s3, q3, s4, q4, ys, yq):
    at = Where(xs)
    order = ("z", "y")
    hr = zb.shape[2] // 2
    gp = xv.shape[1]
    own_x = pltpu.make_async_copy(xg_ref.at[:, at.j], xv, loc_sem.at[0])
    own_x.start()
    at.greet()
    started = []

    def send(src, dst, ssem, rsem, peer):
        copy = remote(src, dst, ssem, rsem, peer)
        copy.start()
        started.append(copy)

    def arrived(dst, ssem, rsem):
        remote(dst, dst, ssem, rsem, at.on_yz(at.block(0, 1))).wait_recv()

    def zat(h, df, dg):
        dz, dy = (df, dg) if order[h] == "z" else (dg, df)
        return zb.at[dz, dy, pl.ds(h * hr, hr)]

    def compute(dz, dy):
        w = w_ref[at.block(dz, dy)]
        z = jnp.dot(w[:, c_a:], a_ref[...], preferred_element_type=jnp.float32)
        z = z + lax.dot_general(w[:, :c_a], o_ref[...], (((1,), (1,)), ((), ())), preferred_element_type=jnp.float32)
        zb[dz, dy] = z

    def compute_cell(i, dz):
        compute(dz, i)
        return dz

    for dy in range(RING):
        compute(2, dy)
    for dz in (0, 1, 3):
        compute(dz, 2)
    for h in range(2):
        for dg in range(RING):
            d = 1 if dg < 2 else 3
            send(zat(h, 2, dg), r1.at[h, dg], s1.at[h, dg], q1.at[h, dg], at.step(order[h], 0, d))
    for dz in (1, 3, 0):
        for dy in (0, 1, 3):
            compute(dz, dy)
    def send2(h, up, dg):
        df, d, s = (1, 1, 0) if up else (3, 3, 1)
        send(zat(h, df, dg), r2.at[h, s, dg], s2.at[h, s, dg], q2.at[h, s, dg], at.step(order[h], 0, d))

    for h in range(2):
        for dg in (2, 3):
            send2(h, True, dg)
        for dg in (0, 1):
            send2(h, False, dg)
    for k in range(2):
        for h in range(2):
            for up in (True, False):
                dg = k if up else 2 + k
                arrived(r1.at[h, dg], s1.at[h, dg], q1.at[h, dg])
                ref = zat(h, 1 if up else 3, dg)
                ref[...] = ref[...] + r1[h, dg]
                send2(h, up, dg)
    def plane(h, dg):
        for s in range(2):
            arrived(r2.at[h, s, dg], s2.at[h, s, dg], q2.at[h, s, dg])
        ref = zat(h, 0, dg)
        ref[...] = ref[...] + r2[h, 0, dg] + r2[h, 1, dg]

    hh = hr // 2

    def part(h, dg, k):
        dz, dy = (0, dg) if order[h] == "z" else (dg, 0)
        return zb.at[dz, dy, pl.ds(h * hr + k * hh, hh)]

    def send4(h, up, k):
        dg, d, s = (1, 1, 0) if up else (3, 3, 1)
        send(part(h, dg, k), r4.at[h, s, k], s4.at[h, s, k], q4.at[h, s, k], at.step(order[h], 1, d))

    for h in range(2):
        plane(h, 2)
        send(part(h, 2, 0), r3.at[h, 0], s3.at[h, 0], q3.at[h, 0], at.step(order[h], 1, 1))
        send(part(h, 2, 1), r3.at[h, 1], s3.at[h, 1], q3.at[h, 1], at.step(order[h], 1, 3))
    for h in range(2):
        plane(h, 1)
        send4(h, True, 1)
        plane(h, 3)
        send4(h, False, 0)
    for h in range(2):
        plane(h, 0)
    for h in range(2):
        arrived(r3.at[h, 0], s3.at[h, 0], q3.at[h, 0])
        ref = part(h, 1, 0)
        ref[...] = ref[...] + r3[h, 0]
        send4(h, True, 0)
        arrived(r3.at[h, 1], s3.at[h, 1], q3.at[h, 1])
        ref = part(h, 3, 1)
        ref[...] = ref[...] + r3[h, 1]
        send4(h, False, 1)
    own_x.wait()
    for h in range(2):
        for k in range(2):
            for s in range(2):
                arrived(r4.at[h, s, k], s4.at[h, s, k], q4.at[h, s, k])
            z = zb[0, 0, pl.ds(h * hr + k * hh, hh)] + r4[h, 0, k] + r4[h, 1, k]
            n = hh // gp
            for i in range(n):
                x = h * 2 * n + k * n + i
                yv[x] = (xv[x].astype(jnp.float32) + z[i * gp:(i + 1) * gp]).astype(jnp.bfloat16)
    own_y = pltpu.make_async_copy(yv.at[at.x], y_ref.at[at.x], loc_sem.at[1])
    own_y.start()
    for d in range(1, xs):
        to = (at.x + d) % xs
        send(yv.at[to], y_ref.at[at.x], ys.at[d - 1], yq.at[d - 1], at.on_x(to))
    for d in range(1, xs):
        arrived(y_ref.at[(at.x + xs - d) % xs], ys.at[d - 1], yq.at[d - 1])
    own_y.wait()
    for copy in started:
        copy.wait_send()


def project_and_scatter(w2, mlp_t, attn_rows, xg):
    yzs, block, _ = w2.shape
    xs, _, gp, rows = xg.shape
    c_a = attn_rows.shape[1]
    dma = pltpu.SemaphoreType.DMA
    vmem = lambda *s: pltpu.VMEM(s, jnp.float32)
    hr = block // 2
    return pl.pallas_call(
        functools.partial(scatter_kernel, xs, c_a),
        out_shape=jax.ShapeDtypeStruct((xs, gp, rows), jnp.bfloat16),
        in_specs=[pl.BlockSpec(memory_space=pltpu.VMEM)] * 3 + [pl.BlockSpec(memory_space=pl.ANY)],
        out_specs=pl.BlockSpec(memory_space=pl.ANY),
        scratch_shapes=[
            vmem(RING, RING, block, rows),
            vmem(2, RING, hr, rows),
            vmem(2, 2, RING, hr, rows),
            vmem(2, 2, hr // 2, rows),
            vmem(2, 2, 2, hr // 2, rows),
            pltpu.VMEM((xs, gp, rows), jnp.bfloat16),
            pltpu.VMEM((xs, gp, rows), jnp.bfloat16),
            dma((2,)),
            dma((2, RING)), dma((2, RING)),
            dma((2, 2, RING)), dma((2, 2, RING)),
            dma((2, 2)), dma((2, 2)),
            dma((2, 2, 2)), dma((2, 2, 2)),
            dma((xs - 1,)), dma((xs - 1,)),
        ],
        compiler_params=pltpu.CompilerParams(collective_id=1, has_side_effects=True, vmem_limit_bytes=VMEM_LIMIT),
        name="project_and_scatter",
    )(w2, mlp_t, attn_rows, xg)


def solution(mesh):
    xs = mesh.shape["x"]
    yzs = mesh.shape["yz"]
    both_axes = ("x", "yz")
    row_spec = P("dp", both_axes)
    in_w_spec = P("x", "yz")
    out_w_spec = P("yz", "x")
    cache_spec = P(("dp", "x", "yz"), None, None)
    len_spec = P(("dp", "x", "yz"))

    def local_layer(x_loc, gain_loc, wqkv_loc, wgate_loc, wup_loc, wao_loc, wmo_loc, kc_loc, vc_loc, len_loc):
        n_rows, grp = x_loc.shape
        pad = -grp % 8
        gp = grp + pad
        d_model = grp * xs * yzs
        head_dim = kc_loc.shape[2]
        dev_rows = kc_loc.shape[0]
        rows = n_rows // xs
        attn_cols = wao_loc.shape[0] * yzs
        num_heads = attn_cols // head_dim
        f32, bf16 = jnp.float32, jnp.bfloat16

        w1_loc = jnp.concatenate([wqkv_loc, wgate_loc, wup_loc], axis=1)
        n1 = w1_loc.shape[1]
        w1_loc = jnp.pad(w1_loc.reshape(yzs, grp, n1), ((0, 0), (0, pad), (0, 0))).reshape(yzs * gp, n1)
        w2_loc = jnp.concatenate([wao_loc, wmo_loc], axis=0).T
        n2 = w2_loc.shape[1]
        w2_loc = jnp.pad(w2_loc.reshape(yzs, grp, n2), ((0, 0), (0, pad), (0, 0))).reshape(yzs * gp, n2)
        w2 = lax.all_gather(w2_loc, "x", axis=0, tiled=False)
        w2_p = w2.reshape(xs, yzs, gp, n2).transpose(1, 0, 2, 3).reshape(yzs, xs * gp, n2)

        x_t = x_loc.T.reshape(grp, xs, rows).transpose(1, 0, 2)
        gain_row = jnp.broadcast_to(jnp.pad(gain_loc, (0, rows - grp)).reshape(1, 1, rows), (xs, 1, rows))
        x_pad = jnp.concatenate([x_t, gain_row, jnp.zeros((xs, pad - 1, rows), bf16)], axis=1)
        x_all, w1 = gather_inputs(x_pad, w1_loc, xs, yzs)
        w1 = w1.reshape(xs * yzs * gp, n1)
        gain = x_all[:, :, grp, :grp].astype(f32)[..., None]
        x_f32 = x_all[:, :, :grp, :].astype(f32)
        row_mean = jnp.sum(x_f32, axis=(0, 1, 2), keepdims=True) / d_model
        row_var = jnp.sum(x_f32 * x_f32, axis=(0, 1, 2), keepdims=True) / d_model - row_mean * row_mean
        normed = ((x_f32 - row_mean) * lax.rsqrt(row_var + 1e-6) * gain).astype(bf16)
        normed = jnp.pad(normed, ((0, 0), (0, 0), (0, pad), (0, 0))).reshape(xs * yzs * gp, rows)

        c_q = wqkv_loc.shape[1]
        c_f = wgate_loc.shape[1]
        cd = (((0,), (0,)), ((), ()))
        qkv = lax.dot_general(normed, w1[:, :c_q], cd, preferred_element_type=f32).astype(bf16)
        gate = lax.dot_general(w1[:, c_q:c_q + c_f], normed, cd, preferred_element_type=f32).astype(bf16)
        up = lax.dot_general(w1[:, c_q + c_f:], normed, cd, preferred_element_type=f32).astype(bf16)
        mlp_t = (jax.nn.silu(gate.astype(f32)) * up.astype(f32)).astype(bf16)

        qkv_dev = lax.all_to_all(qkv, "yz", 0, 1, tiled=True)
        q_heads = qkv_dev[:, :attn_cols].reshape(dev_rows, num_heads, head_dim)
        k_new = qkv_dev[:, attn_cols:attn_cols + head_dim]
        v_new = qkv_dev[:, attn_cols + head_dim:]
        q_rot = apply_rope(q_heads.astype(f32), len_loc[:, None]).astype(bf16)
        k_rot = apply_rope(k_new.astype(f32), len_loc).astype(bf16)
        new_slot = (jnp.arange(kc_loc.shape[1])[None, :] == len_loc[:, None])[:, :, None]
        k_all = jnp.where(new_slot, k_rot[:, None, :], kc_loc)
        v_all = jnp.where(new_slot, v_new[:, None, :], vc_loc)
        attn_dev = attend_local(q_rot, k_all, v_all, len_loc).reshape(dev_rows, attn_cols)
        attn_rows = lax.all_to_all(attn_dev, "yz", 1, 0, tiled=True)

        y_back = project_and_scatter(w2_p, mlp_t, attn_rows, x_all)
        y_loc = y_back[:, :grp].transpose(1, 0, 2).reshape(grp, n_rows).T
        return y_loc, k_all, v_all

    in_specs = (row_spec, P(both_axes), in_w_spec, in_w_spec, in_w_spec, out_w_spec, out_w_spec, cache_spec, cache_spec, len_spec)
    out_specs = (row_spec, cache_spec, cache_spec)
    return jax.shard_map(local_layer, mesh=mesh, in_specs=in_specs, out_specs=out_specs, check_vma=False)
```

```python
import functools

import jax
import jax.numpy as jnp
from jax import lax
from jax.experimental import pallas as pl
from jax.experimental.pallas import tpu as pltpu
from jax.sharding import PartitionSpec as P

MESH = pl.DeviceIdType.MESH
RING = 4
VMEM_LIMIT = 62 * 1024 * 1024


def apply_rope(vecs, positions):
    half_dim = vecs.shape[-1] // 2
    inv_freq = 10000.0 ** (-jnp.arange(half_dim, dtype=jnp.float32) / half_dim)
    angles = positions.astype(jnp.float32)[..., None] * inv_freq
    cos_t = jnp.cos(angles)
    sin_t = jnp.sin(angles)
    first_half = vecs[..., :half_dim]
    second_half = vecs[..., half_dim:]
    return jnp.concatenate([first_half * cos_t - second_half * sin_t, second_half * cos_t + first_half * sin_t], axis=-1)


def attend_local(q_rot, k_all, v_all, ctx_len):
    head_dim = q_rot.shape[-1]
    positions = jnp.arange(k_all.shape[1])
    scores = jnp.einsum("bhd,btd->bht", q_rot, k_all, preferred_element_type=jnp.float32) * head_dim ** -0.5
    visible = (positions[None, :] <= ctx_len[:, None])[:, None, :]
    scores = jnp.where(visible, scores, -1e30)
    attn_probs = jax.nn.softmax(scores, axis=-1).astype(jnp.bfloat16)
    return jnp.einsum("bht,btd->bhd", attn_probs, v_all, preferred_element_type=jnp.float32).astype(jnp.bfloat16)


class Where:
    def __init__(self, xs, yzs):
        self.xs = xs
        self.yzs = yzs
        self.dp = lax.axis_index("dp")
        self.x = lax.axis_index("x")
        self.j = lax.axis_index("yz")
        self.zz = self.j // RING
        self.yy = self.j % RING
        self.chip = self.x // 2
        self.core = self.x % 2

    def block(self, dz, dy):
        return ((self.zz + dz) % RING) * RING + (self.yy + dy) % RING

    def on_yz(self, j):
        return (self.dp, j, self.x)

    def on_x(self, x):
        return (self.dp, self.j, x)

    def axis_block(self, first, df, dg):
        return self.block(df, dg) if first == "z" else self.block(dg, df)

    def step(self, first, axis, d):
        return self.on_yz(self.axis_block(first, d, 0) if axis == 0 else self.axis_block(first, 0, d))

    def x_of(self, dc):
        return ((self.chip + dc) % RING) * 2 + self.core

    def x_other(self, dc):
        return ((self.chip + dc) % RING) * 2 + (1 - self.core)

    def greet(self):
        barrier = pltpu.get_barrier_semaphore()
        peers = [self.on_x((self.x + d) % self.xs) for d in range(1, self.xs)]
        peers += [self.on_yz((self.j + d) % self.yzs) for d in range(1, self.yzs)]
        for peer in peers:
            pl.semaphore_signal(barrier, inc=1, device_id=peer, device_id_type=MESH)
        pl.semaphore_wait(barrier, len(peers))


class Copies:
    def __init__(self, any_peer):
        self.any_peer = any_peer
        self.started = []

    def send(self, src, dst, ssem, rsem, peer):
        copy = pltpu.make_async_remote_copy(src_ref=src, dst_ref=dst, send_sem=ssem, recv_sem=rsem, device_id=peer, device_id_type=MESH)
        copy.start()
        self.started.append(copy)

    def arrived(self, dst, ssem, rsem):
        pltpu.make_async_remote_copy(
            src_ref=dst, dst_ref=dst, send_sem=ssem, recv_sem=rsem, device_id=self.any_peer, device_id_type=MESH
        ).wait_recv()

    def finish(self):
        for copy in self.started:
            copy.wait_send()


def front_kernel(xs, yzs, grp, c_q, c_f, x_ref, w1_ref, w2_ref, act_ref, qkv_ref, w2g_ref, xo_ref, xg, h, w1, qkv_s, loc_sem, xsend, xrecv, gsend, grecv, wsend, wrecv, vsend, vrecv, qsend, qrecv):
    f32, bf16 = jnp.float32, jnp.bfloat16
    at = Where(xs, yzs)
    half = xs // 2
    quarter = half // 2
    gp, rows = x_ref.shape[1:]
    dev_rows = rows // yzs
    kx = w1_ref.shape[1]
    at.greet()
    copies = Copies(at.on_yz(at.block(0, 1)))

    def send(src, dst, sems, idx, peer):
        copies.send(src, dst, sems[0].at[idx], sems[1].at[idx], peer)

    def arrived(region, sems, idx):
        copies.arrived(region, sems[0].at[idx], sems[1].at[idx])

    xsem, wsem, vsem, qsem = (xsend, xrecv), (wsend, wrecv), (vsend, vrecv), (qsend, qrecv)
    own_x = pltpu.make_async_copy(x_ref.at[at.x], xg.at[at.x, at.j], loc_sem.at[0])
    own_x.start()
    for d in range(1, xs):
        to = (at.x + d) % xs
        send(x_ref.at[to], xg.at[at.x, at.j], xsem, d - 1, at.on_x(to))

    n1 = w1_ref.shape[0]
    n2 = w2_ref.shape[0]

    def w1_at(x, k=None):
        cols = pl.ds(pl.multiple_of(x * kx, 128), kx)
        return w1.at[:, cols] if k is None else w1.at[pl.ds(k * (n1 // 2), n1 // 2), cols]

    def w2_at(x, k=None):
        return w2g_ref.at[:, x] if k is None else w2g_ref.at[pl.ds(k * (n2 // 2), n2 // 2), x]

    def spread_own(src, region, sems, loc):
        own = pltpu.make_async_copy(src, region(at.x), loc_sem.at[loc])
        own.start()
        send(src, region(at.x), sems, 0, at.on_x(at.x_of(1)))
        send(src, region(at.x), sems, 1, at.on_x(at.x_of(3)))
        send(src, region(at.x), sems, 2, at.on_x(at.x_other(0)))
        return own

    def pass_on(r, sems, slot, x):
        send(r, r, sems, slot, at.on_x(x))

    def forward_near(region, sems):
        arrived(region(at.x_of(3)), sems, 0)
        pass_on(region(at.x_of(3), 0), sems, 3, at.x_of(1))
        arrived(region(at.x_of(1)), sems, 1)
        pass_on(region(at.x_of(1), 1), sems, 4, at.x_of(3))
        pass_on(region(at.x_of(3)), sems, 5, at.x_other(0))
        pass_on(region(at.x_of(1)), sems, 6, at.x_other(0))

    def forward_far(region, sems):
        arrived(region(at.x_of(2), 0), sems, 3)
        pass_on(region(at.x_of(2), 0), sems, 7, at.x_other(0))
        arrived(region(at.x_of(2), 1), sems, 4)
        pass_on(region(at.x_of(2), 1), sems, 8, at.x_other(0))

    def all_in(region, sems, own):
        arrived(region(at.x_other(0)), sems, 2)
        arrived(region(at.x_other(3)), sems, 5)
        arrived(region(at.x_other(1)), sems, 6)
        arrived(region(at.x_other(2), 0), sems, 7)
        arrived(region(at.x_other(2), 1), sems, 8)
        own.wait()

    own_w1 = spread_own(w1_ref, w1_at, wsem, 1)
    own_x.wait()
    for d in range(1, xs):
        arrived(xg.at[(at.x + xs - d) % xs, at.j], xsem, d - 1)

    order = ("y", "z")

    def region(h_, df, dg, lo=0, n=half):
        return xg.at[pl.ds(h_ * half + lo, n), at.axis_block(order[h_], df, dg)]

    def gsend_block(h_, df, dg, axis, d, slot, lo=0, n=half):
        r = region(h_, df, dg, lo, n)
        send(r, r, (gsend.at[h_], grecv.at[h_]), slot, at.step(order[h_], axis, d))

    def garrived(h_, df, dg, slot, lo=0, n=half):
        arrived(region(h_, df, dg, lo, n), (gsend.at[h_], grecv.at[h_]), slot)

    for h_ in range(2):
        gsend_block(h_, 0, 0, 0, 1, 0)
        gsend_block(h_, 0, 0, 0, 3, 1)
        gsend_block(h_, 0, 0, 1, 1, 4)
        gsend_block(h_, 0, 0, 1, 3, 8)
    xo_ref[...] = xg[:, at.j]
    for h_ in range(2):
        garrived(h_, 3, 0, 0)
        gsend_block(h_, 3, 0, 0, 1, 2, 0, quarter)
        garrived(h_, 1, 0, 1)
        gsend_block(h_, 1, 0, 0, 3, 3, quarter, quarter)
        gsend_block(h_, 3, 0, 1, 1, 4 + 3)
        gsend_block(h_, 3, 0, 1, 3, 8 + 3)
        gsend_block(h_, 1, 0, 1, 1, 4 + 1)
        gsend_block(h_, 1, 0, 1, 3, 8 + 1)
    for h_ in range(2):
        garrived(h_, 2, 0, 2, 0, quarter)
        garrived(h_, 2, 0, 3, quarter, quarter)
        gsend_block(h_, 2, 0, 1, 1, 4 + 2)
        gsend_block(h_, 2, 0, 1, 3, 8 + 2)
    for h_ in range(2):
        for df in (0, 3):
            garrived(h_, df, 3, 4 + df)
            gsend_block(h_, df, 3, 1, 1, 12 + df)
    forward_near(w1_at, wsem)
    own_w2 = spread_own(w2_ref, w2_at, vsem, 2)
    for h_ in range(2):
        for df in (1, 2):
            garrived(h_, df, 1, 8 + df)
            gsend_block(h_, df, 1, 1, 3, 12 + df)
    for h_ in range(2):
        for df in (1, 2):
            garrived(h_, df, 3, 4 + df)
        for df in (0, 3):
            garrived(h_, df, 1, 8 + df)
        for df in range(4):
            garrived(h_, df, 2, 12 + df)

    pairs = yzs // 2
    feature = lax.broadcasted_iota(jnp.int32, (2, gp, 1), 1).reshape(2 * gp, 1)
    real = feature < grp
    diagonal = lax.broadcasted_iota(jnp.int32, (gp, 128), 0) == lax.broadcasted_iota(jnp.int32, (gp, 128), 1)

    def load(q):
        return xg[q // pairs, pl.ds((q % pairs) * 2, 2)].astype(f32).reshape(2 * gp, rows)

    def add_up(q, sums):
        v = jnp.where(real, load(q), 0.0)
        parts = v.reshape(2 * gp // 8, 8, rows)
        return sums[0] + jnp.sum(parts, axis=0), sums[1] + jnp.sum(parts * parts, axis=0)

    zero = jnp.zeros((8, rows), f32)
    s1, s2 = lax.fori_loop(0, xs * pairs, add_up, (zero, zero))
    d_model = grp * xs * yzs
    mean = jnp.sum(s1, axis=0, keepdims=True) / d_model
    var = jnp.sum(s2, axis=0, keepdims=True) / d_model - mean * mean
    scale = lax.rsqrt(var + 1e-6)

    def normalize(q, c):
        v = load(q)
        gains = [
            jnp.sum(jnp.where(diagonal, v[k * gp + grp:k * gp + grp + 1, :128], 0.0), axis=1, keepdims=True)
            for k in range(2)
        ]
        out = (v - mean) * scale * jnp.concatenate(gains, axis=0)
        h[pl.ds(pl.multiple_of(q * 2 * gp, 16), 2 * gp), :] = jnp.where(real, out, 0.0).astype(bf16)
        return c

    lax.fori_loop(0, xs * pairs, normalize, 0)
    forward_far(w1_at, wsem)
    all_in(w1_at, wsem, own_w1)

    nt = 256

    def query(n, c):
        q = jnp.dot(w1[:c_q], h[:, pl.ds(pl.multiple_of(n * nt, nt), nt)], preferred_element_type=f32)
        qkv_s[pl.ds(pl.multiple_of(n * nt, nt), nt), :] = q.T.astype(bf16)
        return c

    lax.fori_loop(0, rows // nt, query, 0)
    own_q = pltpu.make_async_copy(qkv_s.at[pl.ds(pl.multiple_of(at.j * dev_rows, dev_rows), dev_rows)], qkv_ref.at[at.j], loc_sem.at[3])
    own_q.start()
    for d in range(1, yzs):
        to = (at.j + d) % yzs
        src = qkv_s.at[pl.ds(pl.multiple_of(to * dev_rows, dev_rows), dev_rows)]
        send(src, qkv_ref.at[at.j], qsem, d - 1, at.on_yz(to))

    def mlp(n, c):
        cols = pl.ds(pl.multiple_of(n * nt, nt), nt)
        gate = jnp.dot(w1[c_q:c_q + c_f], h[:, cols], preferred_element_type=f32).astype(bf16).astype(f32)
        up = jnp.dot(w1[c_q + c_f:], h[:, cols], preferred_element_type=f32).astype(bf16).astype(f32)
        act_ref[:, cols] = (jax.nn.silu(gate) * up).astype(bf16)
        return c

    steps = rows // nt
    lax.fori_loop(0, steps // 2, mlp, 0)
    forward_near(w2_at, vsem)
    lax.fori_loop(steps // 2, steps, mlp, 0)
    forward_far(w2_at, vsem)
    for d in range(1, yzs):
        arrived(qkv_ref.at[(at.j + yzs - d) % yzs], qsem, d - 1)
    own_q.wait()
    all_in(w2_at, vsem, own_w2)
    copies.finish()


def front(x_pad, w1_loc, w2_loc, xs, yzs, grp, c_q, c_f):
    _, gp, rows = x_pad.shape
    n1, kx = w1_loc.shape
    dma = pltpu.SemaphoreType.DMA
    bf16 = jnp.bfloat16
    vspec, aspec = pl.BlockSpec(memory_space=pltpu.VMEM), pl.BlockSpec(memory_space=pl.ANY)
    sems = lambda *s: [dma(s), dma(s)]
    return pl.pallas_call(
        functools.partial(front_kernel, xs, yzs, grp, c_q, c_f),
        out_shape=(
            jax.ShapeDtypeStruct((c_f, rows), bf16),
            jax.ShapeDtypeStruct((yzs, rows // yzs, c_q), bf16),
            jax.ShapeDtypeStruct((yzs, xs) + w2_loc.shape[1:], bf16),
            jax.ShapeDtypeStruct((xs, gp, rows), bf16),
        ),
        in_specs=[vspec] * 3,
        out_specs=(vspec, aspec, aspec, vspec),
        scratch_shapes=[
            pltpu.VMEM((xs, yzs, gp, rows), bf16),
            pltpu.VMEM((xs * yzs * gp, rows), bf16),
            pltpu.VMEM((n1, xs * kx), bf16),
            pltpu.VMEM((rows, c_q), bf16),
            dma((4,)),
        ] + sems(xs - 1) + sems(2, 16) + sems(9) + sems(9) + sems(yzs - 1),
        compiler_params=pltpu.CompilerParams(collective_id=0, has_side_effects=True, vmem_limit_bytes=VMEM_LIMIT),
        name="front",
    )(x_pad, w1_loc, w2_loc)


def back_kernel(xs, yzs, w_ref, a_ref, o_ref, x_ref, y_ref, act, ob, zb, r1, r2, r3, r4, yv, loc_sem, os, oq, s1, q1, s2, q2, s3, q3, s4, q4, ys, yq):
    at = Where(xs, yzs)
    order = ("z", "y")
    hr = zb.shape[2] // 2
    gp = x_ref.shape[1]
    dev_rows = o_ref.shape[1]
    c_f = a_ref.shape[0]
    own_a = pltpu.make_async_copy(a_ref, act.at[pl.ds(0, c_f)], loc_sem.at[2])
    own_a.start()
    at.greet()
    copies = Copies(at.on_yz(at.block(0, 1)))
    send, arrived = copies.send, copies.arrived

    def mine(j):
        return ob.at[pl.ds(pl.multiple_of(j * dev_rows, dev_rows), dev_rows)]

    own_o = pltpu.make_async_copy(o_ref.at[at.j], mine(at.j), loc_sem.at[0])
    own_o.start()
    for d in range(1, yzs):
        to = (at.j + d) % yzs
        send(o_ref.at[to], mine(at.j), os.at[d - 1], oq.at[d - 1], at.on_yz(to))
    own_o.wait()
    for d in range(1, yzs):
        arrived(mine((at.j + yzs - d) % yzs), os.at[d - 1], oq.at[d - 1])
    act[pl.ds(c_f, ob.shape[1]), :] = ob[...].T
    own_a.wait()

    def zat(h, df, dg):
        dz, dy = (df, dg) if order[h] == "z" else (dg, df)
        return zb.at[dz, dy, pl.ds(h * hr, hr)]

    def compute(dz, dy):
        zb[dz, dy] = jnp.dot(w_ref[at.block(dz, dy)], act[...], preferred_element_type=jnp.float32)

    def compute_range(dz, dys):
        def body(i, c):
            compute(dz, i)
            return c

        lax.fori_loop(dys[0], dys[1], body, 0)

    def first(i, c):
        dz = jnp.where(i < RING, 2, (i - RING) + (i - RING) // 2)
        dy = jnp.where(i < RING, i, 2)
        compute(dz, dy)
        return c

    lax.fori_loop(0, 2 * RING - 1, first, 0)
    for h in range(2):
        for dg in range(RING):
            d = 1 if dg < 2 else 3
            send(zat(h, 2, dg), r1.at[h, dg], s1.at[h, dg], q1.at[h, dg], at.step(order[h], 0, d))

    def second(i, c):
        k, m = i // 3, i % 3
        compute(k + k // 2, m + m // 2)
        return c

    lax.fori_loop(0, 9, second, 0)

    def send2(h, up, dg):
        df, d, s = (1, 1, 0) if up else (3, 3, 1)
        send(zat(h, df, dg), r2.at[h, s, dg], s2.at[h, s, dg], q2.at[h, s, dg], at.step(order[h], 0, d))

    for h in range(2):
        for dg in (2, 3):
            send2(h, True, dg)
        for dg in (0, 1):
            send2(h, False, dg)
    for k in range(2):
        for h in range(2):
            for up in (True, False):
                dg = k if up else 2 + k
                arrived(r1.at[h, dg], s1.at[h, dg], q1.at[h, dg])
                ref = zat(h, 1 if up else 3, dg)
                ref[...] = ref[...] + r1[h, dg]
                send2(h, up, dg)

    def plane(h, dg):
        for s in range(2):
            arrived(r2.at[h, s, dg], s2.at[h, s, dg], q2.at[h, s, dg])
        ref = zat(h, 0, dg)
        ref[...] = ref[...] + r2[h, 0, dg] + r2[h, 1, dg]

    hh = hr // 2

    def part(h, dg, k):
        dz, dy = (0, dg) if order[h] == "z" else (dg, 0)
        return zb.at[dz, dy, pl.ds(h * hr + k * hh, hh)]

    def send4(h, up, k):
        dg, d, s = (1, 1, 0) if up else (3, 3, 1)
        send(part(h, dg, k), r4.at[h, s, k], s4.at[h, s, k], q4.at[h, s, k], at.step(order[h], 1, d))

    for h in range(2):
        plane(h, 2)
        send(part(h, 2, 0), r3.at[h, 0], s3.at[h, 0], q3.at[h, 0], at.step(order[h], 1, 1))
        send(part(h, 2, 1), r3.at[h, 1], s3.at[h, 1], q3.at[h, 1], at.step(order[h], 1, 3))
    for h in range(2):
        plane(h, 1)
        send4(h, True, 1)
        plane(h, 3)
        send4(h, False, 0)
    for h in range(2):
        plane(h, 0)
    for h in range(2):
        arrived(r3.at[h, 0], s3.at[h, 0], q3.at[h, 0])
        ref = part(h, 1, 0)
        ref[...] = ref[...] + r3[h, 0]
        send4(h, True, 0)
        arrived(r3.at[h, 1], s3.at[h, 1], q3.at[h, 1])
        ref = part(h, 3, 1)
        ref[...] = ref[...] + r3[h, 1]
        send4(h, False, 1)
    for h in range(2):
        for k in range(2):
            for s in range(2):
                arrived(r4.at[h, s, k], s4.at[h, s, k], q4.at[h, s, k])
            z = zb[0, 0, pl.ds(h * hr + k * hh, hh)] + r4[h, 0, k] + r4[h, 1, k]
            n = hh // gp
            for i in range(n):
                x = h * 2 * n + k * n + i
                yv[x] = (x_ref[x].astype(jnp.float32) + z[i * gp:(i + 1) * gp]).astype(jnp.bfloat16)
    own_y = pltpu.make_async_copy(yv.at[at.x], y_ref.at[at.x], loc_sem.at[1])
    own_y.start()
    for d in range(1, xs):
        to = (at.x + d) % xs
        send(yv.at[to], y_ref.at[at.x], ys.at[d - 1], yq.at[d - 1], at.on_x(to))
    for d in range(1, xs):
        arrived(y_ref.at[(at.x + xs - d) % xs], ys.at[d - 1], yq.at[d - 1])
    own_y.wait()
    copies.finish()


def back(w2, act, attn, x_own):
    yzs, block, n2 = w2.shape
    xs, gp, rows = x_own.shape
    dma = pltpu.SemaphoreType.DMA
    bf16 = jnp.bfloat16
    vmem = lambda *s: pltpu.VMEM(s, jnp.float32)
    vspec, aspec = pl.BlockSpec(memory_space=pltpu.VMEM), pl.BlockSpec(memory_space=pl.ANY)
    sems = lambda *s: [dma(s), dma(s)]
    hr = block // 2
    return pl.pallas_call(
        functools.partial(back_kernel, xs, yzs),
        out_shape=jax.ShapeDtypeStruct((xs, gp, rows), bf16),
        in_specs=[vspec, aspec, vspec, vspec],
        out_specs=aspec,
        scratch_shapes=[
            pltpu.VMEM((n2, rows), bf16),
            pltpu.VMEM((rows, attn.shape[2]), bf16),
            vmem(RING, RING, block, rows),
            vmem(2, RING, hr, rows),
            vmem(2, 2, RING, hr, rows),
            vmem(2, 2, hr // 2, rows),
            vmem(2, 2, 2, hr // 2, rows),
            pltpu.VMEM((xs, gp, rows), bf16),
            dma((3,)),
        ] + sems(yzs - 1) + sems(2, RING) + sems(2, 2, RING) + sems(2, 2) + sems(2, 2, 2) + sems(xs - 1),
        compiler_params=pltpu.CompilerParams(collective_id=1, has_side_effects=True, vmem_limit_bytes=VMEM_LIMIT),
        name="back",
    )(w2, act, attn, x_own)


def solution(mesh):
    xs = mesh.shape["x"]
    yzs = mesh.shape["yz"]
    both_axes = ("x", "yz")
    row_spec = P("dp", both_axes)
    in_w_spec = P("x", "yz")
    out_w_spec = P("yz", "x")
    cache_spec = P(("dp", "x", "yz"), None, None)
    len_spec = P(("dp", "x", "yz"))

    def local_layer(x_loc, gain_loc, wqkv_loc, wgate_loc, wup_loc, wao_loc, wmo_loc, kc_loc, vc_loc, len_loc):
        n_rows, grp = x_loc.shape
        pad = -grp % 8
        gp = grp + pad
        head_dim = kc_loc.shape[2]
        dev_rows = kc_loc.shape[0]
        rows = n_rows // xs
        attn_cols = wao_loc.shape[0] * yzs
        num_heads = attn_cols // head_dim
        f32, bf16 = jnp.float32, jnp.bfloat16

        def pad_groups(w):
            n = w.shape[1]
            return jnp.pad(w.reshape(yzs, grp, n), ((0, 0), (0, pad), (0, 0)))

        w1_loc = jnp.concatenate([wqkv_loc, wgate_loc, wup_loc], axis=1)
        w1_loc = pad_groups(w1_loc).reshape(yzs * gp, -1).T
        w2_loc = pad_groups(jnp.concatenate([wmo_loc, wao_loc], axis=0).T)

        x_t = x_loc.T.reshape(grp, xs, rows).transpose(1, 0, 2)
        gain_row = jnp.broadcast_to(jnp.pad(gain_loc, (0, rows - grp)).reshape(1, 1, rows), (xs, 1, rows))
        x_pad = jnp.concatenate([x_t, gain_row, jnp.zeros((xs, pad - 1, rows), bf16)], axis=1)
        c_q = wqkv_loc.shape[1]
        c_f = wgate_loc.shape[1]
        act, qkv_in, w2, x_own = front(x_pad, w1_loc, w2_loc, xs, yzs, grp, c_q, c_f)

        qkv_dev = qkv_in.transpose(1, 0, 2).reshape(dev_rows, yzs * c_q)
        q_heads = qkv_dev[:, :attn_cols].reshape(dev_rows, num_heads, head_dim)
        k_new = qkv_dev[:, attn_cols:attn_cols + head_dim]
        v_new = qkv_dev[:, attn_cols + head_dim:]
        q_rot = apply_rope(q_heads.astype(f32), len_loc[:, None]).astype(bf16)
        k_rot = apply_rope(k_new.astype(f32), len_loc).astype(bf16)
        new_slot = (jnp.arange(kc_loc.shape[1])[None, :] == len_loc[:, None])[:, :, None]
        k_all = jnp.where(new_slot, k_rot[:, None, :], kc_loc)
        v_all = jnp.where(new_slot, v_new[:, None, :], vc_loc)
        attn = attend_local(q_rot, k_all, v_all, len_loc).reshape(dev_rows, yzs, attn_cols // yzs).transpose(1, 0, 2)

        y_back = back(w2.reshape(yzs, xs * gp, -1), act, attn, x_own)
        y_loc = y_back[:, :grp].transpose(1, 0, 2).reshape(grp, n_rows).T
        return y_loc, k_all, v_all

    in_specs = (row_spec, P(both_axes), in_w_spec, in_w_spec, in_w_spec, out_w_spec, out_w_spec, cache_spec, cache_spec, len_spec)
    out_specs = (row_spec, cache_spec, cache_spec)
    return jax.shard_map(local_layer, mesh=mesh, in_specs=in_specs, out_specs=out_specs, check_vma=False)
```

```python
import functools

import jax
import jax.numpy as jnp
from jax import lax
from jax.experimental import pallas as pl
from jax.experimental.pallas import tpu as pltpu
from jax.sharding import PartitionSpec as P

MESH = pl.DeviceIdType.MESH
RING = 4
UP, FAR, DOWN = 1, 2, 3
VMEM_LIMIT = 62 * 1024 * 1024


def rope_tables(positions, head_dim):
    half_dim = head_dim // 2
    inv_freq = 10000.0 ** (-jnp.arange(half_dim, dtype=jnp.float32) / half_dim)
    angles = positions.astype(jnp.float32)[..., None] * inv_freq
    cos_t = jnp.cos(angles)
    sin_t = jnp.sin(angles)
    return jnp.concatenate([cos_t, cos_t], axis=-1), jnp.concatenate([-sin_t, sin_t], axis=-1)


class Where:
    def __init__(self, xs, yzs):
        self.xs = xs
        self.yzs = yzs
        self.dp = lax.axis_index("dp")
        self.x = lax.axis_index("x")
        self.j = lax.axis_index("yz")
        self.zz = self.j // RING
        self.yy = self.j % RING
        self.chip = self.x // 2
        self.core = self.x % 2

    def block(self, dz, dy):
        return ((self.zz + dz) % RING) * RING + (self.yy + dy) % RING

    def on_yz(self, j):
        return (self.dp, j, self.x)

    def on_x(self, x):
        return (self.dp, self.j, x)

    def axis_block(self, first, df, dg):
        return self.block(df, dg) if first == "z" else self.block(dg, df)

    def step(self, first, axis, d):
        return self.on_yz(self.axis_block(first, d, 0) if axis == 0 else self.axis_block(first, 0, d))

    def x_of(self, dc):
        return ((self.chip + dc) % RING) * 2 + self.core

    def x_other(self, dc):
        return ((self.chip + dc) % RING) * 2 + (1 - self.core)

    def greet(self):
        barrier = pltpu.get_barrier_semaphore()
        peers = [self.on_x((self.x + d) % self.xs) for d in range(1, self.xs)]
        peers += [self.on_yz((self.j + d) % self.yzs) for d in range(1, self.yzs)]
        for peer in peers:
            pl.semaphore_signal(barrier, inc=1, device_id=peer, device_id_type=MESH)
        pl.semaphore_wait(barrier, len(peers))


class Copies:
    def __init__(self, any_peer):
        self.any_peer = any_peer
        self.started = []

    def send(self, src, dst, ssem, rsem, peer):
        copy = pltpu.make_async_remote_copy(src_ref=src, dst_ref=dst, send_sem=ssem, recv_sem=rsem, device_id=peer, device_id_type=MESH)
        copy.start()
        self.started.append(copy)

    def arrived(self, dst, ssem, rsem):
        pltpu.make_async_remote_copy(
            src_ref=dst, dst_ref=dst, send_sem=ssem, recv_sem=rsem, device_id=self.any_peer, device_id_type=MESH
        ).wait_recv()

    def finish(self):
        for copy in self.started:
            copy.wait_send()


def front_kernel(
    xs, yzs, grp, c_q, c_f, num_heads, len_ref, x_ref, w1_ref, w2_ref, cos_ref, sin_ref, kc_ref, vc_ref,
    act_ref, w2g_ref, xo_ref, ko_ref, vo_ref,
    xg, h, gcol, w1, qkv_s, qkv_in, heads, k_s, v_s, ko_s, vo_s, o_send, ob,
    loc_sem, xsend, xrecv, gsend, grecv, wsend, wrecv, vsend, vrecv, qsend, qrecv, osend, orecv,
):
    f32, bf16 = jnp.float32, jnp.bfloat16
    at = Where(xs, yzs)
    half = xs // 2
    quarter = half // 2
    gp, rows = x_ref.shape[1:]
    dev_rows = rows // yzs
    kx = w1_ref.shape[1]
    read_k = pltpu.make_async_copy(kc_ref, k_s, loc_sem.at[4])
    read_k.start()
    read_v = pltpu.make_async_copy(vc_ref, v_s, loc_sem.at[5])
    read_v.start()
    at.greet()
    copies = Copies(at.on_yz(at.block(0, UP)))

    def send(src, dst, sems, idx, peer):
        copies.send(src, dst, sems[0].at[idx], sems[1].at[idx], peer)

    def arrived(region, sems, idx):
        copies.arrived(region, sems[0].at[idx], sems[1].at[idx])

    xsem, wsem, vsem, qsem = (xsend, xrecv), (wsend, wrecv), (vsend, vrecv), (qsend, qrecv)
    own_x = pltpu.make_async_copy(x_ref.at[at.x], xg.at[at.x, at.j], loc_sem.at[0])
    own_x.start()
    for d in range(1, xs):
        to = (at.x + d) % xs
        send(x_ref.at[to], xg.at[at.x, at.j], xsem, d - 1, at.on_x(to))

    n1 = w1_ref.shape[0]
    n2 = w2_ref.shape[0]

    def w1_at(x, k=None):
        cols = pl.ds(pl.multiple_of(x * kx, 128), kx)
        return w1.at[:, cols] if k is None else w1.at[pl.ds(k * (n1 // 2), n1 // 2), cols]

    def w2_at(x, k=None):
        return w2g_ref.at[:, x] if k is None else w2g_ref.at[pl.ds(k * (n2 // 2), n2 // 2), x]

    def spread_own(src, region, sems, loc):
        own = pltpu.make_async_copy(src, region(at.x), loc_sem.at[loc])
        own.start()
        send(src, region(at.x), sems, 0, at.on_x(at.x_of(UP)))
        send(src, region(at.x), sems, 1, at.on_x(at.x_of(DOWN)))
        send(src, region(at.x), sems, 2, at.on_x(at.x_other(0)))
        return own

    def pass_on(r, sems, slot, x):
        send(r, r, sems, slot, at.on_x(x))

    def forward_near(region, sems):
        arrived(region(at.x_of(DOWN)), sems, 0)
        pass_on(region(at.x_of(DOWN), 0), sems, 3, at.x_of(UP))
        arrived(region(at.x_of(UP)), sems, 1)
        pass_on(region(at.x_of(UP), 1), sems, 4, at.x_of(DOWN))
        pass_on(region(at.x_of(DOWN)), sems, 5, at.x_other(0))
        pass_on(region(at.x_of(UP)), sems, 6, at.x_other(0))

    def forward_far(region, sems):
        arrived(region(at.x_of(FAR), 0), sems, 3)
        pass_on(region(at.x_of(FAR), 0), sems, 7, at.x_other(0))
        arrived(region(at.x_of(FAR), 1), sems, 4)
        pass_on(region(at.x_of(FAR), 1), sems, 8, at.x_other(0))

    def all_in(region, sems, own):
        arrived(region(at.x_other(0)), sems, 2)
        arrived(region(at.x_other(DOWN)), sems, 5)
        arrived(region(at.x_other(UP)), sems, 6)
        arrived(region(at.x_other(FAR), 0), sems, 7)
        arrived(region(at.x_other(FAR), 1), sems, 8)
        own.wait()

    own_w1 = spread_own(w1_ref, w1_at, wsem, 1)
    own_x.wait()
    for d in range(1, xs):
        arrived(xg.at[(at.x + xs - d) % xs, at.j], xsem, d - 1)

    order = ("y", "z")
    halves = range(len(order))
    first_axis, second_axis = halves
    slot_up, slot_down, slot_far = RING, 2 * RING, 3 * RING

    def region(s, df, dg, lo=0, n=half):
        return xg.at[pl.ds(s * half + lo, n), at.axis_block(order[s], df, dg)]

    def pass_rows(s, df, dg, axis, d, slot, lo=0, n=half):
        r = region(s, df, dg, lo, n)
        send(r, r, (gsend.at[s], grecv.at[s]), slot, at.step(order[s], axis, d))

    def rows_in(s, df, dg, slot, lo=0, n=half):
        arrived(region(s, df, dg, lo, n), (gsend.at[s], grecv.at[s]), slot)

    def both_ways(s, df):
        pass_rows(s, df, 0, second_axis, UP, slot_up + df)
        pass_rows(s, df, 0, second_axis, DOWN, slot_down + df)

    for s in halves:
        pass_rows(s, 0, 0, first_axis, UP, 0)
        pass_rows(s, 0, 0, first_axis, DOWN, 1)
        both_ways(s, 0)
    xo_ref[:] = xg[:, at.j]
    for s in halves:
        rows_in(s, DOWN, 0, 0)
        pass_rows(s, DOWN, 0, first_axis, UP, FAR, 0, quarter)
        rows_in(s, UP, 0, 1)
        pass_rows(s, UP, 0, first_axis, DOWN, DOWN, quarter, quarter)
        both_ways(s, DOWN)
        both_ways(s, UP)
    for s in halves:
        rows_in(s, FAR, 0, FAR, 0, quarter)
        rows_in(s, FAR, 0, DOWN, quarter, quarter)
        both_ways(s, FAR)
    for s in halves:
        for df in (0, DOWN):
            rows_in(s, df, DOWN, slot_up + df)
            pass_rows(s, df, DOWN, second_axis, UP, slot_far + df)
    forward_near(w1_at, wsem)
    own_w2 = spread_own(w2_ref, w2_at, vsem, 2)
    for s in halves:
        for df in (UP, FAR):
            rows_in(s, df, UP, slot_down + df)
            pass_rows(s, df, UP, second_axis, DOWN, slot_far + df)
    for s in halves:
        for df in (UP, FAR):
            rows_in(s, df, DOWN, slot_up + df)
        for df in (0, DOWN):
            rows_in(s, df, UP, slot_down + df)
        for df in range(RING):
            rows_in(s, df, FAR, slot_far + df)

    pairs = yzs // 2
    feature = lax.broadcasted_iota(jnp.int32, (2, gp, 1), 1).reshape(2 * gp, 1)
    real = feature < grp
    diagonal = lax.broadcasted_iota(jnp.int32, (gp, 128), 0) == lax.broadcasted_iota(jnp.int32, (gp, 128), 1)

    def load(q):
        return xg[q // pairs, pl.ds((q % pairs) * 2, 2)].astype(f32).reshape(2 * gp, rows)

    def add_up(q, sums):
        raw = load(q)
        for k in range(2):
            row = raw[k * gp + grp:k * gp + grp + 1, :128]
            col = jnp.sum(jnp.where(diagonal, row, 0.0), axis=1, keepdims=True)
            gcol[q, pl.ds(k * gp, gp), :] = jnp.broadcast_to(col, (gp, 128))
        parts = jnp.where(real, raw, 0.0).reshape(2 * gp // 8, 8, rows)
        return sums[0] + jnp.sum(parts, axis=0), sums[1] + jnp.sum(parts * parts, axis=0)

    zero = jnp.zeros((8, rows), f32)
    s1, s2 = lax.fori_loop(0, xs * pairs, add_up, (zero, zero), unroll=4)
    forward_far(w1_at, wsem)
    d_model = grp * xs * yzs
    mean = jnp.sum(s1, axis=0, keepdims=True) / d_model
    var = jnp.sum(s2, axis=0, keepdims=True) / d_model - mean * mean
    scale = lax.rsqrt(var + 1e-6)

    def normalize(q, c):
        gain = jnp.concatenate([gcol[q]] * (rows // 128), axis=1)
        out = jnp.where(real, (load(q) - mean) * scale * gain, 0.0)
        h[pl.ds(pl.multiple_of(q * 2 * gp, 16), 2 * gp), :] = out.astype(bf16)
        return c

    lax.fori_loop(0, xs * pairs, normalize, 0, unroll=2)
    all_in(w1_at, wsem, own_w1)

    nt = 256

    def query(n, c):
        q = jnp.dot(w1[:c_q], h[:, pl.ds(pl.multiple_of(n * nt, nt), nt)], preferred_element_type=f32)
        qkv_s[pl.ds(pl.multiple_of(n * nt, nt), nt), :] = q.T.astype(bf16)
        return c

    lax.fori_loop(0, rows // nt, query, 0)
    def rows_of(ref, j):
        return ref.at[pl.ds(pl.multiple_of(j * dev_rows, dev_rows), dev_rows)]

    own_q = pltpu.make_async_copy(rows_of(qkv_s, at.j), qkv_in.at[at.j], loc_sem.at[3])
    own_q.start()
    for d in range(1, yzs):
        to = (at.j + d) % yzs
        send(rows_of(qkv_s, to), qkv_in.at[at.j], qsem, d - 1, at.on_yz(to))

    def mlp(n, c):
        cols = pl.ds(pl.multiple_of(n * nt, nt), nt)
        gate = jnp.dot(w1[c_q:c_q + c_f], h[:, cols], preferred_element_type=f32).astype(bf16).astype(f32)
        up = jnp.dot(w1[c_q + c_f:], h[:, cols], preferred_element_type=f32).astype(bf16).astype(f32)
        act_ref[pl.ds(0, c_f), cols] = (jax.nn.silu(gate) * up).astype(bf16)
        return c

    lax.fori_loop(0, rows // nt, mlp, 0)
    for d in range(1, yzs):
        arrived(qkv_in.at[(at.j + yzs - d) % yzs], qsem, d - 1)
    own_q.wait()
    forward_near(w2_at, vsem)

    head_dim = k_s.shape[2]
    per = 2 * c_q // head_dim
    for p in range(yzs // 2):
        both = jnp.concatenate([qkv_in[2 * p], qkv_in[2 * p + 1]], axis=1).astype(f32)
        for i in range(per):
            hd = p * per + i
            u = both[:, i * head_dim:(i + 1) * head_dim]
            if hd <= num_heads:
                u = u * cos_ref[:] + pltpu.roll(u, head_dim // 2, 1) * sin_ref[:]
                u = u.astype(bf16).astype(f32)
            heads[hd] = u
    read_k.wait()
    read_v.wait()

    group = 8
    t_len = k_s.shape[1]
    hp = heads.shape[0]
    position = lax.broadcasted_iota(jnp.int32, (t_len, head_dim), 0)
    along = lax.broadcasted_iota(jnp.int32, (hp, t_len), 1)

    def attend(g, c):
        first = pl.multiple_of(g * group, group)
        block = jnp.swapaxes(heads[:, pl.ds(first, group), :], 0, 1)
        scores, values = [], []
        for i in range(group):
            b = first + i
            last = len_ref[b]
            mine = block[i]
            slot = position == last
            kb, vb = [
                jnp.where(slot, mine[row:row + 1], old[b].astype(f32)).astype(bf16)
                for row, old in ((num_heads, k_s), (num_heads + 1, v_s))
            ]
            ko_s[b] = kb
            vo_s[b] = vb
            values.append(vb)
            score = lax.dot_general(mine.astype(bf16), kb, (((1,), (1,)), ((), ())), preferred_element_type=f32) * head_dim ** -0.5
            scores.append(jnp.where(along <= last, score, -1e30))
        scores = jnp.concatenate(scores, axis=0)
        e = jnp.exp(scores - jnp.max(scores, axis=1, keepdims=True))
        probs = (e / jnp.sum(e, axis=1, keepdims=True)).reshape(group, hp, t_len).astype(bf16)
        outs = [jnp.dot(probs[i], values[i], preferred_element_type=f32) for i in range(group)]
        heads[:, pl.ds(first, group), :] = jnp.swapaxes(jnp.stack(outs, axis=0), 0, 1)
        return c

    c_a = ob.shape[1]
    part = dev_rows // 2

    def rows_part(j, k):
        return ob.at[pl.ds(pl.multiple_of(j * dev_rows + k * part, part), part)]

    own_o = []
    for k in range(2):
        lax.fori_loop(k * part // group, (k + 1) * part // group, attend, 0)
        take = pl.ds(k * part, part)
        for jj in range(yzs):
            lo, hi = jj * c_a // head_dim, ((jj + 1) * c_a - 1) // head_dim + 1
            wide = jnp.concatenate([heads[hd, take, :] for hd in range(lo, hi)], axis=1)
            start = jj * c_a - lo * head_dim
            o_send[k, jj] = wide[:, start:start + c_a].astype(bf16)
        own = pltpu.make_async_copy(o_send.at[k, at.j], rows_part(at.j, k), loc_sem.at[6 + k])
        own.start()
        own_o.append(own)
        for d in range(1, yzs):
            to = (at.j + d) % yzs
            send(o_send.at[k, to], rows_part(at.j, k), (osend.at[k], orecv.at[k]), d - 1, at.on_yz(to))
    writes = []
    for out, ref, loc in ((ko_s, ko_ref, 4), (vo_s, vo_ref, 5)):
        write = pltpu.make_async_copy(out, ref, loc_sem.at[loc])
        write.start()
        writes.append(write)
    forward_far(w2_at, vsem)
    for k in range(2):
        for d in range(1, yzs):
            arrived(rows_part((at.j + yzs - d) % yzs, k), (osend.at[k], orecv.at[k]), d - 1)
        own_o[k].wait()
    act_ref[pl.ds(c_f, c_a), :] = ob[:].T
    all_in(w2_at, vsem, own_w2)
    for write in writes:
        write.wait()
    copies.finish()


def front(x_pad, w1_loc, w2_loc, tables, k_cache, v_cache, ctx_len, xs, yzs, grp, c_q, c_f):
    _, gp, rows = x_pad.shape
    n1, kx = w1_loc.shape
    n2 = w2_loc.shape[2]
    dev_rows, t_len, head_dim = k_cache.shape
    hp = yzs * c_q // head_dim
    num_heads = hp - 2
    c_a = n2 - c_f
    dma = pltpu.SemaphoreType.DMA
    f32, bf16 = jnp.float32, jnp.bfloat16
    vspec, aspec = pl.BlockSpec(memory_space=pltpu.VMEM), pl.BlockSpec(memory_space=pl.ANY)
    sems = lambda *s: [dma(s), dma(s)]
    cache = jax.ShapeDtypeStruct(k_cache.shape, bf16)
    return pl.pallas_call(
        functools.partial(front_kernel, xs, yzs, grp, c_q, c_f, num_heads),
        out_shape=(
            jax.ShapeDtypeStruct((n2, rows), bf16),
            jax.ShapeDtypeStruct((yzs, xs) + w2_loc.shape[1:], bf16),
            jax.ShapeDtypeStruct((xs, gp, rows), bf16),
            cache,
            cache,
        ),
        in_specs=[pl.BlockSpec(memory_space=pltpu.SMEM)] + [vspec] * 5 + [aspec] * 2,
        out_specs=(vspec, aspec, vspec, aspec, aspec),
        scratch_shapes=[
            pltpu.VMEM((xs, yzs, gp, rows), bf16),
            pltpu.VMEM((xs * yzs * gp, rows), bf16),
            pltpu.VMEM((xs * yzs // 2, 2 * gp, 128), f32),
            pltpu.VMEM((n1, xs * kx), bf16),
            pltpu.VMEM((rows, c_q), bf16),
            pltpu.VMEM((yzs, dev_rows, c_q), bf16),
            pltpu.VMEM((hp, dev_rows, head_dim), f32),
        ] + [pltpu.VMEM(k_cache.shape, bf16)] * 4 + [
            pltpu.VMEM((2, yzs, dev_rows // 2, c_a), bf16),
            pltpu.VMEM((rows, c_a), bf16),
            dma((8,)),
        ] + sems(xs - 1) + sems(2, RING * RING) + sems(9) + sems(9) + sems(yzs - 1) + sems(2, yzs - 1),
        compiler_params=pltpu.CompilerParams(collective_id=0, has_side_effects=True, vmem_limit_bytes=VMEM_LIMIT),
        name="front",
    )(ctx_len, x_pad, w1_loc, w2_loc, *tables, k_cache, v_cache)


def back_kernel(xs, yzs, w_ref, act, x_ref, y_ref, zb, r1, r2, r3, r4, yv, loc_sem, s1, q1, s2, q2, s3, q3, s4, q4, ys, yq):
    at = Where(xs, yzs)
    order = ("z", "y")
    hr = zb.shape[2] // 2
    gp = x_ref.shape[1]
    at.greet()
    copies = Copies(at.on_yz(at.block(0, UP)))
    send, arrived = copies.send, copies.arrived

    def zat(h, df, dg):
        dz, dy = (df, dg) if order[h] == "z" else (dg, df)
        return zb.at[dz, dy, pl.ds(h * hr, hr)]

    def compute(dz, dy):
        zb[dz, dy] = jnp.dot(w_ref[at.block(dz, dy)], act[:], preferred_element_type=jnp.float32)

    def send1(h, dg):
        d = 1 if dg < 2 else 3
        send(zat(h, 2, dg), r1.at[h, dg], s1.at[h, dg], q1.at[h, dg], at.step(order[h], 0, d))

    compute(2, 2)
    send1(0, 2)
    send1(1, 2)
    for k in (0, 1, 3):
        compute(2, k)
        send1(0, k)
        compute(k, 2)
        send1(1, k)

    def second(i, c):
        k, m = i // 3, i % 3
        compute(k + k // 2, m + m // 2)
        return c

    lax.fori_loop(0, 9, second, 0)

    def send2(h, up, dg):
        df, d, s = (1, 1, 0) if up else (3, 3, 1)
        send(zat(h, df, dg), r2.at[h, s, dg], s2.at[h, s, dg], q2.at[h, s, dg], at.step(order[h], 0, d))

    for h in range(2):
        for dg in (2, 3):
            send2(h, True, dg)
        for dg in (0, 1):
            send2(h, False, dg)
    for k in range(2):
        for h in range(2):
            for up in (True, False):
                dg = k if up else 2 + k
                arrived(r1.at[h, dg], s1.at[h, dg], q1.at[h, dg])
                ref = zat(h, 1 if up else 3, dg)
                ref[:] = ref[:] + r1[h, dg]
                send2(h, up, dg)

    def plane(h, dg):
        for s in range(2):
            arrived(r2.at[h, s, dg], s2.at[h, s, dg], q2.at[h, s, dg])
        ref = zat(h, 0, dg)
        ref[:] = ref[:] + r2[h, 0, dg] + r2[h, 1, dg]

    hh = hr // 2

    def part(h, dg, k):
        dz, dy = (0, dg) if order[h] == "z" else (dg, 0)
        return zb.at[dz, dy, pl.ds(h * hr + k * hh, hh)]

    def send4(h, up, k):
        dg, d, s = (1, 1, 0) if up else (3, 3, 1)
        send(part(h, dg, k), r4.at[h, s, k], s4.at[h, s, k], q4.at[h, s, k], at.step(order[h], 1, d))

    for h in range(2):
        plane(h, 2)
        send(part(h, 2, 0), r3.at[h, 0], s3.at[h, 0], q3.at[h, 0], at.step(order[h], 1, 1))
        send(part(h, 2, 1), r3.at[h, 1], s3.at[h, 1], q3.at[h, 1], at.step(order[h], 1, 3))
    for h in range(2):
        plane(h, 1)
        send4(h, True, 1)
        plane(h, 3)
        send4(h, False, 0)
    for h in range(2):
        plane(h, 0)
    for h in range(2):
        arrived(r3.at[h, 0], s3.at[h, 0], q3.at[h, 0])
        ref = part(h, 1, 0)
        ref[:] = ref[:] + r3[h, 0]
        send4(h, True, 0)
        arrived(r3.at[h, 1], s3.at[h, 1], q3.at[h, 1])
        ref = part(h, 3, 1)
        ref[:] = ref[:] + r3[h, 1]
        send4(h, False, 1)
    def y_copy(x, d):
        return pltpu.make_async_remote_copy(
            src_ref=yv.at[x], dst_ref=y_ref.at[at.x], send_sem=ys.at[d - 1], recv_sem=yq.at[d - 1], device_id=at.on_x(x), device_id_type=MESH
        )

    for h in range(2):
        for k in range(2):
            for s in range(2):
                arrived(r4.at[h, s, k], s4.at[h, s, k], q4.at[h, s, k])
            z = zb[0, 0, pl.ds(h * hr + k * hh, hh)] + r4[h, 0, k] + r4[h, 1, k]
            n = hh // gp
            for i in range(n):
                x = h * 2 * n + k * n + i
                yv[x] = (x_ref[x].astype(jnp.float32) + z[i * gp:(i + 1) * gp]).astype(jnp.bfloat16)
                d = lax.rem(x - at.x + xs, xs)

                @pl.when(d == 0)
                def _():
                    pltpu.make_async_copy(yv.at[x], y_ref.at[x], loc_sem.at[0]).start()

                @pl.when(d != 0)
                def _():
                    y_copy(x, d).start()

    for d in range(1, xs):
        arrived(y_ref.at[(at.x + xs - d) % xs], ys.at[d - 1], yq.at[d - 1])
    pltpu.make_async_copy(yv.at[at.x], y_ref.at[at.x], loc_sem.at[0]).wait()
    for d in range(1, xs):
        y_copy((at.x + d) % xs, d).wait_send()
    copies.finish()


def back(w2, act, x_own):
    _, block, _ = w2.shape
    yzs = w2.shape[0]
    xs, gp, rows = x_own.shape
    dma = pltpu.SemaphoreType.DMA
    bf16 = jnp.bfloat16
    vmem = lambda *s: pltpu.VMEM(s, jnp.float32)
    vspec, aspec = pl.BlockSpec(memory_space=pltpu.VMEM), pl.BlockSpec(memory_space=pl.ANY)
    sems = lambda *s: [dma(s), dma(s)]
    hr = block // 2
    return pl.pallas_call(
        functools.partial(back_kernel, xs, yzs),
        out_shape=jax.ShapeDtypeStruct((xs, gp, rows), bf16),
        in_specs=[vspec] * 3,
        out_specs=aspec,
        scratch_shapes=[
            vmem(RING, RING, block, rows),
            vmem(2, RING, hr, rows),
            vmem(2, 2, RING, hr, rows),
            vmem(2, 2, hr // 2, rows),
            vmem(2, 2, 2, hr // 2, rows),
            pltpu.VMEM((xs, gp, rows), bf16),
            dma((1,)),
        ] + sems(2, RING) + sems(2, 2, RING) + sems(2, 2) + sems(2, 2, 2) + sems(xs - 1),
        compiler_params=pltpu.CompilerParams(collective_id=1, has_side_effects=True, vmem_limit_bytes=VMEM_LIMIT),
        name="back",
    )(w2, act, x_own)


def solution(mesh):
    xs = mesh.shape["x"]
    yzs = mesh.shape["yz"]
    both_axes = ("x", "yz")
    row_spec = P("dp", both_axes)
    in_w_spec = P("x", "yz")
    out_w_spec = P("yz", "x")
    cache_spec = P(("dp", "x", "yz"), None, None)
    len_spec = P(("dp", "x", "yz"))

    def local_layer(x_loc, gain_loc, wqkv_loc, wgate_loc, wup_loc, wao_loc, wmo_loc, kc_loc, vc_loc, len_loc):
        n_rows, grp = x_loc.shape
        pad = -grp % 8
        gp = grp + pad
        rows = n_rows // xs
        bf16 = jnp.bfloat16

        def pad_groups(w):
            n = w.shape[1]
            return jnp.pad(w.reshape(yzs, grp, n), ((0, 0), (0, pad), (0, 0)))

        w1_loc = jnp.concatenate([wqkv_loc, wgate_loc, wup_loc], axis=1)
        w1_loc = pad_groups(w1_loc).reshape(yzs * gp, -1).T
        w2_loc = pad_groups(jnp.concatenate([wmo_loc, wao_loc], axis=0).T)

        x_t = x_loc.T.reshape(grp, xs, rows).transpose(1, 0, 2)
        gain_row = jnp.broadcast_to(jnp.pad(gain_loc, (0, rows - grp)).reshape(1, 1, rows), (xs, 1, rows))
        x_pad = jnp.concatenate([x_t, gain_row, jnp.zeros((xs, pad - 1, rows), bf16)], axis=1)
        c_q = wqkv_loc.shape[1]
        c_f = wgate_loc.shape[1]
        tables = rope_tables(len_loc, kc_loc.shape[2])
        act, w2, x_own, k_all, v_all = front(x_pad, w1_loc, w2_loc, tables, kc_loc, vc_loc, len_loc, xs, yzs, grp, c_q, c_f)
        y_back = back(w2.reshape(yzs, xs * gp, -1), act, x_own)
        y_loc = y_back[:, :grp].transpose(1, 0, 2).reshape(grp, n_rows).T
        return y_loc, k_all, v_all

    in_specs = (row_spec, P(both_axes), in_w_spec, in_w_spec, in_w_spec, out_w_spec, out_w_spec, cache_spec, cache_spec, len_spec)
    out_specs = (row_spec, cache_spec, cache_spec)
    return jax.shard_map(local_layer, mesh=mesh, in_specs=in_specs, out_specs=out_specs, check_vma=False)
```

```python
import functools

import jax
import jax.numpy as jnp
from jax import lax
from jax.experimental import pallas as pl
from jax.experimental.pallas import tpu as pltpu
from jax.sharding import PartitionSpec as P

MESH = pl.DeviceIdType.MESH
RING = 4
UP, FAR, DOWN = 1, 2, 3
VMEM_LIMIT = 62 * 1024 * 1024


def rope_tables(positions, head_dim):
    half_dim = head_dim // 2
    inv_freq = 10000.0 ** (-jnp.arange(half_dim, dtype=jnp.float32) / half_dim)
    angles = positions.astype(jnp.float32)[..., None] * inv_freq
    cos_t = jnp.cos(angles)
    sin_t = jnp.sin(angles)
    return jnp.concatenate([cos_t, cos_t], axis=-1), jnp.concatenate([-sin_t, sin_t], axis=-1)


class Where:
    def __init__(self, xs, yzs):
        self.xs = xs
        self.yzs = yzs
        self.dp = lax.axis_index("dp")
        self.x = lax.axis_index("x")
        self.j = lax.axis_index("yz")
        self.zz = self.j // RING
        self.yy = self.j % RING
        self.chip = self.x // 2
        self.core = self.x % 2

    def block(self, dz, dy):
        return ((self.zz + dz) % RING) * RING + (self.yy + dy) % RING

    def on_yz(self, j):
        return (self.dp, j, self.x)

    def on_x(self, x):
        return (self.dp, self.j, x)

    def axis_block(self, first, df, dg):
        return self.block(df, dg) if first == "z" else self.block(dg, df)

    def step(self, first, axis, d):
        return self.on_yz(self.axis_block(first, d, 0) if axis == 0 else self.axis_block(first, 0, d))

    def x_of(self, dc):
        return ((self.chip + dc) % RING) * 2 + self.core

    def x_other(self, dc):
        return ((self.chip + dc) % RING) * 2 + (1 - self.core)

    def greet(self):
        barrier = pltpu.get_barrier_semaphore()
        peers = [self.on_x((self.x + d) % self.xs) for d in range(1, self.xs)]
        peers += [self.on_yz((self.j + d) % self.yzs) for d in range(1, self.yzs)]
        for peer in peers:
            pl.semaphore_signal(barrier, inc=1, device_id=peer, device_id_type=MESH)
        pl.semaphore_wait(barrier, len(peers))


class Copies:
    def __init__(self, any_peer):
        self.any_peer = any_peer
        self.started = []

    def send(self, src, dst, ssem, rsem, peer):
        copy = pltpu.make_async_remote_copy(src_ref=src, dst_ref=dst, send_sem=ssem, recv_sem=rsem, device_id=peer, device_id_type=MESH)
        copy.start()
        self.started.append(copy)

    def arrived(self, dst, ssem, rsem):
        pltpu.make_async_remote_copy(
            src_ref=dst, dst_ref=dst, send_sem=ssem, recv_sem=rsem, device_id=self.any_peer, device_id_type=MESH
        ).wait_recv()

    def finish(self):
        for copy in self.started:
            copy.wait_send()


def layer_kernel(
    xs, yzs, grp, c_q, c_f, num_heads, len_ref, x_ref, w1_ref, w2_ref, cos_ref, sin_ref, kc_ref, vc_ref,
    y_ref, ko_ref, vo_ref,
    act, w2v, xo, k_s, v_s, o_send, ob,
    loc_sem, xsend, xrecv, gsend, grecv, wsend, wrecv, vsend, vrecv, qsend, qrecv, osend, orecv,
    s1, q1, s2, q2, s3, q3, s4, q4, ys, yq, ready,
):
    f32, bf16 = jnp.float32, jnp.bfloat16
    dma, vmem = pltpu.SemaphoreType.DMA, pltpu.VMEM
    gp, rows = x_ref.shape[1:]
    dev_rows, t_len, head_dim = k_s.shape
    n1, kx = w1_ref.shape
    c_a = ob.shape[1]
    part = dev_rows // 2
    block = xs * grp
    hr = block // 2
    at = Where(xs, yzs)
    any_peer = at.on_yz(at.block(0, UP))

    def w2_at(x, k=None):
        n2 = w2v.shape[0]
        return w2v.at[:, x] if k is None else w2v.at[pl.ds(k * (n2 // 2), n2 // 2), x]

    def o_rows(j, k):
        return ob.at[pl.ds(pl.multiple_of(j * dev_rows + k * part, part), part)]

    def o_copy(k, d):
        to = (at.j + d) % yzs
        return remote(o_send.at[k, to], o_rows(at.j, k), osend.at[k, d - 1], orecv.at[k, d - 1], at.on_yz(to))

    def o_own(k):
        return pltpu.make_async_copy(o_send.at[k, at.j], o_rows(at.j, k), loc_sem.at[6 + k])

    def cache_writes():
        return [pltpu.make_async_copy(src, dst, loc_sem.at[loc]) for src, dst, loc in ((k_s, ko_ref, 4), (v_s, vo_ref, 5))]

    gather_and_attend = functools.partial(
        first_phase, xs, yzs, grp, c_q, c_f, num_heads, at, any_peer, w2_at, o_copy, o_own, cache_writes,
        len_ref, x_ref, w1_ref, w2_ref, cos_ref, sin_ref, kc_ref, vc_ref, act, xo, k_s, v_s, o_send,
        loc_sem, (xsend, xrecv), (gsend, grecv), (wsend, wrecv), (vsend, vrecv), (qsend, qrecv),
    )
    pl.run_scoped(
        gather_and_attend,
        vmem((xs, yzs, gp, rows), bf16),
        vmem((xs * yzs * gp, rows), bf16),
        vmem((xs * yzs // 2, 2 * gp, 128), f32),
        vmem((n1, xs * kx), bf16),
        vmem((rows, c_q), bf16),
        vmem((yzs, dev_rows, c_q), bf16),
        vmem((num_heads + 2, dev_rows, head_dim), f32),
    )

    def finish_first():
        late = Copies(any_peer)
        forward_far(late, at, w2_at, (vsend, vrecv))
        for k in range(2):
            for d in range(1, yzs):
                late.arrived(o_rows((at.j + yzs - d) % yzs, k), osend.at[k, d - 1], orecv.at[k, d - 1])
            o_own(k).wait()
        act[pl.ds(c_f, c_a), :] = ob[:].T
        all_in(late, at, w2_at, (vsend, vrecv), pltpu.make_async_copy(w2_ref, w2_at(at.x), loc_sem.at[2]))
        return late

    def finish_last(late):
        for write in cache_writes():
            write.wait()
        for k in range(2):
            for d in range(1, yzs):
                o_copy(k, d).wait_send()
        for slot, k in enumerate((None, None, None, 0, 0, None, None)):
            remote(w2_at(at.x, k), w2_at(at.x, k), vsend.at[slot], vrecv.at[slot], any_peer).wait_send()
        late.finish()

    sum_and_return = functools.partial(
        second_phase, xs, yzs, grp, at, any_peer, finish_first, finish_last, w2v, act, xo, y_ref,
        loc_sem, (s1, q1), (s2, q2), (s3, q3), (s4, q4), (ys, yq), ready,
    )
    big = hr // 2 + hr // 2 % 8
    pl.run_scoped(
        sum_and_return,
        vmem((RING, RING, block, rows), f32),
        vmem((2, RING, hr, rows), f32),
        vmem((2, 2, RING, hr, rows), f32),
        vmem((2, 2, big, rows), f32),
        vmem((2, 2, 2, big, rows), f32),
        vmem((xs, gp, rows), bf16),
        vmem((block, w2v.shape[3]), f32),
    )


def remote(src, dst, ssem, rsem, peer):
    return pltpu.make_async_remote_copy(src_ref=src, dst_ref=dst, send_sem=ssem, recv_sem=rsem, device_id=peer, device_id_type=MESH)


def spread_own(copies, at, src, region, sems, loc_sem):
    own = pltpu.make_async_copy(src, region(at.x), loc_sem)
    own.start()
    for slot, to in enumerate((at.x_of(UP), at.x_of(DOWN), at.x_other(0))):
        copies.send(src, region(at.x), sems[0].at[slot], sems[1].at[slot], at.on_x(to))
    return own


def pass_on(copies, at, r, sems, slot, x):
    copies.send(r, r, sems[0].at[slot], sems[1].at[slot], at.on_x(x))


def block_in(copies, r, sems, slot):
    copies.arrived(r, sems[0].at[slot], sems[1].at[slot])


def forward_near(copies, at, region, sems):
    block_in(copies, region(at.x_of(DOWN)), sems, 0)
    pass_on(copies, at, region(at.x_of(DOWN), 0), sems, 3, at.x_of(UP))
    block_in(copies, region(at.x_of(UP)), sems, 1)
    pass_on(copies, at, region(at.x_of(UP), 1), sems, 4, at.x_of(DOWN))
    pass_on(copies, at, region(at.x_of(DOWN)), sems, 5, at.x_other(0))
    pass_on(copies, at, region(at.x_of(UP)), sems, 6, at.x_other(0))


def forward_far(copies, at, region, sems):
    for k in range(2):
        r = region(at.x_of(FAR), k)
        block_in(copies, r, sems, 3 + k)
        pass_on(copies, at, r, sems, 7 + k, at.x_other(0))


def all_in(copies, at, region, sems, own):
    block_in(copies, region(at.x_other(0)), sems, 2)
    block_in(copies, region(at.x_other(DOWN)), sems, 5)
    block_in(copies, region(at.x_other(UP)), sems, 6)
    for k in range(2):
        block_in(copies, region(at.x_other(FAR), k), sems, 7 + k)
    own.wait()


def first_phase(
    xs, yzs, grp, c_q, c_f, num_heads, at, any_peer, w2_at, o_copy, o_own, cache_writes,
    len_ref, x_ref, w1_ref, w2_ref, cos_ref, sin_ref, kc_ref, vc_ref, act, xo, k_s, v_s, o_send,
    loc_sem, xsem, gsem, wsem, vsem, qsem, xg, h, gcol, w1, qkv_s, qkv_in, heads,
):
    f32, bf16 = jnp.float32, jnp.bfloat16
    half = xs // 2
    quarter = half // 2
    gp, rows = x_ref.shape[1:]
    dev_rows = rows // yzs
    kx = w1_ref.shape[1]
    read_k = pltpu.make_async_copy(kc_ref, k_s, loc_sem.at[4])
    read_k.start()
    read_v = pltpu.make_async_copy(vc_ref, v_s, loc_sem.at[5])
    read_v.start()
    at.greet()
    copies, late = Copies(any_peer), Copies(any_peer)

    def send(src, dst, sems, idx, peer):
        copies.send(src, dst, sems[0].at[idx], sems[1].at[idx], peer)

    def arrived(region, sems, idx):
        copies.arrived(region, sems[0].at[idx], sems[1].at[idx])

    own_x = pltpu.make_async_copy(x_ref.at[at.x], xg.at[at.x, at.j], loc_sem.at[0])
    own_x.start()
    for d in range(1, xs):
        to = (at.x + d) % xs
        send(x_ref.at[to], xg.at[at.x, at.j], xsem, d - 1, at.on_x(to))

    n1 = w1_ref.shape[0]

    def w1_at(x, k=None):
        cols = pl.ds(pl.multiple_of(x * kx, 128), kx)
        return w1.at[:, cols] if k is None else w1.at[pl.ds(k * (n1 // 2), n1 // 2), cols]

    own_w1 = spread_own(copies, at, w1_ref, w1_at, wsem, loc_sem.at[1])
    own_x.wait()
    for d in range(1, xs):
        arrived(xg.at[(at.x + xs - d) % xs, at.j], xsem, d - 1)

    order = ("y", "z")
    halves = range(len(order))
    first_axis, second_axis = halves
    slot_up, slot_down, slot_far = RING, 2 * RING, 3 * RING

    def region(s, df, dg, lo=0, n=half):
        return xg.at[pl.ds(s * half + lo, n), at.axis_block(order[s], df, dg)]

    def pass_rows(s, df, dg, axis, d, slot, lo=0, n=half):
        r = region(s, df, dg, lo, n)
        send(r, r, (gsem[0].at[s], gsem[1].at[s]), slot, at.step(order[s], axis, d))

    def rows_in(s, df, dg, slot, lo=0, n=half):
        arrived(region(s, df, dg, lo, n), (gsem[0].at[s], gsem[1].at[s]), slot)

    def both_ways(s, df):
        pass_rows(s, df, 0, second_axis, UP, slot_up + df)
        pass_rows(s, df, 0, second_axis, DOWN, slot_down + df)

    for s in halves:
        pass_rows(s, 0, 0, first_axis, UP, 0)
        pass_rows(s, 0, 0, first_axis, DOWN, 1)
        both_ways(s, 0)
    xo[:] = xg[:, at.j]
    for s in halves:
        rows_in(s, DOWN, 0, 0)
        pass_rows(s, DOWN, 0, first_axis, UP, FAR, 0, quarter)
        rows_in(s, UP, 0, 1)
        pass_rows(s, UP, 0, first_axis, DOWN, DOWN, quarter, quarter)
        both_ways(s, DOWN)
        both_ways(s, UP)
    for s in halves:
        rows_in(s, FAR, 0, FAR, 0, quarter)
        rows_in(s, FAR, 0, DOWN, quarter, quarter)
        both_ways(s, FAR)
    for s in halves:
        for df in (0, DOWN):
            rows_in(s, df, DOWN, slot_up + df)
            pass_rows(s, df, DOWN, second_axis, UP, slot_far + df)
    forward_near(copies, at, w1_at, wsem)
    spread_own(late, at, w2_ref, w2_at, vsem, loc_sem.at[2])
    for s in halves:
        for df in (UP, FAR):
            rows_in(s, df, UP, slot_down + df)
            pass_rows(s, df, UP, second_axis, DOWN, slot_far + df)
    for s in halves:
        for df in (UP, FAR):
            rows_in(s, df, DOWN, slot_up + df)
        for df in (0, DOWN):
            rows_in(s, df, UP, slot_down + df)
        for df in range(RING):
            rows_in(s, df, FAR, slot_far + df)

    pairs = yzs // 2
    feature = lax.broadcasted_iota(jnp.int32, (2, gp, 1), 1).reshape(2 * gp, 1)
    real = feature < grp
    diagonal = lax.broadcasted_iota(jnp.int32, (gp, 128), 0) == lax.broadcasted_iota(jnp.int32, (gp, 128), 1)

    def load(q):
        return xg[q // pairs, pl.ds((q % pairs) * 2, 2)].astype(f32).reshape(2 * gp, rows)

    def add_up(q, sums):
        raw = load(q)
        for k in range(2):
            row = raw[k * gp + grp:k * gp + grp + 1, :128]
            col = jnp.sum(jnp.where(diagonal, row, 0.0), axis=1, keepdims=True)
            gcol[q, pl.ds(k * gp, gp), :] = jnp.broadcast_to(col, (gp, 128))
        parts = jnp.where(real, raw, 0.0).reshape(2 * gp // 8, 8, rows)
        return sums[0] + jnp.sum(parts, axis=0), sums[1] + jnp.sum(parts * parts, axis=0)

    zero = jnp.zeros((8, rows), f32)
    s1, s2 = lax.fori_loop(0, xs * pairs, add_up, (zero, zero), unroll=4)
    forward_far(copies, at, w1_at, wsem)
    d_model = grp * xs * yzs
    mean = jnp.sum(s1, axis=0, keepdims=True) / d_model
    var = jnp.sum(s2, axis=0, keepdims=True) / d_model - mean * mean
    scale = lax.rsqrt(var + 1e-6)

    def normalize(q, c):
        gain = jnp.concatenate([gcol[q]] * (rows // 128), axis=1)
        out = jnp.where(real, (load(q) - mean) * scale * gain, 0.0)
        h[pl.ds(pl.multiple_of(q * 2 * gp, 16), 2 * gp), :] = out.astype(bf16)
        return c

    lax.fori_loop(0, xs * pairs, normalize, 0, unroll=2)
    all_in(copies, at, w1_at, wsem, own_w1)

    nt = 256

    def query(n, c):
        q = jnp.dot(w1[:c_q], h[:, pl.ds(pl.multiple_of(n * nt, nt), nt)], preferred_element_type=f32)
        qkv_s[pl.ds(pl.multiple_of(n * nt, nt), nt), :] = q.T.astype(bf16)
        return c

    lax.fori_loop(0, rows // nt, query, 0)
    def rows_of(ref, j):
        return ref.at[pl.ds(pl.multiple_of(j * dev_rows, dev_rows), dev_rows)]

    own_q = pltpu.make_async_copy(rows_of(qkv_s, at.j), qkv_in.at[at.j], loc_sem.at[3])
    own_q.start()
    for d in range(1, yzs):
        to = (at.j + d) % yzs
        send(rows_of(qkv_s, to), qkv_in.at[at.j], qsem, d - 1, at.on_yz(to))

    def mlp(n, c):
        cols = pl.ds(pl.multiple_of(n * nt, nt), nt)
        gate = jnp.dot(w1[c_q:c_q + c_f], h[:, cols], preferred_element_type=f32).astype(bf16).astype(f32)
        up = jnp.dot(w1[c_q + c_f:], h[:, cols], preferred_element_type=f32).astype(bf16).astype(f32)
        act[pl.ds(0, c_f), cols] = (jax.nn.silu(gate) * up).astype(bf16)
        return c

    lax.fori_loop(0, rows // nt, mlp, 0)
    for d in range(1, yzs):
        arrived(qkv_in.at[(at.j + yzs - d) % yzs], qsem, d - 1)
    own_q.wait()
    forward_near(late, at, w2_at, vsem)

    head_dim = k_s.shape[2]
    per = 2 * c_q // head_dim
    for p in range(yzs // 2):
        both = jnp.concatenate([qkv_in[2 * p], qkv_in[2 * p + 1]], axis=1).astype(f32)
        for i in range(per):
            hd = p * per + i
            u = both[:, i * head_dim:(i + 1) * head_dim]
            if hd <= num_heads:
                u = u * cos_ref[:] + pltpu.roll(u, head_dim // 2, 1) * sin_ref[:]
                u = u.astype(bf16).astype(f32)
            heads[hd] = u
    read_k.wait()
    read_v.wait()

    group = 8
    t_len = k_s.shape[1]
    hp = heads.shape[0]
    position = lax.broadcasted_iota(jnp.int32, (t_len, head_dim), 0)
    along = lax.broadcasted_iota(jnp.int32, (hp, t_len), 1)

    def attend(g, c):
        first = pl.multiple_of(g * group, group)
        block = jnp.swapaxes(heads[:, pl.ds(first, group), :], 0, 1)
        scores, keys, values = [], [], []
        for i in range(group):
            b = first + i
            last = len_ref[b]
            mine = block[i]
            slot = position == last
            kb, vb = [
                jnp.where(slot, mine[row:row + 1], old[b].astype(f32)).astype(bf16)
                for row, old in ((num_heads, k_s), (num_heads + 1, v_s))
            ]
            keys.append(kb)
            values.append(vb)
            score = lax.dot_general(mine.astype(bf16), kb, (((1,), (1,)), ((), ())), preferred_element_type=f32) * head_dim ** -0.5
            scores.append(jnp.where(along <= last, score, -1e30))
        for i in range(group):
            k_s[first + i] = keys[i]
            v_s[first + i] = values[i]
        scores = jnp.concatenate(scores, axis=0)
        e = jnp.exp(scores - jnp.max(scores, axis=1, keepdims=True))
        probs = (e / jnp.sum(e, axis=1, keepdims=True)).reshape(group, hp, t_len).astype(bf16)
        outs = [jnp.dot(probs[i], values[i], preferred_element_type=f32) for i in range(group)]
        heads[:, pl.ds(first, group), :] = jnp.swapaxes(jnp.stack(outs, axis=0), 0, 1)
        return c

    c_a = o_send.shape[3]
    part = dev_rows // 2
    for k in range(2):
        lax.fori_loop(k * part // group, (k + 1) * part // group, attend, 0)
        take = pl.ds(k * part, part)
        for jj in range(yzs):
            lo, hi = jj * c_a // head_dim, ((jj + 1) * c_a - 1) // head_dim + 1
            wide = jnp.concatenate([heads[hd, take, :] for hd in range(lo, hi)], axis=1)
            start = jj * c_a - lo * head_dim
            o_send[k, jj] = wide[:, start:start + c_a].astype(bf16)
        o_own(k).start()
        for d in range(1, yzs):
            o_copy(k, d).start()
    for write in cache_writes():
        write.start()
    copies.finish()


def second_phase(
    xs, yzs, grp, at, any_peer, finish_first, finish_last, w2v, act, xo, y_ref,
    loc_sem, sem1, sem2, sem3, sem4, ysem, ready, zb, r1, r2, r3, r4, yv, ws,
):
    for d in (UP, DOWN):
        for peer in (at.block(d, 0), at.block(0, d)):
            pl.semaphore_signal(ready, inc=1, device_id=at.on_yz(peer), device_id_type=MESH)
    yv[:] = jnp.zeros_like(yv)
    late = finish_first()
    (s1, q1), (s2, q2), (s3, q3), (s4, q4), (ys, yq) = sem1, sem2, sem3, sem4, ysem
    order = ("z", "y")
    hr = zb.shape[2] // 2
    copies = Copies(any_peer)
    send, arrived = copies.send, copies.arrived

    def zat(h, df, dg):
        dz, dy = (df, dg) if order[h] == "z" else (dg, df)
        return zb.at[dz, dy, pl.ds(h * hr, hr)]

    def compute(dz, dy):
        w = w2v[at.block(dz, dy)].astype(jnp.float32)
        for x in range(xs):
            ws[pl.ds(x * grp, grp), :] = w[x, :grp]
        zb[dz, dy] = jnp.dot(ws[:].astype(jnp.bfloat16), act[:], preferred_element_type=jnp.float32)

    def send1(h, dg):
        d = 1 if dg < 2 else 3
        send(zat(h, 2, dg), r1.at[h, dg], s1.at[h, dg], q1.at[h, dg], at.step(order[h], 0, d))

    compute(2, 2)
    pl.semaphore_wait(ready, RING)
    send1(0, 2)
    send1(1, 2)
    for k in (0, 1, 3):
        compute(2, k)
        send1(0, k)
        compute(k, 2)
        send1(1, k)

    def second(i, c):
        k, m = i // 3, i % 3
        compute(k + k // 2, m + m // 2)
        return c

    lax.fori_loop(0, 9, second, 0)

    def send2(h, up, dg):
        df, d, s = (1, 1, 0) if up else (3, 3, 1)
        send(zat(h, df, dg), r2.at[h, s, dg], s2.at[h, s, dg], q2.at[h, s, dg], at.step(order[h], 0, d))

    for h in range(2):
        for dg in (2, 3):
            send2(h, True, dg)
        for dg in (0, 1):
            send2(h, False, dg)
    for k in range(2):
        for h in range(2):
            for up in (True, False):
                dg = k if up else 2 + k
                arrived(r1.at[h, dg], s1.at[h, dg], q1.at[h, dg])
                ref = zat(h, 1 if up else 3, dg)
                ref[:] = ref[:] + r1[h, dg]
                send2(h, up, dg)

    def plane(h, dg):
        for s in range(2):
            arrived(r2.at[h, s, dg], s2.at[h, s, dg], q2.at[h, s, dg])
        ref = zat(h, 0, dg)
        ref[:] = ref[:] + r2[h, 0, dg] + r2[h, 1, dg]

    big = r3.shape[2]
    sizes = (big, hr - big)

    def part(h, dg, k):
        dz, dy = (0, dg) if order[h] == "z" else (dg, 0)
        return zb.at[dz, dy, pl.ds(h * hr + k * big, sizes[k])]

    def r3_at(h, k):
        return r3.at[h, k, pl.ds(0, sizes[k])]

    def r4_at(h, s, k):
        return r4.at[h, s, k, pl.ds(0, sizes[k])]

    def send4(h, up, k):
        dg, d, s = (1, 1, 0) if up else (3, 3, 1)
        send(part(h, dg, k), r4_at(h, s, k), s4.at[h, s, k], q4.at[h, s, k], at.step(order[h], 1, d))

    for h in range(2):
        plane(h, 2)
        send(part(h, 2, 0), r3_at(h, 0), s3.at[h, 0], q3.at[h, 0], at.step(order[h], 1, 1))
        send(part(h, 2, 1), r3_at(h, 1), s3.at[h, 1], q3.at[h, 1], at.step(order[h], 1, 3))
    for h in range(2):
        plane(h, 1)
        send4(h, True, 1)
        plane(h, 3)
        send4(h, False, 0)
    for h in range(2):
        plane(h, 0)
    for h in range(2):
        arrived(r3_at(h, 0), s3.at[h, 0], q3.at[h, 0])
        ref = part(h, 1, 0)
        ref[:] = ref[:] + r3_at(h, 0)[:]
        send4(h, True, 0)
        arrived(r3_at(h, 1), s3.at[h, 1], q3.at[h, 1])
        ref = part(h, 3, 1)
        ref[:] = ref[:] + r3_at(h, 1)[:]
        send4(h, False, 1)
    def y_copy(x, d):
        return pltpu.make_async_remote_copy(
            src_ref=yv.at[x], dst_ref=y_ref.at[at.x], send_sem=ys.at[d - 1], recv_sem=yq.at[d - 1], device_id=at.on_x(x), device_id_type=MESH
        )

    for h in range(2):
        for k in range(2):
            for s in range(2):
                arrived(r4_at(h, s, k), s4.at[h, s, k], q4.at[h, s, k])
            ref = part(h, 0, k)
            ref[:] = ref[:] + r4_at(h, 0, k)[:] + r4_at(h, 1, k)[:]
            done = xs // 4
            for x in range((2 * h + k) * done, (2 * h + k + 1) * done):
                z = zb[0, 0, pl.ds(x * grp, grp), :]
                yv[x, :grp, :] = (xo[x, :grp, :].astype(jnp.float32) + z).astype(jnp.bfloat16)
                d = lax.rem(x - at.x + xs, xs)

                @pl.when(d == 0)
                def _():
                    pltpu.make_async_copy(yv.at[x], y_ref.at[x], loc_sem.at[3]).start()

                @pl.when(d != 0)
                def _():
                    y_copy(x, d).start()

    for d in range(1, xs):
        arrived(y_ref.at[(at.x + xs - d) % xs], ys.at[d - 1], yq.at[d - 1])
    pltpu.make_async_copy(yv.at[at.x], y_ref.at[at.x], loc_sem.at[3]).wait()
    for d in range(1, xs):
        y_copy((at.x + d) % xs, d).wait_send()
    copies.finish()
    finish_last(late)


def layer(x_pad, w1_loc, w2_loc, tables, k_cache, v_cache, ctx_len, xs, yzs, grp, c_q, c_f):
    _, gp, rows = x_pad.shape
    n2 = w2_loc.shape[2]
    dev_rows, t_len, head_dim = k_cache.shape
    num_heads = yzs * c_q // head_dim - 2
    c_a = n2 - c_f
    dma, vmem = pltpu.SemaphoreType.DMA, pltpu.VMEM
    bf16 = jnp.bfloat16
    vspec, aspec = pl.BlockSpec(memory_space=vmem), pl.BlockSpec(memory_space=pl.ANY)
    sems = lambda *shape: [dma(shape), dma(shape)]
    cache = jax.ShapeDtypeStruct(k_cache.shape, bf16)
    return pl.pallas_call(
        functools.partial(layer_kernel, xs, yzs, grp, c_q, c_f, num_heads),
        out_shape=(jax.ShapeDtypeStruct((xs, gp, rows), bf16), cache, cache),
        in_specs=[pl.BlockSpec(memory_space=pltpu.SMEM)] + [vspec] * 5 + [aspec] * 2,
        out_specs=(aspec, aspec, aspec),
        scratch_shapes=[
            vmem((n2, rows), bf16),
            vmem((yzs, xs) + w2_loc.shape[1:], bf16),
            vmem((xs, gp, rows), bf16),
            vmem(k_cache.shape, bf16),
            vmem(k_cache.shape, bf16),
            vmem((2, yzs, dev_rows // 2, c_a), bf16),
            vmem((rows, c_a), bf16),
            dma((8,)),
        ]
        + sems(xs - 1) + sems(2, RING * RING) + sems(9) + sems(9) + sems(yzs - 1) + sems(2, yzs - 1)
        + sems(2, RING) + sems(2, 2, RING) + sems(2, 2) + sems(2, 2, 2) + sems(xs - 1)
        + [pltpu.SemaphoreType.REGULAR],
        compiler_params=pltpu.CompilerParams(collective_id=0, has_side_effects=True, vmem_limit_bytes=VMEM_LIMIT),
        name="layer",
    )(ctx_len, x_pad, w1_loc, w2_loc, *tables, k_cache, v_cache)


def solution(mesh):
    xs = mesh.shape["x"]
    yzs = mesh.shape["yz"]
    both_axes = ("x", "yz")
    row_spec = P("dp", both_axes)
    in_w_spec = P("x", "yz")
    out_w_spec = P("yz", "x")
    cache_spec = P(("dp", "x", "yz"), None, None)
    len_spec = P(("dp", "x", "yz"))

    def local_layer(x_loc, gain_loc, wqkv_loc, wgate_loc, wup_loc, wao_loc, wmo_loc, kc_loc, vc_loc, len_loc):
        n_rows, grp = x_loc.shape
        pad = -grp % 8
        gp = grp + pad
        rows = n_rows // xs
        bf16 = jnp.bfloat16

        def pad_groups(w):
            n = w.shape[1]
            return jnp.pad(w.reshape(yzs, grp, n), ((0, 0), (0, pad), (0, 0)))

        w1_loc = jnp.concatenate([wqkv_loc, wgate_loc, wup_loc], axis=1)
        w1_loc = pad_groups(w1_loc).reshape(yzs * gp, -1).T
        w2_loc = pad_groups(jnp.concatenate([wmo_loc, wao_loc], axis=0).T)

        x_t = x_loc.T.reshape(grp, xs, rows).transpose(1, 0, 2)
        gain_row = jnp.broadcast_to(jnp.pad(gain_loc, (0, rows - grp)).reshape(1, 1, rows), (xs, 1, rows))
        x_pad = jnp.concatenate([x_t, gain_row, jnp.zeros((xs, pad - 1, rows), bf16)], axis=1)
        c_q = wqkv_loc.shape[1]
        c_f = wgate_loc.shape[1]
        tables = rope_tables(len_loc, kc_loc.shape[2])
        y_back, k_all, v_all = layer(x_pad, w1_loc, w2_loc, tables, kc_loc, vc_loc, len_loc, xs, yzs, grp, c_q, c_f)
        y_loc = y_back[:, :grp].transpose(1, 0, 2).reshape(grp, n_rows).T
        return y_loc, k_all, v_all

    in_specs = (row_spec, P(both_axes), in_w_spec, in_w_spec, in_w_spec, out_w_spec, out_w_spec, cache_spec, cache_spec, len_spec)
    out_specs = (row_spec, cache_spec, cache_spec)
    return jax.shard_map(local_layer, mesh=mesh, in_specs=in_specs, out_specs=out_specs, check_vma=False)
```

```python
import functools

import jax
import jax.numpy as jnp
from jax import lax
from jax.experimental import pallas as pl
from jax.experimental.pallas import tpu as pltpu
from jax.sharding import PartitionSpec as P

MESH = pl.DeviceIdType.MESH
RING = 4
UP, FAR, DOWN = 1, 2, 3
VMEM_LIMIT = 62 * 1024 * 1024


def rope_tables(positions, head_dim):
    half_dim = head_dim // 2
    inv_freq = 10000.0 ** (-jnp.arange(half_dim, dtype=jnp.float32) / half_dim)
    angles = positions.astype(jnp.float32)[..., None] * inv_freq
    cos_t = jnp.cos(angles)
    sin_t = jnp.sin(angles)
    return jnp.concatenate([cos_t, cos_t], axis=-1), jnp.concatenate([-sin_t, sin_t], axis=-1)


class Where:
    def __init__(self, xs, yzs):
        self.xs = xs
        self.yzs = yzs
        self.dp = lax.axis_index("dp")
        self.x = lax.axis_index("x")
        self.j = lax.axis_index("yz")
        self.zz = self.j // RING
        self.yy = self.j % RING
        self.chip = self.x // 2
        self.core = self.x % 2

    def block(self, dz, dy):
        return ((self.zz + dz) % RING) * RING + (self.yy + dy) % RING

    def on_yz(self, j):
        return (self.dp, j, self.x)

    def on_x(self, x):
        return (self.dp, self.j, x)

    def axis_block(self, first, df, dg):
        return self.block(df, dg) if first == "z" else self.block(dg, df)

    def step(self, first, axis, d):
        return self.on_yz(self.axis_block(first, d, 0) if axis == 0 else self.axis_block(first, 0, d))

    def x_of(self, dc):
        return ((self.chip + dc) % RING) * 2 + self.core

    def x_other(self, dc):
        return ((self.chip + dc) % RING) * 2 + (1 - self.core)

    def peers(self):
        on_x = [self.on_x((self.x + d) % self.xs) for d in range(1, self.xs)]
        return on_x + [self.on_yz((self.j + d) % self.yzs) for d in range(1, self.yzs)]

    def greet(self):
        for peer in self.peers():
            pl.semaphore_signal(pltpu.get_barrier_semaphore(), inc=1, device_id=peer, device_id_type=MESH)

    def greeted(self):
        pl.semaphore_wait(pltpu.get_barrier_semaphore(), len(self.peers()))


class Copies:
    def __init__(self, any_peer):
        self.any_peer = any_peer
        self.started = []

    def send(self, src, dst, ssem, rsem, peer):
        copy = pltpu.make_async_remote_copy(src_ref=src, dst_ref=dst, send_sem=ssem, recv_sem=rsem, device_id=peer, device_id_type=MESH)
        copy.start()
        self.started.append(copy)

    def arrived(self, dst, ssem, rsem):
        pltpu.make_async_remote_copy(
            src_ref=dst, dst_ref=dst, send_sem=ssem, recv_sem=rsem, device_id=self.any_peer, device_id_type=MESH
        ).wait_recv()

    def finish(self):
        for copy in self.started:
            copy.wait_send()


def layer_kernel(
    xs, yzs, gp, len_ref, x_ref, gain_ref, wq_ref, wg_ref, wu_ref, wa_ref, wm_ref, cos_ref, sin_ref, kc_ref, vc_ref,
    y_ref, ko_ref, vo_ref,
    act, w2v, xo, k_s, v_s, o_send, ob,
    loc_sem, xsend, xrecv, gsend, grecv, wsend, wrecv, vsend, vrecv, qsend, qrecv, osend, orecv,
    s1, q1, s2, q2, s3, q3, s4, q4, ys, yq, ready,
):
    f32, bf16 = jnp.float32, jnp.bfloat16
    dma, vmem = pltpu.SemaphoreType.DMA, pltpu.VMEM
    grp = x_ref.shape[0]
    rows, c_a = ob.shape
    dev_rows, t_len, head_dim = k_s.shape
    c_q, k_loc = wq_ref.shape
    n1 = c_q + 2 * wg_ref.shape[1]
    c_f = wm_ref.shape[0]
    num_heads = yzs * c_a // head_dim
    part = dev_rows // 2
    block = xs * grp
    hr = block // 2
    at = Where(xs, yzs)
    any_peer = at.on_yz(at.block(0, UP))

    def w2_at(x, k=None):
        n2 = w2v.shape[0]
        return w2v.at[:, x] if k is None else w2v.at[pl.ds(k * (n2 // 2), n2 // 2), x]

    def o_rows(j, k):
        return ob.at[pl.ds(pl.multiple_of(j * dev_rows + k * part, part), part)]

    def o_copy(k, d):
        to = (at.j + d) % yzs
        return remote(o_send.at[k, to], o_rows(at.j, k), osend.at[k, d - 1], orecv.at[k, d - 1], at.on_yz(to))

    def o_own(k):
        return pltpu.make_async_copy(o_send.at[k, at.j], o_rows(at.j, k), loc_sem.at[6 + k])

    def cache_writes():
        return [pltpu.make_async_copy(src, dst, loc_sem.at[loc]) for src, dst, loc in ((k_s, ko_ref, 4), (v_s, vo_ref, 5))]

    gather_and_attend = functools.partial(
        first_phase, xs, yzs, num_heads, at, any_peer, w2_at, o_copy, o_own, cache_writes,
        len_ref, x_ref, gain_ref, wq_ref, wg_ref, wu_ref, wa_ref, wm_ref, cos_ref, sin_ref, kc_ref, vc_ref,
        act, w2v, xo, k_s, v_s, o_send,
        loc_sem, (xsend, xrecv), (gsend, grecv), (wsend, wrecv), (vsend, vrecv), (qsend, qrecv),
    )
    pl.run_scoped(
        gather_and_attend,
        vmem((xs, yzs, gp, rows), bf16),
        vmem((xs * yzs * gp, rows), bf16),
        vmem((xs * yzs // 2, 2 * gp, 128), f32),
        vmem((n1, xs * yzs * gp), bf16),
        vmem((rows, c_q), bf16),
        vmem((yzs, dev_rows, c_q), bf16),
        vmem((num_heads + 2, dev_rows, head_dim), f32),
        vmem((xs, gp, rows), bf16),
        vmem((gp, rows), f32),
        vmem((k_loc + 8, c_f + c_a), f32),
        vmem((yzs * gp, c_f), f32),
        vmem((c_f + c_a, k_loc), f32),
    )

    def finish_first():
        late = Copies(any_peer)
        share_far(late, at, w2_at, (vsend, vrecv))
        for k in range(2):
            for d in range(1, yzs):
                late.arrived(o_rows((at.j + yzs - d) % yzs, k), osend.at[k, d - 1], orecv.at[k, d - 1])
            o_own(k).wait()
        act[pl.ds(c_f, c_a), :] = ob[:].T
        all_in(late, at, w2_at, (vsend, vrecv))
        return late

    def finish_last(late):
        for write in cache_writes():
            write.wait()
        for k in range(2):
            for d in range(1, yzs):
                o_copy(k, d).wait_send()
        for slot in range(9):
            r = w2_at(at.x, None if slot in (4, 7, 8) else 0)
            remote(r, r, vsend.at[slot], vrecv.at[slot], any_peer).wait_send()
        late.finish()

    sum_and_return = functools.partial(
        second_phase, xs, yzs, grp, at, any_peer, finish_first, finish_last, w2v, act, xo, y_ref,
        loc_sem, (s1, q1), (s2, q2), (s3, q3), (s4, q4), (ys, yq), ready,
    )
    big = hr // 2 + hr // 2 % 8
    pl.run_scoped(
        sum_and_return,
        vmem((RING, RING, block, rows), f32),
        vmem((2, RING, hr, rows), f32),
        vmem((2, 2, RING, hr, rows), f32),
        vmem((2, 2, big, rows), f32),
        vmem((2, 2, 2, big, rows), f32),
        vmem((xs, gp, rows), bf16),
        vmem((block, w2v.shape[3]), f32),
    )


def remote(src, dst, ssem, rsem, peer):
    return pltpu.make_async_remote_copy(src_ref=src, dst_ref=dst, send_sem=ssem, recv_sem=rsem, device_id=peer, device_id_type=MESH)


def spread_own(copies, at, region, sems):
    def send(slot, k, x):
        r = region(at.x, k)
        copies.send(r, r, sems[0].at[slot], sems[1].at[slot], at.on_x(x))

    for k in range(2):
        send(2 * k, k, at.x_of(UP))
        send(2 * k + 1, 1 - k, at.x_of(DOWN))
    send(4, None, at.x_other(0))


def pass_on(copies, at, r, sems, slot, x):
    copies.send(r, r, sems[0].at[slot], sems[1].at[slot], at.on_x(x))


def block_in(copies, r, sems, slot):
    copies.arrived(r, sems[0].at[slot], sems[1].at[slot])


def forward_half(copies, at, region, sems):
    for slot, k, here, to in ((0, 0, DOWN, UP), (1, 1, UP, DOWN)):
        r = region(at.x_of(here), k)
        block_in(copies, r, sems, slot)
        pass_on(copies, at, r, sems, slot + 5, at.x_of(to))


def share_near(copies, at, region, sems):
    for slot, k, here in ((2, 1, DOWN), (3, 0, UP)):
        block_in(copies, region(at.x_of(here), k), sems, slot)
        pass_on(copies, at, region(at.x_of(here)), sems, slot + 5, at.x_other(0))


def share_far(copies, at, region, sems):
    for k in range(2):
        r = region(at.x_of(FAR), k)
        block_in(copies, r, sems, 5 + k)
        pass_on(copies, at, r, sems, 9 + k, at.x_other(0))


def all_in(copies, at, region, sems):
    for slot, here in ((4, 0), (7, DOWN), (8, UP)):
        block_in(copies, region(at.x_other(here)), sems, slot)
    for k in range(2):
        block_in(copies, region(at.x_other(FAR), k), sems, 9 + k)


def first_phase(
    xs, yzs, num_heads, at, any_peer, w2_at, o_copy, o_own, cache_writes,
    len_ref, x_ref, gain_ref, wq_ref, wg_ref, wu_ref, wa_ref, wm_ref, cos_ref, sin_ref, kc_ref, vc_ref,
    act, w2v, xo, k_s, v_s, o_send,
    loc_sem, xsem, gsem, wsem, vsem, qsem, xg, h, gcol, w1, qkv_s, qkv_in, heads, x_send, stage, tall, wide_s, narrow,
):
    f32, bf16 = jnp.float32, jnp.bfloat16
    half = xs // 2
    quarter = half // 2
    grp = x_ref.shape[0]
    _, gp, rows = x_send.shape
    dev_rows = rows // yzs
    c_q, k_loc = wq_ref.shape
    c_f, c_a = wm_ref.shape[0], wa_ref.shape[0]
    kx = yzs * gp
    at.greet()
    read_k = pltpu.make_async_copy(kc_ref, k_s, loc_sem.at[4])
    read_k.start()
    read_v = pltpu.make_async_copy(vc_ref, v_s, loc_sem.at[5])
    read_v.start()
    stage[:] = jnp.zeros_like(stage)
    stage[grp:grp + 1, :grp] = gain_ref[:].astype(f32)
    for x in range(xs):
        stage[:grp, :] = x_ref[:, x * rows:(x + 1) * rows].astype(f32)
        x_send[x] = stage[:].astype(bf16)
    at.greeted()
    copies, late = Copies(any_peer), Copies(any_peer)

    def send(src, dst, sems, idx, peer):
        copies.send(src, dst, sems[0].at[idx], sems[1].at[idx], peer)

    def arrived(region, sems, idx):
        copies.arrived(region, sems[0].at[idx], sems[1].at[idx])

    own_x = pltpu.make_async_copy(x_send.at[at.x], xg.at[at.x, at.j], loc_sem.at[0])
    own_x.start()
    for d in range(1, xs):
        to = (at.x + d) % xs
        send(x_send.at[to], xg.at[at.x, at.j], xsem, d - 1, at.on_x(to))

    n1 = w1.shape[0]

    def w1_at(x, k=None):
        cols = pl.ds(pl.multiple_of(x * kx, 128), kx)
        return w1.at[:, cols] if k is None else w1.at[pl.ds(k * (n1 // 2), n1 // 2), cols]

    own_cols = pl.ds(pl.multiple_of(at.x * kx, 128), kx)
    tall[k_loc:, :] = jnp.zeros((tall.shape[0] - k_loc, tall.shape[1]), f32)
    row = 0
    for ref in (wq_ref, wg_ref, wu_ref):
        w = ref[:].astype(f32)
        w = w.T if ref is wq_ref else w
        n = w.shape[1]
        tall[:k_loc, :n] = w
        for j in range(yzs):
            wide_s[j * gp:(j + 1) * gp, :n] = tall[j * grp:j * grp + gp, :n]
        w1[row:row + n, own_cols] = wide_s[:, :n].T.astype(bf16)
        row += n
    spread_own(copies, at, w1_at, wsem)
    own_x.wait()
    for d in range(1, xs):
        arrived(xg.at[(at.x + xs - d) % xs, at.j], xsem, d - 1)

    order = ("y", "z")
    halves = range(len(order))
    first_axis, second_axis = halves
    slot_up, slot_down, slot_far = RING, 2 * RING, 3 * RING

    def region(s, df, dg, lo=0, n=half):
        return xg.at[pl.ds(s * half + lo, n), at.axis_block(order[s], df, dg)]

    def pass_rows(s, df, dg, axis, d, slot, lo=0, n=half):
        r = region(s, df, dg, lo, n)
        send(r, r, (gsem[0].at[s], gsem[1].at[s]), slot, at.step(order[s], axis, d))

    def rows_in(s, df, dg, slot, lo=0, n=half):
        arrived(region(s, df, dg, lo, n), (gsem[0].at[s], gsem[1].at[s]), slot)

    def both_ways(s, df):
        pass_rows(s, df, 0, second_axis, UP, slot_up + df)
        pass_rows(s, df, 0, second_axis, DOWN, slot_down + df)

    for s in halves:
        pass_rows(s, 0, 0, first_axis, UP, 0)
        pass_rows(s, 0, 0, first_axis, DOWN, 1)
        both_ways(s, 0)
    xo[:] = xg[:, at.j]
    narrow[:c_f, :] = wm_ref[:].astype(f32)
    narrow[c_f:, :] = wa_ref[:].astype(f32)
    tall[:k_loc, :] = narrow[:].T
    for j in range(yzs):
        w2v[j, at.x] = tall[j * grp:j * grp + gp, :].astype(bf16)
    for s in halves:
        rows_in(s, DOWN, 0, 0)
        pass_rows(s, DOWN, 0, first_axis, UP, FAR, 0, quarter)
        rows_in(s, UP, 0, 1)
        pass_rows(s, UP, 0, first_axis, DOWN, DOWN, quarter, quarter)
        both_ways(s, DOWN)
        both_ways(s, UP)
    for s in halves:
        rows_in(s, FAR, 0, FAR, 0, quarter)
        rows_in(s, FAR, 0, DOWN, quarter, quarter)
        both_ways(s, FAR)
    forward_half(copies, at, w1_at, wsem)
    spread_own(late, at, w2_at, vsem)
    for s in halves:
        for df in (0, DOWN):
            rows_in(s, df, DOWN, slot_up + df)
            pass_rows(s, df, DOWN, second_axis, UP, slot_far + df)
    share_near(copies, at, w1_at, wsem)
    for s in halves:
        for df in (UP, FAR):
            rows_in(s, df, UP, slot_down + df)
            pass_rows(s, df, UP, second_axis, DOWN, slot_far + df)
    for s in halves:
        for df in (UP, FAR):
            rows_in(s, df, DOWN, slot_up + df)
        for df in (0, DOWN):
            rows_in(s, df, UP, slot_down + df)
        for df in range(RING):
            rows_in(s, df, FAR, slot_far + df)

    pairs = yzs // 2
    feature = lax.broadcasted_iota(jnp.int32, (2, gp, 1), 1).reshape(2 * gp, 1)
    real = feature < grp
    diagonal = lax.broadcasted_iota(jnp.int32, (gp, 128), 0) == lax.broadcasted_iota(jnp.int32, (gp, 128), 1)

    def load(q):
        return xg[q // pairs, pl.ds((q % pairs) * 2, 2)].astype(f32).reshape(2 * gp, rows)

    def add_up(q, sums):
        raw = load(q)
        for k in range(2):
            row = raw[k * gp + grp:k * gp + grp + 1, :128]
            col = jnp.sum(jnp.where(diagonal, row, 0.0), axis=1, keepdims=True)
            gcol[q, pl.ds(k * gp, gp), :] = jnp.broadcast_to(col, (gp, 128))
        parts = jnp.where(real, raw, 0.0).reshape(2 * gp // 8, 8, rows)
        return sums[0] + jnp.sum(parts, axis=0), sums[1] + jnp.sum(parts * parts, axis=0)

    zero = jnp.zeros((8, rows), f32)
    s1, s2 = lax.fori_loop(0, xs * pairs, add_up, (zero, zero), unroll=4)
    share_far(copies, at, w1_at, wsem)
    d_model = grp * xs * yzs
    mean = jnp.sum(s1, axis=0, keepdims=True) / d_model
    var = jnp.sum(s2, axis=0, keepdims=True) / d_model - mean * mean
    scale = lax.rsqrt(var + 1e-6)

    def normalize(q, c):
        gain = jnp.concatenate([gcol[q]] * (rows // 128), axis=1)
        out = jnp.where(real, (load(q) - mean) * scale * gain, 0.0)
        h[pl.ds(pl.multiple_of(q * 2 * gp, 16), 2 * gp), :] = out.astype(bf16)
        return c

    lax.fori_loop(0, xs * pairs, normalize, 0, unroll=2)
    all_in(copies, at, w1_at, wsem)

    nt = 256

    def query(n, c):
        q = jnp.dot(w1[:c_q], h[:, pl.ds(pl.multiple_of(n * nt, nt), nt)], preferred_element_type=f32)
        qkv_s[pl.ds(pl.multiple_of(n * nt, nt), nt), :] = q.T.astype(bf16)
        return c

    lax.fori_loop(0, rows // nt, query, 0)
    def rows_of(ref, j):
        return ref.at[pl.ds(pl.multiple_of(j * dev_rows, dev_rows), dev_rows)]

    own_q = pltpu.make_async_copy(rows_of(qkv_s, at.j), qkv_in.at[at.j], loc_sem.at[3])
    own_q.start()
    for d in range(1, yzs):
        to = (at.j + d) % yzs
        send(rows_of(qkv_s, to), qkv_in.at[at.j], qsem, d - 1, at.on_yz(to))

    def mlp(n, c):
        cols = pl.ds(pl.multiple_of(n * nt, nt), nt)
        gate = jnp.dot(w1[c_q:c_q + c_f], h[:, cols], preferred_element_type=f32).astype(bf16).astype(f32)
        up = jnp.dot(w1[c_q + c_f:], h[:, cols], preferred_element_type=f32).astype(bf16).astype(f32)
        act[pl.ds(0, c_f), cols] = (jax.nn.silu(gate) * up).astype(bf16)
        return c

    forward_half(late, at, w2_at, vsem)
    steps = rows // nt
    lax.fori_loop(0, steps - 1, mlp, 0)
    for d in range(1, yzs):
        arrived(qkv_in.at[(at.j + yzs - d) % yzs], qsem, d - 1)
    own_q.wait()
    share_near(late, at, w2_at, vsem)

    head_dim = k_s.shape[2]
    per = 2 * c_q // head_dim
    for p in range(yzs // 2):
        both = jnp.concatenate([qkv_in[2 * p], qkv_in[2 * p + 1]], axis=1).astype(f32)
        for i in range(per):
            hd = p * per + i
            u = both[:, i * head_dim:(i + 1) * head_dim]
            if hd <= num_heads:
                u = u * cos_ref[:] + pltpu.roll(u, head_dim // 2, 1) * sin_ref[:]
                u = u.astype(bf16).astype(f32)
            heads[hd] = u
    read_k.wait()
    read_v.wait()

    group = 8
    t_len = k_s.shape[1]
    hp = heads.shape[0]
    position = lax.broadcasted_iota(jnp.int32, (t_len, head_dim), 0)
    along = lax.broadcasted_iota(jnp.int32, (hp, t_len), 1)

    def attend(g, c):
        first = pl.multiple_of(g * group, group)
        block = jnp.swapaxes(heads[:, pl.ds(first, group), :], 0, 1)
        scores, keys, values = [], [], []
        for i in range(group):
            b = first + i
            last = len_ref[b]
            mine = block[i]
            slot = position == last
            kb, vb = [
                jnp.where(slot, mine[row:row + 1], old[b].astype(f32)).astype(bf16)
                for row, old in ((num_heads, k_s), (num_heads + 1, v_s))
            ]
            keys.append(kb)
            values.append(vb)
            score = lax.dot_general(mine.astype(bf16), kb, (((1,), (1,)), ((), ())), preferred_element_type=f32) * head_dim ** -0.5
            scores.append(jnp.where(along <= last, score, -1e30))
        for i in range(group):
            k_s[first + i] = keys[i]
            v_s[first + i] = values[i]
        scores = jnp.concatenate(scores, axis=0)
        e = jnp.exp(scores - jnp.max(scores, axis=1, keepdims=True))
        probs = (e / jnp.sum(e, axis=1, keepdims=True)).reshape(group, hp, t_len).astype(bf16)
        outs = [jnp.dot(probs[i], values[i], preferred_element_type=f32) for i in range(group)]
        heads[:, pl.ds(first, group), :] = jnp.swapaxes(jnp.stack(outs, axis=0), 0, 1)
        return c

    part = dev_rows // 2
    for k in range(2):
        lax.fori_loop(k * part // group, (k + 1) * part // group, attend, 0)
        take = pl.ds(k * part, part)
        for jj in range(yzs):
            lo, hi = jj * c_a // head_dim, ((jj + 1) * c_a - 1) // head_dim + 1
            wide = jnp.concatenate([heads[hd, take, :] for hd in range(lo, hi)], axis=1)
            start = jj * c_a - lo * head_dim
            o_send[k, jj] = wide[:, start:start + c_a].astype(bf16)
        o_own(k).start()
        for d in range(1, yzs):
            o_copy(k, d).start()
    for write in cache_writes():
        write.start()
    lax.fori_loop(steps - 1, steps, mlp, 0)
    copies.finish()


def second_phase(
    xs, yzs, grp, at, any_peer, finish_first, finish_last, w2v, act, xo, y_ref,
    loc_sem, sem1, sem2, sem3, sem4, ysem, ready, zb, r1, r2, r3, r4, yv, ws,
):
    for d in (UP, DOWN):
        for peer in (at.block(d, 0), at.block(0, d)):
            pl.semaphore_signal(ready, inc=1, device_id=at.on_yz(peer), device_id_type=MESH)
    yv[:] = jnp.zeros_like(yv)
    late = finish_first()
    (s1, q1), (s2, q2), (s3, q3), (s4, q4), (ys, yq) = sem1, sem2, sem3, sem4, ysem
    order = ("z", "y")
    hr = zb.shape[2] // 2
    copies = Copies(any_peer)
    send, arrived = copies.send, copies.arrived

    def zat(h, df, dg):
        dz, dy = (df, dg) if order[h] == "z" else (dg, df)
        return zb.at[dz, dy, pl.ds(h * hr, hr)]

    def compute(dz, dy):
        w = w2v[at.block(dz, dy)].astype(jnp.float32)
        for x in range(xs):
            ws[pl.ds(x * grp, grp), :] = w[x, :grp]
        zb[dz, dy] = jnp.dot(ws[:].astype(jnp.bfloat16), act[:], preferred_element_type=jnp.float32)

    def send1(h, dg):
        d = 1 if dg < 2 else 3
        send(zat(h, 2, dg), r1.at[h, dg], s1.at[h, dg], q1.at[h, dg], at.step(order[h], 0, d))

    compute(2, 2)
    pl.semaphore_wait(ready, RING)
    send1(0, 2)
    send1(1, 2)
    for k in (0, 1, 3):
        compute(2, k)
        send1(0, k)
        compute(k, 2)
        send1(1, k)

    def second(i, c):
        k, m = i // 3, i % 3
        compute(k + k // 2, m + m // 2)
        return c

    lax.fori_loop(0, 9, second, 0)

    def send2(h, up, dg):
        df, d, s = (1, 1, 0) if up else (3, 3, 1)
        send(zat(h, df, dg), r2.at[h, s, dg], s2.at[h, s, dg], q2.at[h, s, dg], at.step(order[h], 0, d))

    for h in range(2):
        for dg in (2, 3):
            send2(h, True, dg)
        for dg in (0, 1):
            send2(h, False, dg)
    for k in range(2):
        for h in range(2):
            for up in (True, False):
                dg = 1 - k if up else 2 + k
                arrived(r1.at[h, dg], s1.at[h, dg], q1.at[h, dg])
                ref = zat(h, 1 if up else 3, dg)
                ref[:] = ref[:] + r1[h, dg]
                send2(h, up, dg)

    def plane(h, dg):
        for s in range(2):
            arrived(r2.at[h, s, dg], s2.at[h, s, dg], q2.at[h, s, dg])
        ref = zat(h, 0, dg)
        ref[:] = ref[:] + r2[h, 0, dg] + r2[h, 1, dg]

    big = r3.shape[2]
    sizes = (big, hr - big)

    def part(h, dg, k):
        dz, dy = (0, dg) if order[h] == "z" else (dg, 0)
        return zb.at[dz, dy, pl.ds(h * hr + k * big, sizes[k])]

    def r3_at(h, k):
        return r3.at[h, k, pl.ds(0, sizes[k])]

    def r4_at(h, s, k):
        return r4.at[h, s, k, pl.ds(0, sizes[k])]

    def send4(h, up, k):
        dg, d, s = (1, 1, 0) if up else (3, 3, 1)
        send(part(h, dg, k), r4_at(h, s, k), s4.at[h, s, k], q4.at[h, s, k], at.step(order[h], 1, d))

    for h in range(2):
        plane(h, 2)
        send(part(h, 2, 0), r3_at(h, 0), s3.at[h, 0], q3.at[h, 0], at.step(order[h], 1, 1))
        send(part(h, 2, 1), r3_at(h, 1), s3.at[h, 1], q3.at[h, 1], at.step(order[h], 1, 3))
    for h in range(2):
        plane(h, 1)
        send4(h, True, 1)
        plane(h, 3)
        send4(h, False, 0)
    for h in range(2):
        plane(h, 0)
    for h in range(2):
        arrived(r3_at(h, 0), s3.at[h, 0], q3.at[h, 0])
        ref = part(h, 1, 0)
        ref[:] = ref[:] + r3_at(h, 0)[:]
        send4(h, True, 0)
        arrived(r3_at(h, 1), s3.at[h, 1], q3.at[h, 1])
        ref = part(h, 3, 1)
        ref[:] = ref[:] + r3_at(h, 1)[:]
        send4(h, False, 1)
    def y_cols(x):
        rows = yv.shape[2]
        return y_ref.at[:, pl.ds(pl.multiple_of(x * rows, 128), rows)]

    def y_copy(x, d):
        return pltpu.make_async_remote_copy(
            src_ref=yv.at[x], dst_ref=y_cols(at.x), send_sem=ys.at[d - 1], recv_sem=yq.at[d - 1], device_id=at.on_x(x), device_id_type=MESH
        )

    for h in range(2):
        for k in range(2):
            for s in range(2):
                arrived(r4_at(h, s, k), s4.at[h, s, k], q4.at[h, s, k])
            ref = part(h, 0, k)
            ref[:] = ref[:] + r4_at(h, 0, k)[:] + r4_at(h, 1, k)[:]
            done = xs // 4
            for x in range((2 * h + k) * done, (2 * h + k + 1) * done):
                z = zb[0, 0, pl.ds(x * grp, grp), :]
                yv[x, :grp, :] = (xo[x, :grp, :].astype(jnp.float32) + z).astype(jnp.bfloat16)
                d = lax.rem(x - at.x + xs, xs)

                @pl.when(d == 0)
                def _():
                    pltpu.make_async_copy(yv.at[x], y_cols(x), loc_sem.at[3]).start()

                @pl.when(d != 0)
                def _():
                    y_copy(x, d).start()

    for d in range(1, xs):
        arrived(y_cols((at.x + xs - d) % xs), ys.at[d - 1], yq.at[d - 1])
    pltpu.make_async_copy(yv.at[at.x], y_cols(at.x), loc_sem.at[3]).wait()
    for d in range(1, xs):
        y_copy((at.x + d) % xs, d).wait_send()
    copies.finish()
    finish_last(late)


def layer(x_t, gain, weights, tables, k_cache, v_cache, ctx_len, xs, yzs, gp):
    n_rows = x_t.shape[1]
    rows = n_rows // xs
    dev_rows = k_cache.shape[0]
    c_a, c_f = weights[3].shape[0], weights[4].shape[0]
    n2 = c_a + c_f
    dma, vmem = pltpu.SemaphoreType.DMA, pltpu.VMEM
    bf16 = jnp.bfloat16
    vspec, aspec = pl.BlockSpec(memory_space=vmem), pl.BlockSpec(memory_space=pl.ANY)
    sems = lambda *shape: [dma(shape), dma(shape)]
    cache = jax.ShapeDtypeStruct(k_cache.shape, bf16)
    return pl.pallas_call(
        functools.partial(layer_kernel, xs, yzs, gp),
        out_shape=(jax.ShapeDtypeStruct((gp, n_rows), bf16), cache, cache),
        in_specs=[pl.BlockSpec(memory_space=pltpu.SMEM)] + [vspec] * 9 + [aspec] * 2,
        out_specs=(aspec, aspec, aspec),
        scratch_shapes=[
            vmem((n2, rows), bf16),
            vmem((yzs, xs, gp, n2), bf16),
            vmem((xs, gp, rows), bf16),
            vmem(k_cache.shape, bf16),
            vmem(k_cache.shape, bf16),
            vmem((2, yzs, dev_rows // 2, c_a), bf16),
            vmem((rows, c_a), bf16),
            dma((8,)),
        ]
        + sems(xs - 1) + sems(2, RING * RING) + sems(11) + sems(11) + sems(yzs - 1) + sems(2, yzs - 1)
        + sems(2, RING) + sems(2, 2, RING) + sems(2, 2) + sems(2, 2, 2) + sems(xs - 1)
        + [pltpu.SemaphoreType.REGULAR],
        compiler_params=pltpu.CompilerParams(collective_id=0, has_side_effects=True, vmem_limit_bytes=VMEM_LIMIT),
        name="layer",
    )(ctx_len, x_t, gain, *weights, *tables, k_cache, v_cache)


def solution(mesh):
    xs = mesh.shape["x"]
    yzs = mesh.shape["yz"]
    both_axes = ("x", "yz")
    row_spec = P("dp", both_axes)
    in_w_spec = P("x", "yz")
    out_w_spec = P("yz", "x")
    cache_spec = P(("dp", "x", "yz"), None, None)
    len_spec = P(("dp", "x", "yz"))

    def local_layer(x_loc, gain_loc, wqkv_loc, wgate_loc, wup_loc, wao_loc, wmo_loc, kc_loc, vc_loc, len_loc):
        grp = x_loc.shape[1]
        gp = grp + -grp % 8
        tables = rope_tables(len_loc, kc_loc.shape[2])
        weights = (wqkv_loc.T, wgate_loc, wup_loc, wao_loc, wmo_loc)
        y_t, k_all, v_all = layer(x_loc.T, gain_loc.reshape(1, grp), weights, tables, kc_loc, vc_loc, len_loc, xs, yzs, gp)
        y_loc = y_t[:grp].T
        return y_loc, k_all, v_all

    in_specs = (row_spec, P(both_axes), in_w_spec, in_w_spec, in_w_spec, out_w_spec, out_w_spec, cache_spec, cache_spec, len_spec)
    out_specs = (row_spec, cache_spec, cache_spec)
    return jax.shard_map(local_layer, mesh=mesh, in_specs=in_specs, out_specs=out_specs, check_vma=False)
```

```python
import functools

import jax
import jax.numpy as jnp
import numpy as np
from jax import lax
from jax.experimental import pallas as pl
from jax.experimental.pallas import tpu as pltpu
from jax.sharding import PartitionSpec as P

MESH = pl.DeviceIdType.MESH
RING = 4
UP, FAR, DOWN = 1, 2, 3
VMEM_LIMIT = 62 * 1024 * 1024


def rope_frequencies(head_dim):
    half_dim = head_dim // 2
    inv_freq = np.float32(10000.0) ** (-np.arange(half_dim, dtype=np.float32) / np.float32(half_dim))
    return jnp.asarray(np.concatenate([inv_freq, inv_freq])[None, :])


class Where:
    def __init__(self, xs, yzs):
        self.xs = xs
        self.yzs = yzs
        self.dp = lax.axis_index("dp")
        self.x = lax.axis_index("x")
        self.j = lax.axis_index("yz")
        self.zz = self.j // RING
        self.yy = self.j % RING
        self.chip = self.x // 2
        self.core = self.x % 2

    def block(self, dz, dy):
        return ((self.zz + dz) % RING) * RING + (self.yy + dy) % RING

    def on_yz(self, j):
        return (self.dp, j, self.x)

    def on_x(self, x):
        return (self.dp, self.j, x)

    def axis_block(self, first, df, dg):
        return self.block(df, dg) if first == "z" else self.block(dg, df)

    def step(self, first, axis, d):
        return self.on_yz(self.axis_block(first, d, 0) if axis == 0 else self.axis_block(first, 0, d))

    def x_of(self, dc):
        return ((self.chip + dc) % RING) * 2 + self.core

    def x_other(self, dc):
        return ((self.chip + dc) % RING) * 2 + (1 - self.core)

    def peers(self):
        on_x = [self.on_x((self.x + d) % self.xs) for d in range(1, self.xs)]
        return on_x + [self.on_yz((self.j + d) % self.yzs) for d in range(1, self.yzs)]

    def greet(self):
        for peer in self.peers():
            pl.semaphore_signal(pltpu.get_barrier_semaphore(), inc=1, device_id=peer, device_id_type=MESH)

    def greeted(self):
        pl.semaphore_wait(pltpu.get_barrier_semaphore(), len(self.peers()))


class Copies:
    def __init__(self, any_peer):
        self.any_peer = any_peer
        self.started = []

    def send(self, src, dst, ssem, rsem, peer):
        copy = pltpu.make_async_remote_copy(src_ref=src, dst_ref=dst, send_sem=ssem, recv_sem=rsem, device_id=peer, device_id_type=MESH)
        copy.start()
        self.started.append(copy)

    def arrived(self, dst, ssem, rsem):
        pltpu.make_async_remote_copy(
            src_ref=dst, dst_ref=dst, send_sem=ssem, recv_sem=rsem, device_id=self.any_peer, device_id_type=MESH
        ).wait_recv()

    def finish(self):
        for copy in self.started:
            copy.wait_send()


def layer_kernel(
    xs, yzs, gp, len_ref, x_ref, gain_ref, wq_ref, wg_ref, wu_ref, wa_ref, wm_ref, freq_ref, kc_ref, vc_ref,
    y_ref, ko_ref, vo_ref,
    act, w2v, xo, k_s, v_s, o_send, ob,
    loc_sem, xsend, xrecv, gsend, grecv, wsend, wrecv, vsend, vrecv, qsend, qrecv, osend, orecv,
    s1, q1, s2, q2, s3, q3, s4, q4, ys, yq, ready,
):
    f32, bf16 = jnp.float32, jnp.bfloat16
    dma, vmem = pltpu.SemaphoreType.DMA, pltpu.VMEM
    grp = x_ref.shape[0]
    rows, c_a = ob.shape
    dev_rows, t_len, head_dim = k_s.shape
    c_q, k_loc = wq_ref.shape
    n1 = c_q + 2 * wg_ref.shape[1]
    c_f = wm_ref.shape[0]
    num_heads = yzs * c_a // head_dim
    part = dev_rows // 2
    block = xs * grp
    hr = block // 2
    at = Where(xs, yzs)
    any_peer = at.on_yz(at.block(0, UP))

    def w2_at(x, k=None):
        n2 = w2v.shape[0]
        return w2v.at[:, x] if k is None else w2v.at[pl.ds(k * (n2 // 2), n2 // 2), x]

    def o_rows(j, k):
        return ob.at[pl.ds(pl.multiple_of(j * dev_rows + k * part, part), part)]

    def o_copy(k, d):
        to = (at.j + d) % yzs
        return remote(o_send.at[k, to], o_rows(at.j, k), osend.at[k, d - 1], orecv.at[k, d - 1], at.on_yz(to))

    def o_own(k):
        return pltpu.make_async_copy(o_send.at[k, at.j], o_rows(at.j, k), loc_sem.at[6 + k])

    def cache_writes():
        return [pltpu.make_async_copy(src, dst, loc_sem.at[loc]) for src, dst, loc in ((k_s, ko_ref, 4), (v_s, vo_ref, 5))]

    gather_and_attend = functools.partial(
        first_phase, xs, yzs, num_heads, at, any_peer, w2_at, o_copy, o_own, cache_writes,
        len_ref, x_ref, gain_ref, wq_ref, wg_ref, wu_ref, wa_ref, wm_ref, freq_ref, kc_ref, vc_ref,
        act, w2v, xo, k_s, v_s, o_send,
        loc_sem, (xsend, xrecv), (gsend, grecv), (wsend, wrecv), (vsend, vrecv), (qsend, qrecv),
    )
    pl.run_scoped(
        gather_and_attend,
        vmem((xs, yzs, gp, rows), bf16),
        vmem((xs * yzs * gp, rows), bf16),
        vmem((xs, yzs, gp, 128), f32),
        vmem((n1, xs * yzs * gp), bf16),
        vmem((yzs, dev_rows + dev_rows // 2, 128), bf16),
        vmem((yzs, dev_rows + dev_rows // 2, 128), bf16),
        vmem((num_heads + 2, dev_rows, head_dim), f32),
        vmem((xs, gp, rows), bf16),
        vmem((gp, rows), f32),
        vmem((k_loc + 8, c_f + c_a), f32),
        vmem((yzs * gp, c_f), f32),
        vmem((c_f + c_a, k_loc), f32),
        vmem((dev_rows, head_dim), f32),
        vmem((dev_rows, head_dim), f32),
        *[vmem(ref.shape, ref.dtype) for ref in (x_ref, gain_ref, wq_ref, wg_ref, wu_ref, wa_ref, wm_ref, freq_ref)],
        dma((8,)),
    )

    def finish_first():
        late = Copies(any_peer)
        share_far(late, at, w2_at, (vsend, vrecv))
        for k in range(2):
            for d in range(1, yzs):
                late.arrived(o_rows((at.j + yzs - d) % yzs, k), osend.at[k, d - 1], orecv.at[k, d - 1])
            o_own(k).wait()
        act[pl.ds(c_f, c_a), :] = ob[:].T
        all_in(late, at, w2_at, (vsend, vrecv))
        return late

    def finish_last(late):
        for write in cache_writes():
            write.wait()
        for k in range(2):
            for d in range(1, yzs):
                o_copy(k, d).wait_send()
        for slot in range(9):
            r = w2_at(at.x, None if slot in (4, 7, 8) else 0)
            remote(r, r, vsend.at[slot], vrecv.at[slot], any_peer).wait_send()
        late.finish()

    sum_and_return = functools.partial(
        second_phase, xs, yzs, grp, at, any_peer, finish_first, finish_last, w2v, act, xo, y_ref,
        loc_sem, (s1, q1), (s2, q2), (s3, q3), (s4, q4), (ys, yq), ready,
    )
    big = hr // 2 + hr // 2 % 8
    pl.run_scoped(
        sum_and_return,
        vmem((RING, RING, block, rows), f32),
        vmem((2, RING, hr, rows), f32),
        vmem((2, 2, RING, hr, rows), f32),
        vmem((2, 2, big, rows), f32),
        vmem((2, 2, 2, big, rows), f32),
        vmem((xs, gp, rows), bf16),
        vmem((block, w2v.shape[3]), f32),
    )


def remote(src, dst, ssem, rsem, peer):
    return pltpu.make_async_remote_copy(src_ref=src, dst_ref=dst, send_sem=ssem, recv_sem=rsem, device_id=peer, device_id_type=MESH)


def spread_own(copies, at, region, sems):
    def send(slot, k, x):
        r = region(at.x, k)
        copies.send(r, r, sems[0].at[slot], sems[1].at[slot], at.on_x(x))

    for k in range(2):
        send(2 * k, k, at.x_of(UP))
        send(2 * k + 1, 1 - k, at.x_of(DOWN))
    send(4, None, at.x_other(0))


def pass_on(copies, at, r, sems, slot, x):
    copies.send(r, r, sems[0].at[slot], sems[1].at[slot], at.on_x(x))


def block_in(copies, r, sems, slot):
    copies.arrived(r, sems[0].at[slot], sems[1].at[slot])


def forward_half(copies, at, region, sems):
    for slot, k, here, to in ((0, 0, DOWN, UP), (1, 1, UP, DOWN)):
        r = region(at.x_of(here), k)
        block_in(copies, r, sems, slot)
        pass_on(copies, at, r, sems, slot + 5, at.x_of(to))


def share_near(copies, at, region, sems):
    for slot, k, here in ((2, 1, DOWN), (3, 0, UP)):
        block_in(copies, region(at.x_of(here), k), sems, slot)
        pass_on(copies, at, region(at.x_of(here)), sems, slot + 5, at.x_other(0))


def share_far(copies, at, region, sems):
    for k in range(2):
        r = region(at.x_of(FAR), k)
        block_in(copies, r, sems, 5 + k)
        pass_on(copies, at, r, sems, 9 + k, at.x_other(0))


def all_in(copies, at, region, sems):
    for slot, here in ((4, 0), (7, DOWN), (8, UP)):
        block_in(copies, region(at.x_other(here)), sems, slot)
    for k in range(2):
        block_in(copies, region(at.x_other(FAR), k), sems, 9 + k)


def first_phase(
    xs, yzs, num_heads, at, any_peer, w2_at, o_copy, o_own, cache_writes,
    len_ref, x_hbm, gain_hbm, wq_hbm, wg_hbm, wu_hbm, wa_hbm, wm_hbm, freq_hbm, kc_ref, vc_ref,
    act, w2v, xo, k_s, v_s, o_send,
    loc_sem, xsem, gsem, wsem, vsem, qsem, xg, h, gcol, w1, qkv_s, qkv_in, heads, x_send, stage, tall, wide_s, narrow, cos_s, sin_s,
    x_ref, gain_ref, wq_ref, wg_ref, wu_ref, wa_ref, wm_ref, freq_ref, in_sem,
):
    f32, bf16 = jnp.float32, jnp.bfloat16
    half = xs // 2
    quarter = half // 2
    grp = x_ref.shape[0]
    _, gp, rows = x_send.shape
    dev_rows = rows // yzs
    c_q, k_loc = wq_ref.shape
    c_f, c_a = wm_ref.shape[0], wa_ref.shape[0]
    kx = yzs * gp
    at.greet()
    operands = ((x_hbm, x_ref), (gain_hbm, gain_ref), (wq_hbm, wq_ref), (wg_hbm, wg_ref), (wu_hbm, wu_ref), (wa_hbm, wa_ref), (wm_hbm, wm_ref), (freq_hbm, freq_ref))
    reads = [pltpu.make_async_copy(src, dst, in_sem.at[i]) for i, (src, dst) in enumerate(operands)]
    for read in reads:
        read.start()
    read_k = pltpu.make_async_copy(kc_ref, k_s, loc_sem.at[4])
    read_k.start()
    read_v = pltpu.make_async_copy(vc_ref, v_s, loc_sem.at[5])
    read_v.start()
    stage[:] = jnp.zeros_like(stage)
    for read in reads:
        read.wait()
    stage[grp:grp + 1, :grp] = gain_ref[:].astype(f32)
    for x in range(xs):
        stage[:grp, :] = x_ref[:, x * rows:(x + 1) * rows].astype(f32)
        x_send[x] = stage[:].astype(bf16)
    at.greeted()
    copies, late = Copies(any_peer), Copies(any_peer)

    def send(src, dst, sems, idx, peer):
        copies.send(src, dst, sems[0].at[idx], sems[1].at[idx], peer)

    def arrived(region, sems, idx):
        copies.arrived(region, sems[0].at[idx], sems[1].at[idx])

    own_x = pltpu.make_async_copy(x_send.at[at.x], xg.at[at.x, at.j], loc_sem.at[0])
    own_x.start()
    for d in range(1, xs):
        to = (at.x + d) % xs
        send(x_send.at[to], xg.at[at.x, at.j], xsem, d - 1, at.on_x(to))

    n1 = w1.shape[0]

    def w1_at(x, k=None):
        cols = pl.ds(pl.multiple_of(x * kx, 128), kx)
        return w1.at[:, cols] if k is None else w1.at[pl.ds(k * (n1 // 2), n1 // 2), cols]

    own_cols = pl.ds(pl.multiple_of(at.x * kx, 128), kx)
    tall[k_loc:, :] = jnp.zeros((tall.shape[0] - k_loc, tall.shape[1]), f32)
    row = 0
    for ref in (wq_ref, wg_ref, wu_ref):
        w = ref[:].astype(f32)
        w = w.T if ref is wq_ref else w
        n = w.shape[1]
        tall[:k_loc, :n] = w
        for j in range(yzs):
            wide_s[j * gp:(j + 1) * gp, :n] = tall[j * grp:j * grp + gp, :n]
        w1[row:row + n, own_cols] = wide_s[:, :n].T.astype(bf16)
        row += n
    spread_own(copies, at, w1_at, wsem)
    own_x.wait()
    for d in range(1, xs):
        arrived(xg.at[(at.x + xs - d) % xs, at.j], xsem, d - 1)

    order = ("y", "z")
    halves = range(len(order))
    first_axis, second_axis = halves
    slot_up, slot_down, slot_far = RING, 2 * RING, 3 * RING

    def region(s, df, dg, lo=0, n=half):
        return xg.at[pl.ds(s * half + lo, n), at.axis_block(order[s], df, dg)]

    def pass_rows(s, df, dg, axis, d, slot, lo=0, n=half):
        r = region(s, df, dg, lo, n)
        send(r, r, (gsem[0].at[s], gsem[1].at[s]), slot, at.step(order[s], axis, d))

    def rows_in(s, df, dg, slot, lo=0, n=half):
        arrived(region(s, df, dg, lo, n), (gsem[0].at[s], gsem[1].at[s]), slot)

    def both_ways(s, df):
        pass_rows(s, df, 0, second_axis, UP, slot_up + df)
        pass_rows(s, df, 0, second_axis, DOWN, slot_down + df)

    for s in halves:
        pass_rows(s, 0, 0, first_axis, UP, 0)
        pass_rows(s, 0, 0, first_axis, DOWN, 1)
        both_ways(s, 0)
    xo[:] = xg[:, at.j]
    narrow[:c_f, :] = wm_ref[:].astype(f32)
    narrow[c_f:, :] = wa_ref[:].astype(f32)
    tall[:k_loc, :] = narrow[:].T
    for j in range(yzs):
        w2v[j, at.x] = tall[j * grp:j * grp + gp, :].astype(bf16)
    head_dim = k_s.shape[2]
    request = lax.broadcasted_iota(jnp.int32, (dev_rows, head_dim), 0)
    lane = lax.broadcasted_iota(jnp.int32, (dev_rows, head_dim), 1)

    def place(b, p):
        return jnp.where(request == b, len_ref[b].astype(f32), p)

    angles = lax.fori_loop(0, dev_rows, place, jnp.zeros((dev_rows, head_dim), f32), unroll=8) * freq_ref[:]
    cos_s[:] = jnp.cos(angles)
    sin_s[:] = jnp.where(lane < head_dim // 2, -1.0, 1.0) * jnp.sin(angles)
    for s in halves:
        rows_in(s, DOWN, 0, 0)
        pass_rows(s, DOWN, 0, first_axis, UP, FAR, 0, quarter)
        rows_in(s, UP, 0, 1)
        pass_rows(s, UP, 0, first_axis, DOWN, DOWN, quarter, quarter)
        both_ways(s, DOWN)
        both_ways(s, UP)
    for s in halves:
        rows_in(s, FAR, 0, FAR, 0, quarter)
        rows_in(s, FAR, 0, DOWN, quarter, quarter)
        both_ways(s, FAR)
    forward_half(copies, at, w1_at, wsem)
    spread_own(late, at, w2_at, vsem)

    diagonal = lax.broadcasted_iota(jnp.int32, (gp, 128), 0) == lax.broadcasted_iota(jnp.int32, (gp, 128), 1)
    feature = lax.broadcasted_iota(jnp.int32, (gp, 1), 0)

    def add_up(s, dg, sums):
        def body(i, c):
            x, j = s * half + i // RING, at.axis_block(order[s], i % RING, dg)
            raw = xg[x, j].astype(f32)
            col = jnp.sum(jnp.where(diagonal, raw[grp:grp + 1, :128], 0.0), axis=1, keepdims=True)
            gcol[x, j] = jnp.broadcast_to(col, (gp, 128))
            parts = jnp.where(feature < grp, raw, 0.0).reshape(gp // 8, 8, rows)
            return c[0] + jnp.sum(parts, axis=0), c[1] + jnp.sum(parts * parts, axis=0)

        return lax.fori_loop(0, half * RING, body, sums, unroll=4)

    sums = (jnp.zeros((8, rows), f32), jnp.zeros((8, rows), f32))
    for s in halves:
        sums = add_up(s, 0, sums)
    for s in halves:
        for df in (0, DOWN):
            rows_in(s, df, DOWN, slot_up + df)
            pass_rows(s, df, DOWN, second_axis, UP, slot_far + df)
    share_near(copies, at, w1_at, wsem)
    for s in halves:
        for df in (UP, FAR):
            rows_in(s, df, UP, slot_down + df)
            pass_rows(s, df, UP, second_axis, DOWN, slot_far + df)
    for s in halves:
        for df in (UP, FAR):
            rows_in(s, df, DOWN, slot_up + df)
        for df in (0, DOWN):
            rows_in(s, df, UP, slot_down + df)
    for dg in (DOWN, UP):
        for s in halves:
            sums = add_up(s, dg, sums)
    for s in halves:
        for df in range(RING):
            rows_in(s, df, FAR, slot_far + df)
        sums = add_up(s, FAR, sums)

    pairs = yzs // 2
    real = lax.broadcasted_iota(jnp.int32, (2, gp, 1), 1).reshape(2 * gp, 1) < grp
    s1, s2 = sums
    share_far(copies, at, w1_at, wsem)
    d_model = grp * xs * yzs
    mean = jnp.sum(s1, axis=0, keepdims=True) / d_model
    var = jnp.sum(s2, axis=0, keepdims=True) / d_model - mean * mean
    scale = lax.rsqrt(var + 1e-6)

    def normalize(q, c):
        at_q = q // pairs, pl.ds((q % pairs) * 2, 2)
        gain = jnp.concatenate([gcol[at_q].reshape(2 * gp, 128)] * (rows // 128), axis=1)
        out = jnp.where(real, (xg[at_q].astype(f32).reshape(2 * gp, rows) - mean) * scale * gain, 0.0)
        h[pl.ds(pl.multiple_of(q * 2 * gp, 16), 2 * gp), :] = out.astype(bf16)
        return c

    lax.fori_loop(0, xs * pairs, normalize, 0, unroll=2)
    all_in(copies, at, w1_at, wsem)

    nt = 256

    def query(n, c):
        q = jnp.dot(w1[:c_q], h[:, pl.ds(pl.multiple_of(n * nt, nt), nt)], preferred_element_type=f32)
        q = q.T
        for i in range(nt // dev_rows):
            piece = q[i * dev_rows:(i + 1) * dev_rows]
            to = n * (nt // dev_rows) + i
            qkv_s[to, :dev_rows] = piece[:, :128].astype(bf16)
            qkv_s[to, dev_rows:] = jnp.concatenate([piece[:dev_rows // 2, 128:], piece[dev_rows // 2:, 128:]], axis=1).astype(bf16)
        return c

    def unpacked(j):
        piece = qkv_in[j].astype(f32)
        rest = piece[dev_rows:]
        rest = jnp.concatenate([rest[:, :c_q - 128], rest[:, c_q - 128:]], axis=0)
        return jnp.concatenate([piece[:dev_rows], rest], axis=1)

    lax.fori_loop(0, rows // nt, query, 0)
    own_q = pltpu.make_async_copy(qkv_s.at[at.j], qkv_in.at[at.j], loc_sem.at[3])
    own_q.start()
    for d in range(1, yzs):
        to = (at.j + d) % yzs
        send(qkv_s.at[to], qkv_in.at[at.j], qsem, d - 1, at.on_yz(to))

    def mlp(n, c):
        cols = pl.ds(pl.multiple_of(n * nt, nt), nt)
        gate = jnp.dot(w1[c_q:c_q + c_f], h[:, cols], preferred_element_type=f32).astype(bf16).astype(f32)
        up = jnp.dot(w1[c_q + c_f:], h[:, cols], preferred_element_type=f32).astype(bf16).astype(f32)
        act[pl.ds(0, c_f), cols] = (jax.nn.silu(gate) * up).astype(bf16)
        return c

    steps = rows // nt
    lax.fori_loop(0, steps // 2, mlp, 0)
    forward_half(late, at, w2_at, vsem)
    lax.fori_loop(steps // 2, steps - 1, mlp, 0)
    for d in range(1, yzs):
        arrived(qkv_in.at[(at.j + yzs - d) % yzs], qsem, d - 1)
    own_q.wait()
    share_near(late, at, w2_at, vsem)

    per = 2 * c_q // head_dim
    for p in range(yzs // 2):
        both = jnp.concatenate([unpacked(2 * p), unpacked(2 * p + 1)], axis=1)
        for i in range(per):
            hd = p * per + i
            u = both[:, i * head_dim:(i + 1) * head_dim]
            if hd <= num_heads:
                u = u * cos_s[:] + pltpu.roll(u, head_dim // 2, 1) * sin_s[:]
                u = u.astype(bf16).astype(f32)
            heads[hd] = u
    read_k.wait()
    read_v.wait()

    group = 8
    t_len = k_s.shape[1]
    hp = heads.shape[0]
    position = lax.broadcasted_iota(jnp.int32, (t_len, head_dim), 0)
    along = lax.broadcasted_iota(jnp.int32, (hp, t_len), 1)

    def attend(g, c):
        first = pl.multiple_of(g * group, group)
        block = jnp.swapaxes(heads[:, pl.ds(first, group), :], 0, 1)
        scores, keys, values = [], [], []
        for i in range(group):
            b = first + i
            last = len_ref[b]
            mine = block[i]
            slot = position == last
            kb, vb = [
                jnp.where(slot, mine[row:row + 1], old[b].astype(f32)).astype(bf16)
                for row, old in ((num_heads, k_s), (num_heads + 1, v_s))
            ]
            keys.append(kb)
            values.append(vb)
            score = lax.dot_general(mine.astype(bf16), kb, (((1,), (1,)), ((), ())), preferred_element_type=f32) * head_dim ** -0.5
            scores.append(jnp.where(along <= last, score, -1e30))
        for i in range(group):
            k_s[first + i] = keys[i]
            v_s[first + i] = values[i]
        scores = jnp.concatenate(scores, axis=0)
        e = jnp.exp(scores - jnp.max(scores, axis=1, keepdims=True))
        probs = (e / jnp.sum(e, axis=1, keepdims=True)).reshape(group, hp, t_len).astype(bf16)
        outs = [jnp.dot(probs[i], values[i], preferred_element_type=f32) for i in range(group)]
        heads[:, pl.ds(first, group), :] = jnp.swapaxes(jnp.stack(outs, axis=0), 0, 1)
        return c

    part = dev_rows // 2
    for k in range(2):
        lax.fori_loop(k * part // group, (k + 1) * part // group, attend, 0)
        take = pl.ds(k * part, part)
        for jj in range(yzs):
            lo, hi = jj * c_a // head_dim, ((jj + 1) * c_a - 1) // head_dim + 1
            wide = jnp.concatenate([heads[hd, take, :] for hd in range(lo, hi)], axis=1)
            start = jj * c_a - lo * head_dim
            o_send[k, jj] = wide[:, start:start + c_a].astype(bf16)
        o_own(k).start()
        for d in range(1, yzs):
            o_copy(k, d).start()
    for write in cache_writes():
        write.start()
    lax.fori_loop(steps - 1, steps, mlp, 0)
    copies.finish()


def second_phase(
    xs, yzs, grp, at, any_peer, finish_first, finish_last, w2v, act, xo, y_ref,
    loc_sem, sem1, sem2, sem3, sem4, ysem, ready, zb, r1, r2, r3, r4, yv, ws,
):
    for d in (UP, DOWN):
        for peer in (at.block(d, 0), at.block(0, d)):
            pl.semaphore_signal(ready, inc=1, device_id=at.on_yz(peer), device_id_type=MESH)
    yv[:] = jnp.zeros_like(yv)
    late = finish_first()
    (s1, q1), (s2, q2), (s3, q3), (s4, q4), (ys, yq) = sem1, sem2, sem3, sem4, ysem
    order = ("z", "y")
    hr = zb.shape[2] // 2
    copies = Copies(any_peer)
    send, arrived = copies.send, copies.arrived

    def zat(h, df, dg):
        dz, dy = (df, dg) if order[h] == "z" else (dg, df)
        return zb.at[dz, dy, pl.ds(h * hr, hr)]

    def compute(dz, dy):
        w = w2v[at.block(dz, dy)].astype(jnp.float32)
        for x in range(xs):
            ws[pl.ds(x * grp, grp), :] = w[x, :grp]
        zb[dz, dy] = jnp.dot(ws[:].astype(jnp.bfloat16), act[:], preferred_element_type=jnp.float32)

    def send1(h, dg):
        d = 1 if dg < 2 else 3
        send(zat(h, 2, dg), r1.at[h, dg], s1.at[h, dg], q1.at[h, dg], at.step(order[h], 0, d))

    compute(2, 2)
    pl.semaphore_wait(ready, RING)
    send1(0, 2)
    send1(1, 2)
    for k in (0, 1, 3):
        compute(2, k)
        send1(0, k)
        compute(k, 2)
        send1(1, k)

    def second(i, c):
        k, m = i // 3, i % 3
        compute(k + k // 2, m + m // 2)
        return c

    lax.fori_loop(0, 9, second, 0)

    def send2(h, up, dg):
        df, d, s = (1, 1, 0) if up else (3, 3, 1)
        send(zat(h, df, dg), r2.at[h, s, dg], s2.at[h, s, dg], q2.at[h, s, dg], at.step(order[h], 0, d))

    for h in range(2):
        for dg in (2, 3):
            send2(h, True, dg)
        for dg in (0, 1):
            send2(h, False, dg)
    for k in range(2):
        for h in range(2):
            for up in (True, False):
                dg = 1 - k if up else 2 + k
                arrived(r1.at[h, dg], s1.at[h, dg], q1.at[h, dg])
                ref = zat(h, 1 if up else 3, dg)
                ref[:] = ref[:] + r1[h, dg]
                send2(h, up, dg)

    def plane(h, dg):
        for s in range(2):
            arrived(r2.at[h, s, dg], s2.at[h, s, dg], q2.at[h, s, dg])
        ref = zat(h, 0, dg)
        ref[:] = ref[:] + r2[h, 0, dg] + r2[h, 1, dg]

    big = r3.shape[2]
    sizes = (big, hr - big)

    def part(h, dg, k):
        dz, dy = (0, dg) if order[h] == "z" else (dg, 0)
        return zb.at[dz, dy, pl.ds(h * hr + k * big, sizes[k])]

    def r3_at(h, k):
        return r3.at[h, k, pl.ds(0, sizes[k])]

    def r4_at(h, s, k):
        return r4.at[h, s, k, pl.ds(0, sizes[k])]

    def send4(h, up, k):
        dg, d, s = (1, 1, 0) if up else (3, 3, 1)
        send(part(h, dg, k), r4_at(h, s, k), s4.at[h, s, k], q4.at[h, s, k], at.step(order[h], 1, d))

    for h in range(2):
        plane(h, 2)
        send(part(h, 2, 0), r3_at(h, 0), s3.at[h, 0], q3.at[h, 0], at.step(order[h], 1, 1))
        send(part(h, 2, 1), r3_at(h, 1), s3.at[h, 1], q3.at[h, 1], at.step(order[h], 1, 3))
    for h in range(2):
        plane(h, 1)
        send4(h, True, 1)
        plane(h, 3)
        send4(h, False, 0)
    for h in range(2):
        plane(h, 0)
    for h in range(2):
        arrived(r3_at(h, 0), s3.at[h, 0], q3.at[h, 0])
        ref = part(h, 1, 0)
        ref[:] = ref[:] + r3_at(h, 0)[:]
        send4(h, True, 0)
        arrived(r3_at(h, 1), s3.at[h, 1], q3.at[h, 1])
        ref = part(h, 3, 1)
        ref[:] = ref[:] + r3_at(h, 1)[:]
        send4(h, False, 1)
    def y_cols(x):
        rows = yv.shape[2]
        return y_ref.at[:, pl.ds(pl.multiple_of(x * rows, 128), rows)]

    def y_copy(x, d):
        return pltpu.make_async_remote_copy(
            src_ref=yv.at[x], dst_ref=y_cols(at.x), send_sem=ys.at[d - 1], recv_sem=yq.at[d - 1], device_id=at.on_x(x), device_id_type=MESH
        )

    for h in range(2):
        for k in range(2):
            for s in range(2):
                arrived(r4_at(h, s, k), s4.at[h, s, k], q4.at[h, s, k])
            ref = part(h, 0, k)
            ref[:] = ref[:] + r4_at(h, 0, k)[:] + r4_at(h, 1, k)[:]
            done = xs // 4
            for x in range((2 * h + k) * done, (2 * h + k + 1) * done):
                z = zb[0, 0, pl.ds(x * grp, grp), :]
                yv[x, :grp, :] = (xo[x, :grp, :].astype(jnp.float32) + z).astype(jnp.bfloat16)
                d = lax.rem(x - at.x + xs, xs)

                @pl.when(d == 0)
                def _():
                    pltpu.make_async_copy(yv.at[x], y_cols(x), loc_sem.at[3]).start()

                @pl.when(d != 0)
                def _():
                    y_copy(x, d).start()

    for d in range(1, xs):
        arrived(y_cols((at.x + xs - d) % xs), ys.at[d - 1], yq.at[d - 1])
    pltpu.make_async_copy(yv.at[at.x], y_cols(at.x), loc_sem.at[3]).wait()
    for d in range(1, xs):
        y_copy((at.x + d) % xs, d).wait_send()
    copies.finish()
    finish_last(late)


def layer(x_t, gain, weights, freq, k_cache, v_cache, ctx_len, xs, yzs, gp):
    n_rows = x_t.shape[1]
    rows = n_rows // xs
    dev_rows = k_cache.shape[0]
    c_a, c_f = weights[3].shape[0], weights[4].shape[0]
    n2 = c_a + c_f
    dma, vmem = pltpu.SemaphoreType.DMA, pltpu.VMEM
    bf16 = jnp.bfloat16
    aspec = pl.BlockSpec(memory_space=pl.ANY)
    sems = lambda *shape: [dma(shape), dma(shape)]
    cache = jax.ShapeDtypeStruct(k_cache.shape, bf16)
    return pl.pallas_call(
        functools.partial(layer_kernel, xs, yzs, gp),
        out_shape=(jax.ShapeDtypeStruct((gp, n_rows), bf16), cache, cache),
        in_specs=[pl.BlockSpec(memory_space=pltpu.SMEM)] + [aspec] * 10,
        out_specs=(aspec, aspec, aspec),
        scratch_shapes=[
            vmem((n2, rows), bf16),
            vmem((yzs, xs, gp, n2), bf16),
            vmem((xs, gp, rows), bf16),
            vmem(k_cache.shape, bf16),
            vmem(k_cache.shape, bf16),
            vmem((2, yzs, dev_rows // 2, c_a), bf16),
            vmem((rows, c_a), bf16),
            dma((8,)),
        ]
        + sems(xs - 1) + sems(2, RING * RING) + sems(11) + sems(11) + sems(yzs - 1) + sems(2, yzs - 1)
        + sems(2, RING) + sems(2, 2, RING) + sems(2, 2) + sems(2, 2, 2) + sems(xs - 1)
        + [pltpu.SemaphoreType.REGULAR],
        compiler_params=pltpu.CompilerParams(collective_id=0, has_side_effects=True, vmem_limit_bytes=VMEM_LIMIT),
        name="layer",
    )(ctx_len, x_t, gain, *weights, freq, k_cache, v_cache)


def results_kernel(chunks, y_ref, k_ref, v_ref, yo_ref, ko_ref, vo_ref, y_in, y_out, k_s, v_s, y_sem, in_sem, out_sem):
    n = k_s.shape[0] // chunks
    y_read = pltpu.make_async_copy(y_ref, y_in, y_sem.at[0])
    y_read.start()
    copies = []
    for c in range(chunks):
        for i, (src, buf, dst) in enumerate(((k_ref, k_s, ko_ref), (v_ref, v_s, vo_ref))):
            take = pl.ds(c * n, n)
            read = pltpu.make_async_copy(src.at[take], buf.at[take], in_sem.at[i, c])
            read.start()
            copies.append((read, pltpu.make_async_copy(buf.at[take], dst.at[take], out_sem.at[i, c])))
    y_read.wait()
    y_out[:] = y_in[:y_out.shape[0], :]
    y_write = pltpu.make_async_copy(y_out, yo_ref, y_sem.at[1])
    y_write.start()
    for read, write in copies:
        read.wait()
        write.start()
    y_write.wait()
    for _, write in copies:
        write.wait()


def results(y_t, k_all, v_all, grp):
    chunks = 4
    dma, vmem = pltpu.SemaphoreType.DMA, pltpu.VMEM
    aspec = pl.BlockSpec(memory_space=pl.ANY)
    shapes = ((grp, y_t.shape[1]), k_all.shape, v_all.shape)
    return pl.pallas_call(
        functools.partial(results_kernel, chunks),
        out_shape=tuple(jax.ShapeDtypeStruct(shape, y_t.dtype) for shape in shapes),
        in_specs=[aspec] * 3,
        out_specs=(aspec,) * 3,
        scratch_shapes=[vmem(shape, y_t.dtype) for shape in (y_t.shape,) + shapes] + [dma((2,)), dma((2, chunks)), dma((2, chunks))],
        compiler_params=pltpu.CompilerParams(vmem_limit_bytes=VMEM_LIMIT),
        name="results",
    )(y_t, k_all, v_all)


def solution(mesh):
    xs = mesh.shape["x"]
    yzs = mesh.shape["yz"]
    both_axes = ("x", "yz")
    row_spec = P("dp", both_axes)
    in_w_spec = P("x", "yz")
    out_w_spec = P("yz", "x")
    cache_spec = P(("dp", "x", "yz"), None, None)
    len_spec = P(("dp", "x", "yz"))

    def local_layer(x_loc, gain_loc, wqkv_loc, wgate_loc, wup_loc, wao_loc, wmo_loc, kc_loc, vc_loc, len_loc):
        grp = x_loc.shape[1]
        gp = grp + -grp % 8
        freq = rope_frequencies(kc_loc.shape[2])
        weights = (wqkv_loc.T, wgate_loc, wup_loc, wao_loc, wmo_loc)
        y_t, k_all, v_all = layer(x_loc.T, gain_loc.reshape(1, grp), weights, freq, kc_loc, vc_loc, len_loc, xs, yzs, gp)
        y_t, k_all, v_all = results(y_t, k_all, v_all, grp)
        return y_t.T, k_all, v_all

    in_specs = (row_spec, P(both_axes), in_w_spec, in_w_spec, in_w_spec, out_w_spec, out_w_spec, cache_spec, cache_spec, len_spec)
    out_specs = (row_spec, cache_spec, cache_spec)
    return jax.shard_map(local_layer, mesh=mesh, in_specs=in_specs, out_specs=out_specs, check_vma=False)
```

```python
import functools

import jax
import jax.numpy as jnp
import numpy as np
from jax import lax
from jax.experimental import pallas as pl
from jax.experimental.pallas import tpu as pltpu
from jax.sharding import PartitionSpec as P

MESH = pl.DeviceIdType.MESH
RING = 4
UP, FAR, DOWN = 1, 2, 3
VMEM_LIMIT = 62 * 1024 * 1024


def rope_frequencies(head_dim):
    half_dim = head_dim // 2
    inv_freq = np.float32(10000.0) ** (-np.arange(half_dim, dtype=np.float32) / np.float32(half_dim))
    return jnp.asarray(np.concatenate([inv_freq, inv_freq])[None, :])


class Where:
    def __init__(self, xs, yzs):
        self.xs = xs
        self.yzs = yzs
        self.dp = lax.axis_index("dp")
        self.x = lax.axis_index("x")
        self.j = lax.axis_index("yz")
        self.zz = self.j // RING
        self.yy = self.j % RING
        self.chip = self.x // 2
        self.core = self.x % 2

    def block(self, dz, dy):
        return ((self.zz + dz) % RING) * RING + (self.yy + dy) % RING

    def on_yz(self, j):
        return (self.dp, j, self.x)

    def on_x(self, x):
        return (self.dp, self.j, x)

    def axis_block(self, first, df, dg):
        return self.block(df, dg) if first == "z" else self.block(dg, df)

    def step(self, first, axis, d):
        return self.on_yz(self.axis_block(first, d, 0) if axis == 0 else self.axis_block(first, 0, d))

    def x_of(self, dc):
        return ((self.chip + dc) % RING) * 2 + self.core

    def x_other(self, dc):
        return ((self.chip + dc) % RING) * 2 + (1 - self.core)

    def peers(self):
        on_x = [self.on_x((self.x + d) % self.xs) for d in range(1, self.xs)]
        return on_x + [self.on_yz((self.j + d) % self.yzs) for d in range(1, self.yzs)]

    def greet(self):
        for peer in self.peers():
            pl.semaphore_signal(pltpu.get_barrier_semaphore(), inc=1, device_id=peer, device_id_type=MESH)

    def greeted(self):
        pl.semaphore_wait(pltpu.get_barrier_semaphore(), len(self.peers()))


class Copies:
    def __init__(self, any_peer):
        self.any_peer = any_peer
        self.started = []

    def send(self, src, dst, ssem, rsem, peer):
        copy = pltpu.make_async_remote_copy(src_ref=src, dst_ref=dst, send_sem=ssem, recv_sem=rsem, device_id=peer, device_id_type=MESH)
        copy.start()
        self.started.append(copy)

    def arrived(self, dst, ssem, rsem):
        pltpu.make_async_remote_copy(
            src_ref=dst, dst_ref=dst, send_sem=ssem, recv_sem=rsem, device_id=self.any_peer, device_id_type=MESH
        ).wait_recv()

    def finish(self):
        for copy in self.started:
            copy.wait_send()


def layer_kernel(
    xs, yzs, gp, len_ref, x_ref, gain_ref, wq_ref, wg_ref, wu_ref, wa_ref, wm_ref, freq_ref, kc_ref, vc_ref,
    y_ref, ko_ref, vo_ref,
    act, w2v, xo, k_s, v_s, o_send, ob,
    loc_sem, xsend, xrecv, gsend, grecv, wsend, wrecv, vsend, vrecv, qsend, qrecv, osend, orecv,
    s1, q1, s2, q2, s3, q3, s4, q4, ys, yq, ready,
):
    f32, bf16 = jnp.float32, jnp.bfloat16
    dma, vmem = pltpu.SemaphoreType.DMA, pltpu.VMEM
    grp = x_ref.shape[0]
    rows, c_a = ob.shape
    dev_rows, t_len, head_dim = k_s.shape
    c_q, k_loc = wq_ref.shape
    n1 = c_q + 2 * wg_ref.shape[1]
    c_f = wm_ref.shape[0]
    num_heads = yzs * c_a // head_dim
    part = dev_rows // 2
    block = xs * grp
    hr = block // 2
    at = Where(xs, yzs)
    any_peer = at.on_yz(at.block(0, UP))

    def w2_at(x, k=None):
        n2 = w2v.shape[0]
        return w2v.at[:, x] if k is None else w2v.at[pl.ds(k * (n2 // 2), n2 // 2), x]

    def o_rows(j, k):
        return ob.at[pl.ds(pl.multiple_of(j * dev_rows + k * part, part), part)]

    def o_copy(k, d):
        to = (at.j + d) % yzs
        return remote(o_send.at[k, to], o_rows(at.j, k), osend.at[k, d - 1], orecv.at[k, d - 1], at.on_yz(to))

    def o_own(k):
        return pltpu.make_async_copy(o_send.at[k, at.j], o_rows(at.j, k), loc_sem.at[6 + k])

    def cache_writes():
        return [pltpu.make_async_copy(src, dst, loc_sem.at[loc]) for src, dst, loc in ((k_s, ko_ref, 4), (v_s, vo_ref, 5))]

    gather_and_attend = functools.partial(
        first_phase, xs, yzs, num_heads, at, any_peer, w2_at, o_copy, o_own, cache_writes,
        len_ref, x_ref, gain_ref, wq_ref, wg_ref, wu_ref, wa_ref, wm_ref, freq_ref, kc_ref, vc_ref,
        act, w2v, xo, k_s, v_s, o_send,
        loc_sem, (xsend, xrecv), (gsend, grecv), (wsend, wrecv), (vsend, vrecv), (qsend, qrecv),
    )
    pl.run_scoped(
        gather_and_attend,
        vmem((xs, yzs, gp, rows), bf16),
        vmem((xs * yzs * gp, rows), bf16),
        vmem((xs, yzs, gp, 128), f32),
        vmem((n1, xs * yzs * gp), bf16),
        vmem((2, yzs, part + part // 2, 128), bf16),
        vmem((2, yzs, part + part // 2, 128), bf16),
        vmem((num_heads + 2, dev_rows, head_dim), f32),
        vmem((xs, gp, rows), bf16),
        vmem((gp, rows), f32),
        vmem((k_loc + 8, c_f + c_a), f32),
        vmem((yzs * gp, c_f), f32),
        vmem((c_f + c_a, k_loc), f32),
        vmem((dev_rows, head_dim), f32),
        vmem((dev_rows, head_dim), f32),
        *[vmem(ref.shape, ref.dtype) for ref in (x_ref, gain_ref, wq_ref, wg_ref, wu_ref, wa_ref, wm_ref, freq_ref)],
        pltpu.SMEM(len_ref.shape, len_ref.dtype),
        dma((9,)),
    )

    def finish_first():
        late = Copies(any_peer)
        share_far(late, at, w2_at, (vsend, vrecv))
        for k in range(2):
            for d in range(1, yzs):
                late.arrived(o_rows((at.j + yzs - d) % yzs, k), osend.at[k, d - 1], orecv.at[k, d - 1])
            o_own(k).wait()
        act[pl.ds(c_f, c_a), :] = ob[:].T
        all_in(late, at, w2_at, (vsend, vrecv))
        return late

    def finish_last(late):
        for write in cache_writes():
            write.wait()
        for k in range(2):
            for d in range(1, yzs):
                o_copy(k, d).wait_send()
        for slot in range(9):
            r = w2_at(at.x, None if slot in (4, 7, 8) else 0)
            remote(r, r, vsend.at[slot], vrecv.at[slot], any_peer).wait_send()
        late.finish()

    sum_and_return = functools.partial(
        second_phase, xs, yzs, grp, at, any_peer, finish_first, finish_last, w2v, act, xo, y_ref,
        loc_sem, (s1, q1), (s2, q2), (s3, q3), (s4, q4), (ys, yq), ready,
    )
    big = hr // 2 + hr // 2 % 8
    pl.run_scoped(
        sum_and_return,
        vmem((RING, RING, block, rows), f32),
        vmem((2, RING, hr, rows), f32),
        vmem((2, 2, RING, hr, rows), f32),
        vmem((2, 2, big, rows), f32),
        vmem((2, 2, 2, big, rows), f32),
        vmem((xs, gp, rows), bf16),
        vmem((block, w2v.shape[3]), f32),
    )


def remote(src, dst, ssem, rsem, peer):
    return pltpu.make_async_remote_copy(src_ref=src, dst_ref=dst, send_sem=ssem, recv_sem=rsem, device_id=peer, device_id_type=MESH)


def spread_own(copies, at, region, sems):
    def send(slot, k, x):
        r = region(at.x, k)
        copies.send(r, r, sems[0].at[slot], sems[1].at[slot], at.on_x(x))

    for k in range(2):
        send(2 * k, k, at.x_of(UP))
        send(2 * k + 1, 1 - k, at.x_of(DOWN))
    send(4, None, at.x_other(0))


def pass_on(copies, at, r, sems, slot, x):
    copies.send(r, r, sems[0].at[slot], sems[1].at[slot], at.on_x(x))


def block_in(copies, r, sems, slot):
    copies.arrived(r, sems[0].at[slot], sems[1].at[slot])


def forward_half(copies, at, region, sems):
    for slot, k, here, to in ((0, 0, DOWN, UP), (1, 1, UP, DOWN)):
        r = region(at.x_of(here), k)
        block_in(copies, r, sems, slot)
        pass_on(copies, at, r, sems, slot + 5, at.x_of(to))


def share_near(copies, at, region, sems):
    for slot, k, here in ((2, 1, DOWN), (3, 0, UP)):
        block_in(copies, region(at.x_of(here), k), sems, slot)
        pass_on(copies, at, region(at.x_of(here)), sems, slot + 5, at.x_other(0))


def share_far(copies, at, region, sems):
    for k in range(2):
        r = region(at.x_of(FAR), k)
        block_in(copies, r, sems, 5 + k)
        pass_on(copies, at, r, sems, 9 + k, at.x_other(0))


def all_in(copies, at, region, sems):
    for slot, here in ((4, 0), (7, DOWN), (8, UP)):
        block_in(copies, region(at.x_other(here)), sems, slot)
    for k in range(2):
        block_in(copies, region(at.x_other(FAR), k), sems, 9 + k)


def first_phase(
    xs, yzs, num_heads, at, any_peer, w2_at, o_copy, o_own, cache_writes,
    len_hbm, x_hbm, gain_hbm, wq_hbm, wg_hbm, wu_hbm, wa_hbm, wm_hbm, freq_hbm, kc_ref, vc_ref,
    act, w2v, xo, k_s, v_s, o_send,
    loc_sem, xsem, gsem, wsem, vsem, qsem, xg, h, gcol, w1, qkv_s, qkv_in, heads, x_send, stage, tall, wide_s, narrow, cos_s, sin_s,
    x_ref, gain_ref, wq_ref, wg_ref, wu_ref, wa_ref, wm_ref, freq_ref, len_ref, in_sem,
):
    f32, bf16 = jnp.float32, jnp.bfloat16
    half = xs // 2
    quarter = half // 2
    grp = x_ref.shape[0]
    _, gp, rows = x_send.shape
    dev_rows = rows // yzs
    c_q, k_loc = wq_ref.shape
    c_f, c_a = wm_ref.shape[0], wa_ref.shape[0]
    kx = yzs * gp
    at.greet()
    operands = ((x_hbm, x_ref), (gain_hbm, gain_ref), (wq_hbm, wq_ref), (wg_hbm, wg_ref), (wu_hbm, wu_ref), (wa_hbm, wa_ref), (wm_hbm, wm_ref), (freq_hbm, freq_ref), (len_hbm, len_ref))
    reads = [pltpu.make_async_copy(src, dst, in_sem.at[i]) for i, (src, dst) in enumerate(operands)]
    for read in reads:
        read.start()
    read_k = pltpu.make_async_copy(kc_ref, k_s, loc_sem.at[4])
    read_k.start()
    read_v = pltpu.make_async_copy(vc_ref, v_s, loc_sem.at[5])
    read_v.start()
    stage[:] = jnp.zeros_like(stage)
    for read in reads[:2]:
        read.wait()
    stage[grp:grp + 1, :grp] = gain_ref[:].astype(f32)
    at.greeted()
    copies, late = Copies(any_peer), Copies(any_peer)

    def send(src, dst, sems, idx, peer):
        copies.send(src, dst, sems[0].at[idx], sems[1].at[idx], peer)

    def arrived(region, sems, idx):
        copies.arrived(region, sems[0].at[idx], sems[1].at[idx])

    for d in (*range(1, xs), 0):
        to = (at.x + d) % xs
        stage[:grp, :] = x_ref[:, pl.ds(pl.multiple_of(to * rows, 128), rows)].astype(f32)
        x_send[to] = stage[:].astype(bf16)
        if d:
            send(x_send.at[to], xg.at[at.x, at.j], xsem, d - 1, at.on_x(to))
    own_x = pltpu.make_async_copy(x_send.at[at.x], xg.at[at.x, at.j], loc_sem.at[0])
    own_x.start()
    for read in reads[2:]:
        read.wait()

    n1 = w1.shape[0]

    def w1_at(x, k=None):
        cols = pl.ds(pl.multiple_of(x * kx, 128), kx)
        return w1.at[:, cols] if k is None else w1.at[pl.ds(k * (n1 // 2), n1 // 2), cols]

    own_cols = pl.ds(pl.multiple_of(at.x * kx, 128), kx)
    tall[k_loc:, :] = jnp.zeros((tall.shape[0] - k_loc, tall.shape[1]), f32)
    row = 0
    for ref in (wq_ref, wg_ref, wu_ref):
        w = ref[:].astype(f32)
        w = w.T if ref is wq_ref else w
        n = w.shape[1]
        tall[:k_loc, :n] = w
        for j in range(yzs):
            wide_s[j * gp:(j + 1) * gp, :n] = tall[j * grp:j * grp + gp, :n]
        w1[row:row + n, own_cols] = wide_s[:, :n].T.astype(bf16)
        row += n
    spread_own(copies, at, w1_at, wsem)
    own_x.wait()
    for d in range(1, xs):
        arrived(xg.at[(at.x + xs - d) % xs, at.j], xsem, d - 1)

    order = ("y", "z")
    halves = range(len(order))
    first_axis, second_axis = halves
    slot_up, slot_down, slot_far = RING, 2 * RING, 3 * RING

    def region(s, df, dg, lo=0, n=half):
        return xg.at[pl.ds(s * half + lo, n), at.axis_block(order[s], df, dg)]

    def pass_rows(s, df, dg, axis, d, slot, lo=0, n=half):
        r = region(s, df, dg, lo, n)
        send(r, r, (gsem[0].at[s], gsem[1].at[s]), slot, at.step(order[s], axis, d))

    def rows_in(s, df, dg, slot, lo=0, n=half):
        arrived(region(s, df, dg, lo, n), (gsem[0].at[s], gsem[1].at[s]), slot)

    def both_ways(s, df):
        pass_rows(s, df, 0, second_axis, UP, slot_up + df)
        pass_rows(s, df, 0, second_axis, DOWN, slot_down + df)

    for s in halves:
        pass_rows(s, 0, 0, first_axis, UP, 0)
        pass_rows(s, 0, 0, first_axis, DOWN, 1)
        both_ways(s, 0)
    xo[:] = xg[:, at.j]
    narrow[:c_f, :] = wm_ref[:].astype(f32)
    narrow[c_f:, :] = wa_ref[:].astype(f32)
    tall[:k_loc, :] = narrow[:].T
    for j in range(yzs):
        w2v[j, at.x] = tall[j * grp:j * grp + gp, :].astype(bf16)
    head_dim = k_s.shape[2]
    request = lax.broadcasted_iota(jnp.int32, (dev_rows, head_dim), 0)
    lane = lax.broadcasted_iota(jnp.int32, (dev_rows, head_dim), 1)

    def place(b, p):
        return jnp.where(request == b, len_ref[b].astype(f32), p)

    angles = lax.fori_loop(0, dev_rows, place, jnp.zeros((dev_rows, head_dim), f32), unroll=8) * freq_ref[:]
    cos_s[:] = jnp.cos(angles)
    sin_s[:] = jnp.where(lane < head_dim // 2, -1.0, 1.0) * jnp.sin(angles)
    for s in halves:
        rows_in(s, DOWN, 0, 0)
        pass_rows(s, DOWN, 0, first_axis, UP, FAR, 0, quarter)
        rows_in(s, UP, 0, 1)
        pass_rows(s, UP, 0, first_axis, DOWN, DOWN, quarter, quarter)
        both_ways(s, DOWN)
        both_ways(s, UP)
    for s in halves:
        rows_in(s, FAR, 0, FAR, 0, quarter)
        rows_in(s, FAR, 0, DOWN, quarter, quarter)
        both_ways(s, FAR)
    forward_half(copies, at, w1_at, wsem)
    spread_own(late, at, w2_at, vsem)

    diagonal = lax.broadcasted_iota(jnp.int32, (gp, 128), 0) == lax.broadcasted_iota(jnp.int32, (gp, 128), 1)
    feature = lax.broadcasted_iota(jnp.int32, (gp, 1), 0)

    def add_up(s, dg, sums):
        def body(i, c):
            x, j = s * half + i // RING, at.axis_block(order[s], i % RING, dg)
            raw = xg[x, j].astype(f32)
            col = jnp.sum(jnp.where(diagonal, raw[grp:grp + 1, :128], 0.0), axis=1, keepdims=True)
            gcol[x, j] = jnp.broadcast_to(col, (gp, 128))
            parts = jnp.where(feature < grp, raw, 0.0).reshape(gp // 8, 8, rows)
            return c[0] + jnp.sum(parts, axis=0), c[1] + jnp.sum(parts * parts, axis=0)

        return lax.fori_loop(0, half * RING, body, sums, unroll=4)

    sums = (jnp.zeros((8, rows), f32), jnp.zeros((8, rows), f32))
    for s in halves:
        sums = add_up(s, 0, sums)
    for s in halves:
        for df in (0, DOWN):
            rows_in(s, df, DOWN, slot_up + df)
            pass_rows(s, df, DOWN, second_axis, UP, slot_far + df)
    share_near(copies, at, w1_at, wsem)
    for s in halves:
        for df in (UP, FAR):
            rows_in(s, df, UP, slot_down + df)
            pass_rows(s, df, UP, second_axis, DOWN, slot_far + df)
    for s in halves:
        for df in (UP, FAR):
            rows_in(s, df, DOWN, slot_up + df)
        for df in (0, DOWN):
            rows_in(s, df, UP, slot_down + df)
    for dg in (DOWN, UP):
        for s in halves:
            sums = add_up(s, dg, sums)
    for s in halves:
        for df in range(RING):
            rows_in(s, df, FAR, slot_far + df)
        sums = add_up(s, FAR, sums)

    pairs = yzs // 2
    real = lax.broadcasted_iota(jnp.int32, (2, gp, 1), 1).reshape(2 * gp, 1) < grp
    s1, s2 = sums
    d_model = grp * xs * yzs
    mean = jnp.sum(s1, axis=0, keepdims=True) / d_model
    var = jnp.sum(s2, axis=0, keepdims=True) / d_model - mean * mean
    scale = lax.rsqrt(var + 1e-6)

    def normalize(q, c):
        at_q = q // pairs, pl.ds((q % pairs) * 2, 2)
        gain = jnp.concatenate([gcol[at_q].reshape(2 * gp, 128)] * (rows // 128), axis=1)
        out = jnp.where(real, (xg[at_q].astype(f32).reshape(2 * gp, rows) - mean) * scale * gain, 0.0)
        h[pl.ds(pl.multiple_of(q * 2 * gp, 16), 2 * gp), :] = out.astype(bf16)
        return c

    some = xs * pairs // 2
    lax.fori_loop(0, some, normalize, 0, unroll=2)
    share_far(copies, at, w1_at, wsem)
    lax.fori_loop(some, xs * pairs, normalize, 0, unroll=2)
    all_in(copies, at, w1_at, wsem)

    nt = 256

    def query(n, c):
        q = jnp.dot(w1[:c_q], h[:, pl.ds(pl.multiple_of(n * nt, nt), nt)], preferred_element_type=f32)
        q = q.T
        for i in range(nt // dev_rows):
            to = n * (nt // dev_rows) + i
            for k in range(2):
                piece = q[i * dev_rows + k * part:i * dev_rows + (k + 1) * part]
                qkv_s[k, to, :part] = piece[:, :128].astype(bf16)
                qkv_s[k, to, part:] = jnp.concatenate([piece[:part // 2, 128:], piece[part // 2:, 128:]], axis=1).astype(bf16)
        return c

    def unpacked(k, j):
        piece = qkv_in[k, j].astype(f32)
        rest = piece[part:]
        rest = jnp.concatenate([rest[:, :c_q - 128], rest[:, c_q - 128:]], axis=0)
        return jnp.concatenate([piece[:part], rest], axis=1)

    part = dev_rows // 2
    lax.fori_loop(0, rows // nt, query, 0)
    own_q = []
    for k in range(2):
        own = pltpu.make_async_copy(qkv_s.at[k, at.j], qkv_in.at[k, at.j], loc_sem.at[2 + k])
        own.start()
        own_q.append(own)
        for d in range(1, yzs):
            to = (at.j + d) % yzs
            send(qkv_s.at[k, to], qkv_in.at[k, at.j], (qsem[0].at[k], qsem[1].at[k]), d - 1, at.on_yz(to))

    def mlp(n, c):
        cols = pl.ds(pl.multiple_of(n * nt, nt), nt)
        gate = jnp.dot(w1[c_q:c_q + c_f], h[:, cols], preferred_element_type=f32).astype(bf16).astype(f32)
        up = jnp.dot(w1[c_q + c_f:], h[:, cols], preferred_element_type=f32).astype(bf16).astype(f32)
        act[pl.ds(0, c_f), cols] = (jax.nn.silu(gate) * up).astype(bf16)
        return c

    steps = rows // nt
    lax.fori_loop(0, steps // 2, mlp, 0)
    forward_half(late, at, w2_at, vsem)

    per = 2 * c_q // head_dim

    def rotate(k):
        take = pl.ds(k * part, part)
        for p in range(yzs // 2):
            both = jnp.concatenate([unpacked(k, 2 * p), unpacked(k, 2 * p + 1)], axis=1)
            for i in range(per):
                hd = p * per + i
                u = both[:, i * head_dim:(i + 1) * head_dim]
                if hd <= num_heads:
                    u = u * cos_s[take, :] + pltpu.roll(u, head_dim // 2, 1) * sin_s[take, :]
                    u = u.astype(bf16).astype(f32)
                heads[hd, take, :] = u

    group = 8
    t_len = k_s.shape[1]
    hp = heads.shape[0]
    position = lax.broadcasted_iota(jnp.int32, (t_len, head_dim), 0)
    along = lax.broadcasted_iota(jnp.int32, (hp, t_len), 1)

    def attend(g, c):
        first = pl.multiple_of(g * group, group)
        block = jnp.swapaxes(heads[:, pl.ds(first, group), :], 0, 1)
        scores, keys, values = [], [], []
        for i in range(group):
            b = first + i
            last = len_ref[b]
            mine = block[i]
            slot = position == last
            kb, vb = [
                jnp.where(slot, mine[row:row + 1], old[b].astype(f32)).astype(bf16)
                for row, old in ((num_heads, k_s), (num_heads + 1, v_s))
            ]
            keys.append(kb)
            values.append(vb)
            score = lax.dot_general(mine.astype(bf16), kb, (((1,), (1,)), ((), ())), preferred_element_type=f32) * head_dim ** -0.5
            scores.append(jnp.where(along <= last, score, -1e30))
        for i in range(group):
            k_s[first + i] = keys[i]
            v_s[first + i] = values[i]
        scores = jnp.concatenate(scores, axis=0)
        e = jnp.exp(scores - jnp.max(scores, axis=1, keepdims=True))
        probs = (e / jnp.sum(e, axis=1, keepdims=True)).reshape(group, hp, t_len).astype(bf16)
        outs = [jnp.dot(probs[i], values[i], preferred_element_type=f32) for i in range(group)]
        heads[:, pl.ds(first, group), :] = jnp.swapaxes(jnp.stack(outs, axis=0), 0, 1)
        return c

    read_k.wait()
    read_v.wait()
    for k in range(2):
        for d in range(1, yzs):
            arrived(qkv_in.at[k, (at.j + yzs - d) % yzs], (qsem[0].at[k], qsem[1].at[k]), d - 1)
        own_q[k].wait()
        rotate(k)
        lax.fori_loop(k * part // group, (k + 1) * part // group, attend, 0)
        take = pl.ds(k * part, part)
        for jj in range(yzs):
            lo, hi = jj * c_a // head_dim, ((jj + 1) * c_a - 1) // head_dim + 1
            wide = jnp.concatenate([heads[hd, take, :] for hd in range(lo, hi)], axis=1)
            start = jj * c_a - lo * head_dim
            o_send[k, jj] = wide[:, start:start + c_a].astype(bf16)
        o_own(k).start()
        for d in range(1, yzs):
            o_copy(k, d).start()
    for write in cache_writes():
        write.start()
    share_near(late, at, w2_at, vsem)
    lax.fori_loop(steps // 2, steps, mlp, 0)
    copies.finish()


def second_phase(
    xs, yzs, grp, at, any_peer, finish_first, finish_last, w2v, act, xo, y_ref,
    loc_sem, sem1, sem2, sem3, sem4, ysem, ready, zb, r1, r2, r3, r4, yv, ws,
):
    for d in (UP, DOWN):
        for peer in (at.block(d, 0), at.block(0, d)):
            pl.semaphore_signal(ready, inc=1, device_id=at.on_yz(peer), device_id_type=MESH)
    yv[:] = jnp.zeros_like(yv)
    late = finish_first()
    (s1, q1), (s2, q2), (s3, q3), (s4, q4), (ys, yq) = sem1, sem2, sem3, sem4, ysem
    order = ("z", "y")
    hr = zb.shape[2] // 2
    copies = Copies(any_peer)
    send, arrived = copies.send, copies.arrived

    def zat(h, df, dg):
        dz, dy = (df, dg) if order[h] == "z" else (dg, df)
        return zb.at[dz, dy, pl.ds(h * hr, hr)]

    def compute(dz, dy):
        w = w2v[at.block(dz, dy)].astype(jnp.float32)
        for x in range(xs):
            ws[pl.ds(x * grp, grp), :] = w[x, :grp]
        zb[dz, dy] = jnp.dot(ws[:].astype(jnp.bfloat16), act[:], preferred_element_type=jnp.float32)

    def send1(h, dg):
        d = 1 if dg < 2 else 3
        send(zat(h, 2, dg), r1.at[h, dg], s1.at[h, dg], q1.at[h, dg], at.step(order[h], 0, d))

    compute(2, 2)
    pl.semaphore_wait(ready, RING)
    send1(0, 2)
    send1(1, 2)
    for k in (0, 1, 3):
        compute(2, k)
        send1(0, k)
        compute(k, 2)
        send1(1, k)

    def second(i, c):
        k, m = i // 3, i % 3
        compute(k + k // 2, m + m // 2)
        return c

    lax.fori_loop(0, 9, second, 0)

    def send2(h, up, dg):
        df, d, s = (1, 1, 0) if up else (3, 3, 1)
        send(zat(h, df, dg), r2.at[h, s, dg], s2.at[h, s, dg], q2.at[h, s, dg], at.step(order[h], 0, d))

    for h in range(2):
        for dg in (2, 3):
            send2(h, True, dg)
        for dg in (0, 1):
            send2(h, False, dg)
    for k in range(2):
        for h in range(2):
            for up in (True, False):
                dg = 1 - k if up else 2 + k
                arrived(r1.at[h, dg], s1.at[h, dg], q1.at[h, dg])
                ref = zat(h, 1 if up else 3, dg)
                ref[:] = ref[:] + r1[h, dg]
                send2(h, up, dg)

    def plane(h, dg):
        for s in range(2):
            arrived(r2.at[h, s, dg], s2.at[h, s, dg], q2.at[h, s, dg])
        ref = zat(h, 0, dg)
        ref[:] = ref[:] + r2[h, 0, dg] + r2[h, 1, dg]

    big = r3.shape[2]
    sizes = (big, hr - big)

    def part(h, dg, k):
        dz, dy = (0, dg) if order[h] == "z" else (dg, 0)
        return zb.at[dz, dy, pl.ds(h * hr + k * big, sizes[k])]

    def r3_at(h, k):
        return r3.at[h, k, pl.ds(0, sizes[k])]

    def r4_at(h, s, k):
        return r4.at[h, s, k, pl.ds(0, sizes[k])]

    def send4(h, up, k):
        dg, d, s = (1, 1, 0) if up else (3, 3, 1)
        send(part(h, dg, k), r4_at(h, s, k), s4.at[h, s, k], q4.at[h, s, k], at.step(order[h], 1, d))

    for h in range(2):
        plane(h, 2)
        send(part(h, 2, 0), r3_at(h, 0), s3.at[h, 0], q3.at[h, 0], at.step(order[h], 1, 1))
        send(part(h, 2, 1), r3_at(h, 1), s3.at[h, 1], q3.at[h, 1], at.step(order[h], 1, 3))
    for h in range(2):
        plane(h, 1)
        send4(h, True, 1)
        plane(h, 3)
        send4(h, False, 0)
    for h in range(2):
        plane(h, 0)
    for h in range(2):
        arrived(r3_at(h, 0), s3.at[h, 0], q3.at[h, 0])
        ref = part(h, 1, 0)
        ref[:] = ref[:] + r3_at(h, 0)[:]
        send4(h, True, 0)
        arrived(r3_at(h, 1), s3.at[h, 1], q3.at[h, 1])
        ref = part(h, 3, 1)
        ref[:] = ref[:] + r3_at(h, 1)[:]
        send4(h, False, 1)
    def y_cols(x):
        rows = yv.shape[2]
        return y_ref.at[:, pl.ds(pl.multiple_of(x * rows, 128), rows)]

    def y_copy(x, d):
        return pltpu.make_async_remote_copy(
            src_ref=yv.at[x], dst_ref=y_cols(at.x), send_sem=ys.at[d - 1], recv_sem=yq.at[d - 1], device_id=at.on_x(x), device_id_type=MESH
        )

    for h in range(2):
        for k in range(2):
            for s in range(2):
                arrived(r4_at(h, s, k), s4.at[h, s, k], q4.at[h, s, k])
            ref = part(h, 0, k)
            ref[:] = ref[:] + r4_at(h, 0, k)[:] + r4_at(h, 1, k)[:]
            done = xs // 4
            for x in range((2 * h + k) * done, (2 * h + k + 1) * done):
                z = zb[0, 0, pl.ds(x * grp, grp), :]
                yv[x, :grp, :] = (xo[x, :grp, :].astype(jnp.float32) + z).astype(jnp.bfloat16)
                d = lax.rem(x - at.x + xs, xs)

                @pl.when(d == 0)
                def _():
                    pltpu.make_async_copy(yv.at[x], y_cols(x), loc_sem.at[3]).start()

                @pl.when(d != 0)
                def _():
                    y_copy(x, d).start()

    for d in range(1, xs):
        arrived(y_cols((at.x + xs - d) % xs), ys.at[d - 1], yq.at[d - 1])
    pltpu.make_async_copy(yv.at[at.x], y_cols(at.x), loc_sem.at[3]).wait()
    for d in range(1, xs):
        y_copy((at.x + d) % xs, d).wait_send()
    copies.finish()
    finish_last(late)


def layer(x_t, gain, weights, freq, k_cache, v_cache, ctx_len, xs, yzs, gp):
    n_rows = x_t.shape[1]
    rows = n_rows // xs
    dev_rows = k_cache.shape[0]
    c_a, c_f = weights[3].shape[0], weights[4].shape[0]
    n2 = c_a + c_f
    dma, vmem = pltpu.SemaphoreType.DMA, pltpu.VMEM
    bf16 = jnp.bfloat16
    aspec = pl.BlockSpec(memory_space=pl.ANY)
    sems = lambda *shape: [dma(shape), dma(shape)]
    cache = jax.ShapeDtypeStruct(k_cache.shape, bf16)
    return pl.pallas_call(
        functools.partial(layer_kernel, xs, yzs, gp),
        out_shape=(jax.ShapeDtypeStruct((gp, n_rows), bf16), cache, cache),
        in_specs=[aspec] * 11,
        out_specs=(aspec, aspec, aspec),
        scratch_shapes=[
            vmem((n2, rows), bf16),
            vmem((yzs, xs, gp, n2), bf16),
            vmem((xs, gp, rows), bf16),
            vmem(k_cache.shape, bf16),
            vmem(k_cache.shape, bf16),
            vmem((2, yzs, dev_rows // 2, c_a), bf16),
            vmem((rows, c_a), bf16),
            dma((8,)),
        ]
        + sems(xs - 1) + sems(2, RING * RING) + sems(11) + sems(11) + sems(2, yzs - 1) + sems(2, yzs - 1)
        + sems(2, RING) + sems(2, 2, RING) + sems(2, 2) + sems(2, 2, 2) + sems(xs - 1)
        + [pltpu.SemaphoreType.REGULAR],
        compiler_params=pltpu.CompilerParams(collective_id=0, has_side_effects=True, vmem_limit_bytes=VMEM_LIMIT),
        name="layer",
    )(ctx_len, x_t, gain, *weights, freq, k_cache, v_cache)


def results_kernel(chunks, y_ref, k_ref, v_ref, yo_ref, ko_ref, vo_ref, y_in, y_out, k_s, v_s, y_sem, in_sem, out_sem):
    n = k_s.shape[0] // chunks
    y_read = pltpu.make_async_copy(y_ref, y_in, y_sem.at[0])
    y_read.start()
    copies = []
    for c in range(chunks):
        for i, (src, buf, dst) in enumerate(((k_ref, k_s, ko_ref), (v_ref, v_s, vo_ref))):
            take = pl.ds(c * n, n)
            read = pltpu.make_async_copy(src.at[take], buf.at[take], in_sem.at[i, c])
            read.start()
            copies.append((read, pltpu.make_async_copy(buf.at[take], dst.at[take], out_sem.at[i, c])))
    y_read.wait()
    y_out[:] = y_in[:y_out.shape[0], :]
    y_write = pltpu.make_async_copy(y_out, yo_ref, y_sem.at[1])
    y_write.start()
    for read, write in copies:
        read.wait()
        write.start()
    y_write.wait()
    for _, write in copies:
        write.wait()


def results(y_t, k_all, v_all, grp):
    chunks = 4
    dma, vmem = pltpu.SemaphoreType.DMA, pltpu.VMEM
    aspec = pl.BlockSpec(memory_space=pl.ANY)
    shapes = ((grp, y_t.shape[1]), k_all.shape, v_all.shape)
    return pl.pallas_call(
        functools.partial(results_kernel, chunks),
        out_shape=tuple(jax.ShapeDtypeStruct(shape, y_t.dtype) for shape in shapes),
        in_specs=[aspec] * 3,
        out_specs=(aspec,) * 3,
        scratch_shapes=[vmem(shape, y_t.dtype) for shape in (y_t.shape,) + shapes] + [dma((2,)), dma((2, chunks)), dma((2, chunks))],
        compiler_params=pltpu.CompilerParams(vmem_limit_bytes=VMEM_LIMIT),
        name="results",
    )(y_t, k_all, v_all)


def solution(mesh):
    xs = mesh.shape["x"]
    yzs = mesh.shape["yz"]
    both_axes = ("x", "yz")
    row_spec = P("dp", both_axes)
    in_w_spec = P("x", "yz")
    out_w_spec = P("yz", "x")
    cache_spec = P(("dp", "x", "yz"), None, None)
    len_spec = P(("dp", "x", "yz"))

    def local_layer(x_loc, gain_loc, wqkv_loc, wgate_loc, wup_loc, wao_loc, wmo_loc, kc_loc, vc_loc, len_loc):
        grp = x_loc.shape[1]
        gp = grp + -grp % 8
        freq = rope_frequencies(kc_loc.shape[2])
        weights = (wqkv_loc.T, wgate_loc, wup_loc, wao_loc, wmo_loc)
        y_t, k_all, v_all = layer(x_loc.T, gain_loc.reshape(1, grp), weights, freq, kc_loc, vc_loc, len_loc, xs, yzs, gp)
        y_t, k_all, v_all = results(y_t, k_all, v_all, grp)
        return y_t.T, k_all, v_all

    in_specs = (row_spec, P(both_axes), in_w_spec, in_w_spec, in_w_spec, out_w_spec, out_w_spec, cache_spec, cache_spec, len_spec)
    out_specs = (row_spec, cache_spec, cache_spec)
    return jax.shard_map(local_layer, mesh=mesh, in_specs=in_specs, out_specs=out_specs, check_vma=False)
```

```python
import functools

import jax
import jax.numpy as jnp
import numpy as np
from jax import lax
from jax.experimental import pallas as pl
from jax.experimental.pallas import tpu as pltpu
from jax.sharding import PartitionSpec as P

MESH = pl.DeviceIdType.MESH
RING = 4
UP, FAR, DOWN = 1, 2, 3
VMEM_LIMIT = 62 * 1024 * 1024


def rope_frequencies(head_dim):
    half_dim = head_dim // 2
    inv_freq = np.float32(10000.0) ** (-np.arange(half_dim, dtype=np.float32) / np.float32(half_dim))
    return jnp.asarray(np.concatenate([inv_freq, inv_freq])[None, :])


class Where:
    def __init__(self, xs, yzs):
        self.xs = xs
        self.yzs = yzs
        self.dp = lax.axis_index("dp")
        self.x = lax.axis_index("x")
        self.j = lax.axis_index("yz")
        self.zz = self.j // RING
        self.yy = self.j % RING
        self.chip = self.x // 2
        self.core = self.x % 2

    def block(self, dz, dy):
        return ((self.zz + dz) % RING) * RING + (self.yy + dy) % RING

    def on_yz(self, j):
        return (self.dp, j, self.x)

    def on_x(self, x):
        return (self.dp, self.j, x)

    def axis_block(self, first, df, dg):
        return self.block(df, dg) if first == "z" else self.block(dg, df)

    def step(self, first, axis, d):
        return self.on_yz(self.axis_block(first, d, 0) if axis == 0 else self.axis_block(first, 0, d))

    def x_of(self, dc):
        return ((self.chip + dc) % RING) * 2 + self.core

    def x_other(self, dc):
        return ((self.chip + dc) % RING) * 2 + (1 - self.core)

    def peers(self):
        on_x = [self.on_x((self.x + d) % self.xs) for d in range(1, self.xs)]
        return on_x + [self.on_yz((self.j + d) % self.yzs) for d in range(1, self.yzs)]

    def greet(self):
        for peer in self.peers():
            pl.semaphore_signal(pltpu.get_barrier_semaphore(), inc=1, device_id=peer, device_id_type=MESH)

    def greeted(self):
        pl.semaphore_wait(pltpu.get_barrier_semaphore(), len(self.peers()))


class Copies:
    def __init__(self, any_peer):
        self.any_peer = any_peer
        self.started = []

    def send(self, src, dst, ssem, rsem, peer):
        copy = pltpu.make_async_remote_copy(src_ref=src, dst_ref=dst, send_sem=ssem, recv_sem=rsem, device_id=peer, device_id_type=MESH)
        copy.start()
        self.started.append(copy)

    def arrived(self, dst, ssem, rsem):
        pltpu.make_async_remote_copy(
            src_ref=dst, dst_ref=dst, send_sem=ssem, recv_sem=rsem, device_id=self.any_peer, device_id_type=MESH
        ).wait_recv()

    def sent(self, src, ssem, rsem):
        remote(src, src, ssem, rsem, self.any_peer).wait_send()

    def finish(self):
        for copy in self.started:
            copy.wait_send()


def layer_kernel(
    xs, yzs, gp, len_ref, x_ref, gain_ref, wq_ref, wg_ref, wu_ref, wa_ref, wm_ref, freq_ref, kc_ref, vc_ref,
    y_ref, ko_ref, vo_ref,
    act, w2v, xo, k_s, v_s, o_send, ob,
    loc_sem, xsend, xrecv, gsend, grecv, wsend, wrecv, vsend, vrecv, qsend, qrecv, osend, orecv,
    ys, yq, ready,
):
    f32, bf16 = jnp.float32, jnp.bfloat16
    dma, vmem = pltpu.SemaphoreType.DMA, pltpu.VMEM
    grp = x_ref.shape[0]
    rows, c_a = ob.shape
    dev_rows, t_len, head_dim = k_s.shape
    c_q, k_loc = wq_ref.shape
    n1 = c_q + 2 * wg_ref.shape[1]
    c_f = wm_ref.shape[0]
    num_heads = yzs * c_a // head_dim
    part = dev_rows // 2
    block = xs * grp
    hr = block // 2
    at = Where(xs, yzs)
    any_peer = at.on_yz(at.block(0, UP))

    def w2_at(x, k=None):
        n2 = w2v.shape[0]
        return w2v.at[:, x] if k is None else w2v.at[pl.ds(k * (n2 // 2), n2 // 2), x]

    def o_rows(j, k):
        return ob.at[pl.ds(pl.multiple_of(j * dev_rows + k * part, part), part)]

    def o_copy(k, d):
        to = (at.j + d) % yzs
        return remote(o_send.at[k, to], o_rows(at.j, k), osend.at[k], orecv.at[k], at.on_yz(to))

    def o_own(k):
        return pltpu.make_async_copy(o_send.at[k, at.j], o_rows(at.j, k), loc_sem.at[6 + k])

    def cache_writes():
        return [pltpu.make_async_copy(src, dst, loc_sem.at[loc]) for src, dst, loc in ((k_s, ko_ref, 4), (v_s, vo_ref, 5))]

    gather_and_attend = functools.partial(
        first_phase, xs, yzs, num_heads, at, any_peer, w2_at, o_copy, o_own, cache_writes,
        len_ref, x_ref, gain_ref, wq_ref, wg_ref, wu_ref, wa_ref, wm_ref, freq_ref, kc_ref, vc_ref,
        act, w2v, xo, k_s, v_s, o_send,
        loc_sem, (xsend, xrecv), (gsend, grecv), (wsend, wrecv), (vsend, vrecv), (qsend, qrecv),
    )
    pl.run_scoped(
        gather_and_attend,
        vmem((xs, yzs, gp, rows), bf16),
        vmem((xs * yzs * gp, rows), bf16),
        vmem((xs, yzs, gp, 128), f32),
        vmem((n1, xs * yzs * gp), bf16),
        vmem((2, yzs, part + part // 2, 128), bf16),
        vmem((2, yzs, part + part // 2, 128), bf16),
        vmem((num_heads + 2, dev_rows, head_dim), f32),
        vmem((xs, gp, rows), bf16),
        vmem((gp, rows), f32),
        vmem((k_loc + 8, c_f + c_a), f32),
        vmem((yzs * gp, c_f), f32),
        vmem((c_f + c_a, k_loc), f32),
        vmem((dev_rows, head_dim), f32),
        vmem((dev_rows, head_dim), f32),
        *[vmem(ref.shape, ref.dtype) for ref in (x_ref, gain_ref, wq_ref, wg_ref, wu_ref, wa_ref, wm_ref, freq_ref)],
        pltpu.SMEM(len_ref.shape, len_ref.dtype),
        dma((9,)),
    )

    def finish_first():
        late = Copies(any_peer)
        share_far(late, at, w2_at, (vsend, vrecv))
        for k in range(2):
            late.arrived(ob.at[pl.ds(0, (yzs - 1) * part)], osend.at[k], orecv.at[k])
            o_own(k).wait()
        act[pl.ds(c_f, c_a), :] = ob[:].T
        all_in(late, at, w2_at, (vsend, vrecv))
        return late

    def finish_last(late):
        for write in cache_writes():
            write.wait()
        for k in range(2):
            late.sent(o_send.at[k, pl.ds(0, yzs - 1)], osend.at[k], orecv.at[k])
        for slot in range(9):
            r = w2_at(at.x, None if slot in (4, 7, 8) else 0)
            remote(r, r, vsend.at[slot], vrecv.at[slot], any_peer).wait_send()
        late.finish()

    sum_and_return = functools.partial(
        second_phase, xs, yzs, grp, at, any_peer, finish_first, finish_last, w2v, act, xo, y_ref,
        loc_sem, (gsend, grecv), (ys, yq), ready,
    )
    big = hr // 2 + hr // 2 % 8
    pl.run_scoped(
        sum_and_return,
        vmem((RING, RING, block, rows), f32),
        vmem((2, RING, hr, rows), f32),
        vmem((2, 2, RING, hr, rows), f32),
        vmem((2, 2, big, rows), f32),
        vmem((2, 2, 2, big, rows), f32),
        vmem((xs, gp, rows), bf16),
        vmem((block, w2v.shape[3]), f32),
    )


def remote(src, dst, ssem, rsem, peer):
    return pltpu.make_async_remote_copy(src_ref=src, dst_ref=dst, send_sem=ssem, recv_sem=rsem, device_id=peer, device_id_type=MESH)


def spread_own(copies, at, region, sems):
    def send(slot, k, x):
        r = region(at.x, k)
        copies.send(r, r, sems[0].at[slot], sems[1].at[slot], at.on_x(x))

    for k in range(2):
        send(2 * k, k, at.x_of(UP))
        send(2 * k + 1, 1 - k, at.x_of(DOWN))
    send(4, None, at.x_other(0))


def pass_on(copies, at, r, sems, slot, x):
    copies.send(r, r, sems[0].at[slot], sems[1].at[slot], at.on_x(x))


def block_in(copies, r, sems, slot):
    copies.arrived(r, sems[0].at[slot], sems[1].at[slot])


def forward_half(copies, at, region, sems):
    for slot, k, here, to in ((0, 0, DOWN, UP), (1, 1, UP, DOWN)):
        r = region(at.x_of(here), k)
        block_in(copies, r, sems, slot)
        pass_on(copies, at, r, sems, slot + 5, at.x_of(to))


def share_near(copies, at, region, sems):
    for slot, k, here in ((2, 1, DOWN), (3, 0, UP)):
        block_in(copies, region(at.x_of(here), k), sems, slot)
        pass_on(copies, at, region(at.x_of(here)), sems, slot + 5, at.x_other(0))


def share_far(copies, at, region, sems):
    for k in range(2):
        r = region(at.x_of(FAR), k)
        block_in(copies, r, sems, 5 + k)
        pass_on(copies, at, r, sems, 9 + k, at.x_other(0))


def all_in(copies, at, region, sems):
    for slot, here in ((4, 0), (7, DOWN), (8, UP)):
        block_in(copies, region(at.x_other(here)), sems, slot)
    for k in range(2):
        block_in(copies, region(at.x_other(FAR), k), sems, 9 + k)


def first_phase(
    xs, yzs, num_heads, at, any_peer, w2_at, o_copy, o_own, cache_writes,
    len_hbm, x_hbm, gain_hbm, wq_hbm, wg_hbm, wu_hbm, wa_hbm, wm_hbm, freq_hbm, kc_ref, vc_ref,
    act, w2v, xo, k_s, v_s, o_send,
    loc_sem, xsem, gsem, wsem, vsem, qsem, xg, h, gcol, w1, qkv_s, qkv_in, heads, x_send, stage, tall, wide_s, narrow, cos_s, sin_s,
    x_ref, gain_ref, wq_ref, wg_ref, wu_ref, wa_ref, wm_ref, freq_ref, len_ref, in_sem,
):
    f32, bf16 = jnp.float32, jnp.bfloat16
    half = xs // 2
    quarter = half // 2
    grp = x_ref.shape[0]
    _, gp, rows = x_send.shape
    dev_rows = rows // yzs
    c_q, k_loc = wq_ref.shape
    c_f, c_a = wm_ref.shape[0], wa_ref.shape[0]
    kx = yzs * gp
    at.greet()
    operands = ((x_hbm, x_ref), (gain_hbm, gain_ref), (wq_hbm, wq_ref), (wg_hbm, wg_ref), (wu_hbm, wu_ref), (wa_hbm, wa_ref), (wm_hbm, wm_ref), (freq_hbm, freq_ref), (len_hbm, len_ref))
    reads = [pltpu.make_async_copy(src, dst, in_sem.at[i]) for i, (src, dst) in enumerate(operands)]
    for read in reads:
        read.start()
    read_k = pltpu.make_async_copy(kc_ref, k_s, loc_sem.at[4])
    read_k.start()
    read_v = pltpu.make_async_copy(vc_ref, v_s, loc_sem.at[5])
    read_v.start()
    stage[:] = jnp.zeros_like(stage)
    for read in reads[:2]:
        read.wait()
    stage[grp:grp + 1, :grp] = gain_ref[:].astype(f32)
    at.greeted()
    copies, late = Copies(any_peer), Copies(any_peer)

    def send(src, dst, sems, idx, peer):
        copies.send(src, dst, sems[0].at[idx], sems[1].at[idx], peer)

    def arrived(region, sems, idx):
        copies.arrived(region, sems[0].at[idx], sems[1].at[idx])

    for d in (*range(1, xs), 0):
        to = (at.x + d) % xs
        stage[:grp, :] = x_ref[:, pl.ds(pl.multiple_of(to * rows, 128), rows)].astype(f32)
        x_send[to] = stage[:].astype(bf16)
        if d:
            remote(x_send.at[to], xg.at[at.x, at.j], xsem[0].at[0], xsem[1].at[0], at.on_x(to)).start()
    own_x = pltpu.make_async_copy(x_send.at[at.x], xg.at[at.x, at.j], loc_sem.at[0])
    own_x.start()
    for read in reads[2:]:
        read.wait()

    n1 = w1.shape[0]

    def w1_at(x, k=None):
        cols = pl.ds(pl.multiple_of(x * kx, 128), kx)
        return w1.at[:, cols] if k is None else w1.at[pl.ds(k * (n1 // 2), n1 // 2), cols]

    own_cols = pl.ds(pl.multiple_of(at.x * kx, 128), kx)
    tall[k_loc:, :] = jnp.zeros((tall.shape[0] - k_loc, tall.shape[1]), f32)
    row = 0
    for ref in (wq_ref, wg_ref, wu_ref):
        w = ref[:].astype(f32)
        w = w.T if ref is wq_ref else w
        n = w.shape[1]
        tall[:k_loc, :n] = w
        for j in range(yzs):
            wide_s[j * gp:(j + 1) * gp, :n] = tall[j * grp:j * grp + gp, :n]
        w1[row:row + n, own_cols] = wide_s[:, :n].T.astype(bf16)
        row += n
    spread_own(copies, at, w1_at, wsem)
    own_x.wait()
    arrived(xg.at[pl.ds(0, xs - 1), at.j], xsem, 0)
    copies.sent(x_send.at[pl.ds(0, xs - 1)], xsem[0].at[0], xsem[1].at[0])

    order = ("y", "z")
    halves = range(len(order))
    first_axis, second_axis = halves
    slot_up, slot_down, slot_far = RING, 2 * RING, 3 * RING

    def region(s, df, dg, lo=0, n=half):
        return xg.at[pl.ds(s * half + lo, n), at.axis_block(order[s], df, dg)]

    def pass_rows(s, df, dg, axis, d, slot, lo=0, n=half):
        r = region(s, df, dg, lo, n)
        send(r, r, (gsem[0].at[s], gsem[1].at[s]), slot, at.step(order[s], axis, d))

    def rows_in(s, df, dg, slot, lo=0, n=half):
        arrived(region(s, df, dg, lo, n), (gsem[0].at[s], gsem[1].at[s]), slot)

    def both_ways(s, df):
        pass_rows(s, df, 0, second_axis, UP, slot_up + df)
        pass_rows(s, df, 0, second_axis, DOWN, slot_down + df)

    for s in halves:
        pass_rows(s, 0, 0, first_axis, UP, 0)
        pass_rows(s, 0, 0, first_axis, DOWN, 1)
        both_ways(s, 0)
    xo[:] = xg[:, at.j]
    narrow[:c_f, :] = wm_ref[:].astype(f32)
    narrow[c_f:, :] = wa_ref[:].astype(f32)
    tall[:k_loc, :] = narrow[:].T
    for j in range(yzs):
        w2v[j, at.x] = tall[j * grp:j * grp + gp, :].astype(bf16)
    head_dim = k_s.shape[2]
    request = lax.broadcasted_iota(jnp.int32, (dev_rows, head_dim), 0)
    lane = lax.broadcasted_iota(jnp.int32, (dev_rows, head_dim), 1)

    def place(b, p):
        return jnp.where(request == b, len_ref[b].astype(f32), p)

    angles = lax.fori_loop(0, dev_rows, place, jnp.zeros((dev_rows, head_dim), f32), unroll=8) * freq_ref[:]
    cos_s[:] = jnp.cos(angles)
    sin_s[:] = jnp.where(lane < head_dim // 2, -1.0, 1.0) * jnp.sin(angles)
    for s in halves:
        rows_in(s, DOWN, 0, 0)
        pass_rows(s, DOWN, 0, first_axis, UP, FAR, 0, quarter)
        rows_in(s, UP, 0, 1)
        pass_rows(s, UP, 0, first_axis, DOWN, DOWN, quarter, quarter)
        both_ways(s, DOWN)
        both_ways(s, UP)
    for s in halves:
        rows_in(s, FAR, 0, FAR, 0, quarter)
        rows_in(s, FAR, 0, DOWN, quarter, quarter)
        both_ways(s, FAR)
    forward_half(copies, at, w1_at, wsem)
    spread_own(late, at, w2_at, vsem)

    diagonal = lax.broadcasted_iota(jnp.int32, (gp, 128), 0) == lax.broadcasted_iota(jnp.int32, (gp, 128), 1)
    feature = lax.broadcasted_iota(jnp.int32, (gp, 1), 0)

    def add_up(s, dg, sums):
        def body(i, c):
            x, j = s * half + i // RING, at.axis_block(order[s], i % RING, dg)
            raw = xg[x, j].astype(f32)
            col = jnp.sum(jnp.where(diagonal, raw[grp:grp + 1, :128], 0.0), axis=1, keepdims=True)
            gcol[x, j] = jnp.broadcast_to(col, (gp, 128))
            parts = jnp.where(feature < grp, raw, 0.0).reshape(gp // 8, 8, rows)
            return c[0] + jnp.sum(parts, axis=0), c[1] + jnp.sum(parts * parts, axis=0)

        return lax.fori_loop(0, half * RING, body, sums, unroll=4)

    sums = (jnp.zeros((8, rows), f32), jnp.zeros((8, rows), f32))
    for s in halves:
        sums = add_up(s, 0, sums)
    for s in halves:
        for df in (0, DOWN):
            rows_in(s, df, DOWN, slot_up + df)
            pass_rows(s, df, DOWN, second_axis, UP, slot_far + df)
    share_near(copies, at, w1_at, wsem)
    for s in halves:
        for df in (UP, FAR):
            rows_in(s, df, UP, slot_down + df)
            pass_rows(s, df, UP, second_axis, DOWN, slot_far + df)
    for s in halves:
        for df in (UP, FAR):
            rows_in(s, df, DOWN, slot_up + df)
        for df in (0, DOWN):
            rows_in(s, df, UP, slot_down + df)
    for dg in (DOWN, UP):
        for s in halves:
            sums = add_up(s, dg, sums)
    for s in halves:
        for df in range(RING):
            rows_in(s, df, FAR, slot_far + df)
        sums = add_up(s, FAR, sums)

    pairs = yzs // 2
    real = lax.broadcasted_iota(jnp.int32, (2, gp, 1), 1).reshape(2 * gp, 1) < grp
    s1, s2 = sums
    d_model = grp * xs * yzs
    mean = jnp.sum(s1, axis=0, keepdims=True) / d_model
    var = jnp.sum(s2, axis=0, keepdims=True) / d_model - mean * mean
    scale = lax.rsqrt(var + 1e-6)

    def normalize(q, c):
        at_q = q // pairs, pl.ds((q % pairs) * 2, 2)
        gain = jnp.concatenate([gcol[at_q].reshape(2 * gp, 128)] * (rows // 128), axis=1)
        out = jnp.where(real, (xg[at_q].astype(f32).reshape(2 * gp, rows) - mean) * scale * gain, 0.0)
        h[pl.ds(pl.multiple_of(q * 2 * gp, 16), 2 * gp), :] = out.astype(bf16)
        return c

    some = xs * pairs // 2
    lax.fori_loop(0, some, normalize, 0, unroll=2)
    share_far(copies, at, w1_at, wsem)
    lax.fori_loop(some, xs * pairs, normalize, 0, unroll=2)
    all_in(copies, at, w1_at, wsem)

    nt = 256

    def query(n, c):
        q = jnp.dot(w1[:c_q], h[:, pl.ds(pl.multiple_of(n * nt, nt), nt)], preferred_element_type=f32)
        q = q.T
        for i in range(nt // dev_rows):
            to = n * (nt // dev_rows) + i
            for k in range(2):
                piece = q[i * dev_rows + k * part:i * dev_rows + (k + 1) * part]
                qkv_s[k, to, :part] = piece[:, :128].astype(bf16)
                qkv_s[k, to, part:] = jnp.concatenate([piece[:part // 2, 128:], piece[part // 2:, 128:]], axis=1).astype(bf16)
        return c

    def unpacked(k, j):
        piece = qkv_in[k, j].astype(f32)
        rest = piece[part:]
        rest = jnp.concatenate([rest[:, :c_q - 128], rest[:, c_q - 128:]], axis=0)
        return jnp.concatenate([piece[:part], rest], axis=1)

    part = dev_rows // 2
    lax.fori_loop(0, rows // nt, query, 0)
    own_q = []
    for k in range(2):
        own = pltpu.make_async_copy(qkv_s.at[k, at.j], qkv_in.at[k, at.j], loc_sem.at[2 + k])
        own.start()
        own_q.append(own)
        for d in range(1, yzs):
            to = (at.j + d) % yzs
            remote(qkv_s.at[k, to], qkv_in.at[k, at.j], qsem[0].at[k], qsem[1].at[k], at.on_yz(to)).start()

    def mlp(n, c):
        cols = pl.ds(pl.multiple_of(n * nt, nt), nt)
        gate = jnp.dot(w1[c_q:c_q + c_f], h[:, cols], preferred_element_type=f32).astype(bf16).astype(f32)
        up = jnp.dot(w1[c_q + c_f:], h[:, cols], preferred_element_type=f32).astype(bf16).astype(f32)
        act[pl.ds(0, c_f), cols] = (jax.nn.silu(gate) * up).astype(bf16)
        return c

    steps = rows // nt
    lax.fori_loop(0, steps // 2, mlp, 0)
    forward_half(late, at, w2_at, vsem)

    per = 2 * c_q // head_dim

    def rotate(k):
        take = pl.ds(k * part, part)
        for p in range(yzs // 2):
            both = jnp.concatenate([unpacked(k, 2 * p), unpacked(k, 2 * p + 1)], axis=1)
            for i in range(per):
                hd = p * per + i
                u = both[:, i * head_dim:(i + 1) * head_dim]
                if hd <= num_heads:
                    u = u * cos_s[take, :] + pltpu.roll(u, head_dim // 2, 1) * sin_s[take, :]
                    u = u.astype(bf16).astype(f32)
                heads[hd, take, :] = u

    group = 8
    t_len = k_s.shape[1]
    hp = heads.shape[0]
    position = lax.broadcasted_iota(jnp.int32, (t_len, head_dim), 0)
    along = lax.broadcasted_iota(jnp.int32, (hp, t_len), 1)

    def attend(g, c):
        first = pl.multiple_of(g * group, group)
        block = jnp.swapaxes(heads[:, pl.ds(first, group), :], 0, 1)
        scores, keys, values = [], [], []
        for i in range(group):
            b = first + i
            last = len_ref[b]
            mine = block[i]
            slot = position == last
            kb, vb = [
                jnp.where(slot, mine[row:row + 1], old[b].astype(f32)).astype(bf16)
                for row, old in ((num_heads, k_s), (num_heads + 1, v_s))
            ]
            keys.append(kb)
            values.append(vb)
            score = lax.dot_general(mine.astype(bf16), kb, (((1,), (1,)), ((), ())), preferred_element_type=f32) * head_dim ** -0.5
            scores.append(jnp.where(along <= last, score, -1e30))
        for i in range(group):
            k_s[first + i] = keys[i]
            v_s[first + i] = values[i]
        scores = jnp.concatenate(scores, axis=0)
        e = jnp.exp(scores - jnp.max(scores, axis=1, keepdims=True))
        probs = (e / jnp.sum(e, axis=1, keepdims=True)).reshape(group, hp, t_len).astype(bf16)
        outs = [jnp.dot(probs[i], values[i], preferred_element_type=f32) for i in range(group)]
        heads[:, pl.ds(first, group), :] = jnp.swapaxes(jnp.stack(outs, axis=0), 0, 1)
        return c

    read_k.wait()
    read_v.wait()
    for k in range(2):
        arrived(qkv_in.at[k, pl.ds(0, yzs - 1)], qsem, k)
        copies.sent(qkv_s.at[k, pl.ds(0, yzs - 1)], qsem[0].at[k], qsem[1].at[k])
        own_q[k].wait()
        rotate(k)
        lax.fori_loop(k * part // group, (k + 1) * part // group, attend, 0)
        take = pl.ds(k * part, part)
        for jj in range(yzs):
            lo, hi = jj * c_a // head_dim, ((jj + 1) * c_a - 1) // head_dim + 1
            wide = jnp.concatenate([heads[hd, take, :] for hd in range(lo, hi)], axis=1)
            start = jj * c_a - lo * head_dim
            o_send[k, jj] = wide[:, start:start + c_a].astype(bf16)
        o_own(k).start()
        for d in range(1, yzs):
            o_copy(k, d).start()
    for write in cache_writes():
        write.start()
    share_near(late, at, w2_at, vsem)
    lax.fori_loop(steps // 2, steps, mlp, 0)
    copies.finish()


def second_phase(
    xs, yzs, grp, at, any_peer, finish_first, finish_last, w2v, act, xo, y_ref,
    loc_sem, gsem, ysem, ready, zb, r1, r2, r3, r4, yv, ws,
):
    for d in (UP, DOWN):
        for peer in (at.block(d, 0), at.block(0, d)):
            pl.semaphore_signal(ready, inc=1, device_id=at.on_yz(peer), device_id_type=MESH)
    yv[:] = jnp.zeros_like(yv)
    late = finish_first()
    ys, yq = ysem

    def pair1(h, dg):
        return gsem[0].at[h, dg], gsem[1].at[h, dg]

    def pair2(h, s, dg):
        return pair1(h, RING + RING * s + dg)

    def pair3(h, k):
        return pair1(h, 3 * RING + k)

    def pair4(h, s, k):
        return pair1(h, 3 * RING + 2 + 2 * s + k)

    order = ("z", "y")
    hr = zb.shape[2] // 2
    copies = Copies(any_peer)
    send, arrived = copies.send, copies.arrived

    def zat(h, df, dg):
        dz, dy = (df, dg) if order[h] == "z" else (dg, df)
        return zb.at[dz, dy, pl.ds(h * hr, hr)]

    def compute(dz, dy):
        w = w2v[at.block(dz, dy)].astype(jnp.float32)
        for x in range(xs):
            ws[pl.ds(x * grp, grp), :] = w[x, :grp]
        zb[dz, dy] = jnp.dot(ws[:].astype(jnp.bfloat16), act[:], preferred_element_type=jnp.float32)

    def send1(h, dg):
        d = 1 if dg < 2 else 3
        send(zat(h, 2, dg), r1.at[h, dg], *pair1(h, dg), at.step(order[h], 0, d))

    compute(2, 2)
    pl.semaphore_wait(ready, RING)
    send1(0, 2)
    send1(1, 2)
    for k in (0, 1, 3):
        compute(2, k)
        send1(0, k)
        compute(k, 2)
        send1(1, k)

    def second(i, c):
        k, m = i // 3, i % 3
        compute(k + k // 2, m + m // 2)
        return c

    lax.fori_loop(0, 9, second, 0)

    def send2(h, up, dg):
        df, d, s = (1, 1, 0) if up else (3, 3, 1)
        send(zat(h, df, dg), r2.at[h, s, dg], *pair2(h, s, dg), at.step(order[h], 0, d))

    for h in range(2):
        for dg in (2, 3):
            send2(h, True, dg)
        for dg in (0, 1):
            send2(h, False, dg)
    for k in range(2):
        for h in range(2):
            for up in (True, False):
                dg = 1 - k if up else 2 + k
                arrived(r1.at[h, dg], *pair1(h, dg))
                ref = zat(h, 1 if up else 3, dg)
                ref[:] = ref[:] + r1[h, dg]
                send2(h, up, dg)

    def plane(h, dg):
        for s in range(2):
            arrived(r2.at[h, s, dg], *pair2(h, s, dg))
        ref = zat(h, 0, dg)
        ref[:] = ref[:] + r2[h, 0, dg] + r2[h, 1, dg]

    big = r3.shape[2]
    sizes = (big, hr - big)

    def part(h, dg, k):
        dz, dy = (0, dg) if order[h] == "z" else (dg, 0)
        return zb.at[dz, dy, pl.ds(h * hr + k * big, sizes[k])]

    def r3_at(h, k):
        return r3.at[h, k, pl.ds(0, sizes[k])]

    def r4_at(h, s, k):
        return r4.at[h, s, k, pl.ds(0, sizes[k])]

    def send4(h, up, k):
        dg, d, s = (1, 1, 0) if up else (3, 3, 1)
        send(part(h, dg, k), r4_at(h, s, k), *pair4(h, s, k), at.step(order[h], 1, d))

    for h in range(2):
        plane(h, 2)
        send(part(h, 2, 0), r3_at(h, 0), *pair3(h, 0), at.step(order[h], 1, 1))
        send(part(h, 2, 1), r3_at(h, 1), *pair3(h, 1), at.step(order[h], 1, 3))
    for h in range(2):
        plane(h, 1)
        send4(h, True, 1)
        plane(h, 3)
        send4(h, False, 0)
    for h in range(2):
        plane(h, 0)
    for h in range(2):
        arrived(r3_at(h, 0), *pair3(h, 0))
        ref = part(h, 1, 0)
        ref[:] = ref[:] + r3_at(h, 0)[:]
        send4(h, True, 0)
        arrived(r3_at(h, 1), *pair3(h, 1))
        ref = part(h, 3, 1)
        ref[:] = ref[:] + r3_at(h, 1)[:]
        send4(h, False, 1)
    def y_cols(x):
        rows = yv.shape[2]
        return y_ref.at[:, pl.ds(pl.multiple_of(x * rows, 128), rows)]

    def y_copy(x):
        return pltpu.make_async_remote_copy(
            src_ref=yv.at[x], dst_ref=y_cols(at.x), send_sem=ys.at[0], recv_sem=yq.at[0], device_id=at.on_x(x), device_id_type=MESH
        )

    for h in range(2):
        for k in range(2):
            for s in range(2):
                arrived(r4_at(h, s, k), *pair4(h, s, k))
            ref = part(h, 0, k)
            ref[:] = ref[:] + r4_at(h, 0, k)[:] + r4_at(h, 1, k)[:]
            done = xs // 4
            for x in range((2 * h + k) * done, (2 * h + k + 1) * done):
                z = zb[0, 0, pl.ds(x * grp, grp), :]
                yv[x, :grp, :] = (xo[x, :grp, :].astype(jnp.float32) + z).astype(jnp.bfloat16)
                d = lax.rem(x - at.x + xs, xs)

                @pl.when(d == 0)
                def _():
                    pltpu.make_async_copy(yv.at[x], y_cols(x), loc_sem.at[3]).start()

                @pl.when(d != 0)
                def _():
                    y_copy(x).start()

    arrived(y_ref.at[:, pl.ds(0, (xs - 1) * yv.shape[2])], ys.at[0], yq.at[0])
    pltpu.make_async_copy(yv.at[at.x], y_cols(at.x), loc_sem.at[3]).wait()
    copies.sent(yv.at[pl.ds(0, xs - 1)], ys.at[0], yq.at[0])
    copies.finish()
    finish_last(late)


def layer(x_t, gain, weights, freq, k_cache, v_cache, ctx_len, xs, yzs, gp):
    n_rows = x_t.shape[1]
    rows = n_rows // xs
    dev_rows = k_cache.shape[0]
    c_a, c_f = weights[3].shape[0], weights[4].shape[0]
    n2 = c_a + c_f
    dma, vmem = pltpu.SemaphoreType.DMA, pltpu.VMEM
    bf16 = jnp.bfloat16
    aspec = pl.BlockSpec(memory_space=pl.ANY)
    sems = lambda *shape: [dma(shape), dma(shape)]
    cache = jax.ShapeDtypeStruct(k_cache.shape, bf16)
    return pl.pallas_call(
        functools.partial(layer_kernel, xs, yzs, gp),
        out_shape=(jax.ShapeDtypeStruct((gp, n_rows), bf16), cache, cache),
        in_specs=[aspec] * 11,
        out_specs=(aspec, aspec, aspec),
        scratch_shapes=[
            vmem((n2, rows), bf16),
            vmem((yzs, xs, gp, n2), bf16),
            vmem((xs, gp, rows), bf16),
            vmem(k_cache.shape, bf16),
            vmem(k_cache.shape, bf16),
            vmem((2, yzs, dev_rows // 2, c_a), bf16),
            vmem((rows, c_a), bf16),
            dma((8,)),
        ]
        + sems(1) + sems(2, RING * RING + 2) + sems(11) + sems(11) + sems(2) + sems(2) + sems(1)
        + [pltpu.SemaphoreType.REGULAR],
        compiler_params=pltpu.CompilerParams(collective_id=0, has_side_effects=True, vmem_limit_bytes=VMEM_LIMIT),
        name="layer",
    )(ctx_len, x_t, gain, *weights, freq, k_cache, v_cache)


def results_kernel(chunks, y_ref, k_ref, v_ref, yo_ref, ko_ref, vo_ref, y_in, y_out, k_s, v_s, y_sem, in_sem, out_sem):
    n = k_s.shape[0] // chunks
    y_read = pltpu.make_async_copy(y_ref, y_in, y_sem.at[0])
    y_read.start()
    copies = []
    for c in range(chunks):
        for i, (src, buf, dst) in enumerate(((k_ref, k_s, ko_ref), (v_ref, v_s, vo_ref))):
            take = pl.ds(c * n, n)
            read = pltpu.make_async_copy(src.at[take], buf.at[take], in_sem.at[i, c])
            read.start()
            copies.append((read, pltpu.make_async_copy(buf.at[take], dst.at[take], out_sem.at[i, c])))
    y_read.wait()
    y_out[:] = y_in[:y_out.shape[0], :]
    y_write = pltpu.make_async_copy(y_out, yo_ref, y_sem.at[1])
    y_write.start()
    for read, write in copies:
        read.wait()
        write.start()
    y_write.wait()
    for _, write in copies:
        write.wait()


def results(y_t, k_all, v_all, grp):
    chunks = 4
    dma, vmem = pltpu.SemaphoreType.DMA, pltpu.VMEM
    aspec = pl.BlockSpec(memory_space=pl.ANY)
    shapes = ((grp, y_t.shape[1]), k_all.shape, v_all.shape)
    return pl.pallas_call(
        functools.partial(results_kernel, chunks),
        out_shape=tuple(jax.ShapeDtypeStruct(shape, y_t.dtype) for shape in shapes),
        in_specs=[aspec] * 3,
        out_specs=(aspec,) * 3,
        scratch_shapes=[vmem(shape, y_t.dtype) for shape in (y_t.shape,) + shapes] + [dma((2,)), dma((2, chunks)), dma((2, chunks))],
        compiler_params=pltpu.CompilerParams(vmem_limit_bytes=VMEM_LIMIT),
        name="results",
    )(y_t, k_all, v_all)


def solution(mesh):
    xs = mesh.shape["x"]
    yzs = mesh.shape["yz"]
    both_axes = ("x", "yz")
    row_spec = P("dp", both_axes)
    in_w_spec = P("x", "yz")
    out_w_spec = P("yz", "x")
    cache_spec = P(("dp", "x", "yz"), None, None)
    len_spec = P(("dp", "x", "yz"))

    def local_layer(x_loc, gain_loc, wqkv_loc, wgate_loc, wup_loc, wao_loc, wmo_loc, kc_loc, vc_loc, len_loc):
        grp = x_loc.shape[1]
        gp = grp + -grp % 8
        freq = rope_frequencies(kc_loc.shape[2])
        weights = (wqkv_loc.T, wgate_loc, wup_loc, wao_loc, wmo_loc)
        y_t, k_all, v_all = layer(x_loc.T, gain_loc.reshape(1, grp), weights, freq, kc_loc, vc_loc, len_loc, xs, yzs, gp)
        y_t, k_all, v_all = results(y_t, k_all, v_all, grp)
        return y_t.T, k_all, v_all

    in_specs = (row_spec, P(both_axes), in_w_spec, in_w_spec, in_w_spec, out_w_spec, out_w_spec, cache_spec, cache_spec, len_spec)
    out_specs = (row_spec, cache_spec, cache_spec)
    return jax.shard_map(local_layer, mesh=mesh, in_specs=in_specs, out_specs=out_specs, check_vma=False)
```

```python
import functools

import jax
import jax.numpy as jnp
import numpy as np
from jax import lax
from jax.experimental import pallas as pl
from jax.experimental.pallas import tpu as pltpu
from jax.sharding import PartitionSpec as P

MESH = pl.DeviceIdType.MESH
RING = 4
UP, FAR, DOWN = 1, 2, 3
VMEM_LIMIT = 62 * 1024 * 1024


def rope_frequencies(head_dim):
    half_dim = head_dim // 2
    inv_freq = np.float32(10000.0) ** (-np.arange(half_dim, dtype=np.float32) / np.float32(half_dim))
    return jnp.asarray(np.concatenate([inv_freq, inv_freq])[None, :])


class Where:
    def __init__(self, xs, yzs):
        self.xs = xs
        self.yzs = yzs
        self.dp = lax.axis_index("dp")
        self.x = lax.axis_index("x")
        self.j = lax.axis_index("yz")
        self.zz = self.j // RING
        self.yy = self.j % RING
        self.chip = self.x // 2
        self.core = self.x % 2

    def block(self, dz, dy):
        return ((self.zz + dz) % RING) * RING + (self.yy + dy) % RING

    def on_yz(self, j):
        return (self.dp, j, self.x)

    def on_x(self, x):
        return (self.dp, self.j, x)

    def axis_block(self, first, df, dg):
        return self.block(df, dg) if first == "z" else self.block(dg, df)

    def step(self, first, axis, d):
        return self.on_yz(self.axis_block(first, d, 0) if axis == 0 else self.axis_block(first, 0, d))

    def x_of(self, dc):
        return ((self.chip + dc) % RING) * 2 + self.core

    def x_other(self, dc):
        return ((self.chip + dc) % RING) * 2 + (1 - self.core)

    def peers(self):
        on_x = [self.on_x((self.x + d) % self.xs) for d in range(1, self.xs)]
        return on_x + [self.on_yz((self.j + d) % self.yzs) for d in range(1, self.yzs)]

    def greet(self):
        for peer in self.peers():
            pl.semaphore_signal(pltpu.get_barrier_semaphore(), inc=1, device_id=peer, device_id_type=MESH)

    def greeted(self):
        pl.semaphore_wait(pltpu.get_barrier_semaphore(), len(self.peers()))


class Copies:
    def __init__(self, any_peer):
        self.any_peer = any_peer
        self.started = []

    def send(self, src, dst, ssem, rsem, peer):
        copy = pltpu.make_async_remote_copy(src_ref=src, dst_ref=dst, send_sem=ssem, recv_sem=rsem, device_id=peer, device_id_type=MESH)
        copy.start()
        self.started.append(copy)

    def arrived(self, dst, ssem, rsem):
        pltpu.make_async_remote_copy(
            src_ref=dst, dst_ref=dst, send_sem=ssem, recv_sem=rsem, device_id=self.any_peer, device_id_type=MESH
        ).wait_recv()

    def sent(self, src, ssem, rsem):
        remote(src, src, ssem, rsem, self.any_peer).wait_send()

    def finish(self):
        for copy in self.started:
            copy.wait_send()


def layer_kernel(
    xs, yzs, gp, len_ref, x_ref, gain_ref, wq_ref, wg_ref, wu_ref, wa_ref, wm_ref, freq_ref, kc_ref, vc_ref,
    y_ref, ko_ref, vo_ref,
    act, w2v, xo, k_s, v_s, o_send, ob,
    loc_sem, xsend, xrecv, gsend, grecv, wsend, wrecv, vsend, vrecv, qsend, qrecv, osend, orecv,
    ys, yq, ready,
):
    f32, bf16 = jnp.float32, jnp.bfloat16
    dma, vmem = pltpu.SemaphoreType.DMA, pltpu.VMEM
    grp = x_ref.shape[0]
    rows, c_a = ob.shape
    dev_rows, t_len, head_dim = k_s.shape
    c_q, k_loc = wq_ref.shape
    n1 = c_q + 2 * wg_ref.shape[1]
    c_f = wm_ref.shape[0]
    num_heads = yzs * c_a // head_dim
    part = dev_rows // 2
    block = xs * grp
    hr = block // 2
    at = Where(xs, yzs)
    any_peer = at.on_yz(at.block(0, UP))

    def w2_at(x, k=None):
        return w2v.at[x, pl.ds(0, k_loc)] if k is None else w2v.at[x, pl.ds(k * (k_loc // 2), k_loc // 2)]

    def o_rows(j, k):
        return ob.at[pl.ds(pl.multiple_of(j * dev_rows + k * part, part), part)]

    def o_copy(k, d):
        to = (at.j + d) % yzs
        return remote(o_send.at[k, to], o_rows(at.j, k), osend.at[k], orecv.at[k], at.on_yz(to))

    def o_own(k):
        return pltpu.make_async_copy(o_send.at[k, at.j], o_rows(at.j, k), loc_sem.at[6 + k])

    def cache_writes():
        return [pltpu.make_async_copy(src, dst, loc_sem.at[loc]) for src, dst, loc in ((k_s, ko_ref, 4), (v_s, vo_ref, 5))]

    gather_and_attend = functools.partial(
        first_phase, xs, yzs, num_heads, at, any_peer, w2_at, o_copy, o_own, cache_writes,
        len_ref, x_ref, gain_ref, wq_ref, wg_ref, wu_ref, wa_ref, wm_ref, freq_ref, kc_ref, vc_ref,
        act, w2v, xo, k_s, v_s, o_send,
        loc_sem, (xsend, xrecv), (gsend, grecv), (wsend, wrecv), (vsend, vrecv), (qsend, qrecv),
    )
    pl.run_scoped(
        gather_and_attend,
        vmem((xs, yzs, gp, rows), bf16),
        vmem((xs * yzs * gp, rows), bf16),
        vmem((xs, yzs, gp, 128), f32),
        vmem((n1, xs * yzs * gp), bf16),
        vmem((2, yzs, part + part // 2, 128), bf16),
        vmem((2, yzs, part + part // 2, 128), bf16),
        vmem((num_heads + 2, dev_rows, head_dim), f32),
        vmem((xs, gp, rows), bf16),
        vmem((gp, rows), f32),
        vmem((k_loc + 8, c_f + c_a), f32),
        vmem((yzs * gp, c_f), f32),
        vmem((c_f + c_a, k_loc), f32),
        vmem((dev_rows, head_dim), f32),
        vmem((dev_rows, head_dim), f32),
        *[vmem(ref.shape, ref.dtype) for ref in (x_ref, gain_ref, wq_ref, wg_ref, wu_ref, wa_ref, wm_ref, freq_ref)],
        pltpu.SMEM(len_ref.shape, len_ref.dtype),
        dma((9,)),
    )

    def finish_first():
        late = Copies(any_peer)
        share_far(late, at, w2_at, (vsend, vrecv))
        for k in range(2):
            late.arrived(ob.at[pl.ds(0, (yzs - 1) * part)], osend.at[k], orecv.at[k])
            o_own(k).wait()
        act[pl.ds(c_f, c_a), :] = ob[:].T
        all_in(late, at, w2_at, (vsend, vrecv))
        return late

    def finish_last(late):
        for write in cache_writes():
            write.wait()
        for k in range(2):
            late.sent(o_send.at[k, pl.ds(0, yzs - 1)], osend.at[k], orecv.at[k])
        for slot in range(9):
            r = w2_at(at.x, None if slot in (4, 7, 8) else 0)
            remote(r, r, vsend.at[slot], vrecv.at[slot], any_peer).wait_send()
        late.finish()

    sum_and_return = functools.partial(
        second_phase, xs, yzs, grp, at, any_peer, finish_first, finish_last, w2v, act, xo, y_ref,
        loc_sem, (gsend, grecv), (ys, yq), ready,
    )
    big = hr // 2 + hr // 2 % 8
    pl.run_scoped(
        sum_and_return,
        vmem((RING, RING, block, rows), f32),
        vmem((2, RING, hr, rows), f32),
        vmem((2, 2, RING, hr, rows), f32),
        vmem((2, 2, big, rows), f32),
        vmem((2, 2, 2, big, rows), f32),
        vmem((xs, gp, rows), bf16),
        vmem((block, w2v.shape[2]), f32),
    )


def remote(src, dst, ssem, rsem, peer):
    return pltpu.make_async_remote_copy(src_ref=src, dst_ref=dst, send_sem=ssem, recv_sem=rsem, device_id=peer, device_id_type=MESH)


def spread_own(copies, at, region, sems):
    def send(slot, k, x):
        r = region(at.x, k)
        copies.send(r, r, sems[0].at[slot], sems[1].at[slot], at.on_x(x))

    for k in range(2):
        send(2 * k, k, at.x_of(UP))
        send(2 * k + 1, 1 - k, at.x_of(DOWN))
    send(4, None, at.x_other(0))


def pass_on(copies, at, r, sems, slot, x):
    copies.send(r, r, sems[0].at[slot], sems[1].at[slot], at.on_x(x))


def block_in(copies, r, sems, slot):
    copies.arrived(r, sems[0].at[slot], sems[1].at[slot])


def forward_half(copies, at, region, sems):
    for slot, k, here, to in ((0, 0, DOWN, UP), (1, 1, UP, DOWN)):
        r = region(at.x_of(here), k)
        block_in(copies, r, sems, slot)
        pass_on(copies, at, r, sems, slot + 5, at.x_of(to))


def share_near(copies, at, region, sems):
    for slot, k, here in ((2, 1, DOWN), (3, 0, UP)):
        block_in(copies, region(at.x_of(here), k), sems, slot)
        pass_on(copies, at, region(at.x_of(here)), sems, slot + 5, at.x_other(0))


def share_far(copies, at, region, sems):
    for k in range(2):
        r = region(at.x_of(FAR), k)
        block_in(copies, r, sems, 5 + k)
        pass_on(copies, at, r, sems, 9 + k, at.x_other(0))


def all_in(copies, at, region, sems):
    for slot, here in ((4, 0), (7, DOWN), (8, UP)):
        block_in(copies, region(at.x_other(here)), sems, slot)
    for k in range(2):
        block_in(copies, region(at.x_other(FAR), k), sems, 9 + k)


def first_phase(
    xs, yzs, num_heads, at, any_peer, w2_at, o_copy, o_own, cache_writes,
    len_hbm, x_hbm, gain_hbm, wq_hbm, wg_hbm, wu_hbm, wa_hbm, wm_hbm, freq_hbm, kc_ref, vc_ref,
    act, w2v, xo, k_s, v_s, o_send,
    loc_sem, xsem, gsem, wsem, vsem, qsem, xg, h, gcol, w1, qkv_s, qkv_in, heads, x_send, stage, tall, wide_s, narrow, cos_s, sin_s,
    x_ref, gain_ref, wq_ref, wg_ref, wu_ref, wa_ref, wm_ref, freq_ref, len_ref, in_sem,
):
    f32, bf16 = jnp.float32, jnp.bfloat16
    half = xs // 2
    quarter = half // 2
    grp = x_ref.shape[0]
    _, gp, rows = x_send.shape
    dev_rows = rows // yzs
    c_q, k_loc = wq_ref.shape
    c_f, c_a = wm_ref.shape[0], wa_ref.shape[0]
    kx = yzs * gp
    at.greet()
    operands = ((x_hbm, x_ref), (gain_hbm, gain_ref), (wq_hbm, wq_ref), (wg_hbm, wg_ref), (wu_hbm, wu_ref), (wa_hbm, wa_ref), (wm_hbm, wm_ref), (freq_hbm, freq_ref), (len_hbm, len_ref))
    reads = [pltpu.make_async_copy(src, dst, in_sem.at[i]) for i, (src, dst) in enumerate(operands)]
    for read in reads:
        read.start()
    read_k = pltpu.make_async_copy(kc_ref, k_s, loc_sem.at[4])
    read_k.start()
    read_v = pltpu.make_async_copy(vc_ref, v_s, loc_sem.at[5])
    read_v.start()
    stage[:] = jnp.zeros_like(stage)
    for read in reads[:2]:
        read.wait()
    stage[grp:grp + 1, :grp] = gain_ref[:].astype(f32)
    at.greeted()
    copies, late = Copies(any_peer), Copies(any_peer)

    def send(src, dst, sems, idx, peer):
        copies.send(src, dst, sems[0].at[idx], sems[1].at[idx], peer)

    def arrived(region, sems, idx):
        copies.arrived(region, sems[0].at[idx], sems[1].at[idx])

    for d in (*range(1, xs), 0):
        to = (at.x + d) % xs
        stage[:grp, :] = x_ref[:, pl.ds(pl.multiple_of(to * rows, 128), rows)].astype(f32)
        x_send[to] = stage[:].astype(bf16)
        if d:
            remote(x_send.at[to], xg.at[at.x, at.j], xsem[0].at[0], xsem[1].at[0], at.on_x(to)).start()
    own_x = pltpu.make_async_copy(x_send.at[at.x], xg.at[at.x, at.j], loc_sem.at[0])
    own_x.start()
    for read in reads[2:]:
        read.wait()

    n1 = w1.shape[0]

    def w1_at(x, k=None):
        cols = pl.ds(pl.multiple_of(x * kx, 128), kx)
        return w1.at[:, cols] if k is None else w1.at[pl.ds(k * (n1 // 2), n1 // 2), cols]

    own_cols = pl.ds(pl.multiple_of(at.x * kx, 128), kx)
    tall[k_loc:, :] = jnp.zeros((tall.shape[0] - k_loc, tall.shape[1]), f32)
    row = 0
    for ref in (wq_ref, wg_ref, wu_ref):
        w = ref[:].astype(f32)
        w = w.T if ref is wq_ref else w
        n = w.shape[1]
        tall[:k_loc, :n] = w
        for j in range(yzs):
            wide_s[j * gp:(j + 1) * gp, :n] = tall[j * grp:j * grp + gp, :n]
        w1[row:row + n, own_cols] = wide_s[:, :n].T.astype(bf16)
        row += n
    spread_own(copies, at, w1_at, wsem)
    own_x.wait()
    arrived(xg.at[pl.ds(0, xs - 1), at.j], xsem, 0)
    copies.sent(x_send.at[pl.ds(0, xs - 1)], xsem[0].at[0], xsem[1].at[0])

    order = ("y", "z")
    halves = range(len(order))
    first_axis, second_axis = halves
    slot_up, slot_down, slot_far = RING, 2 * RING, 3 * RING

    def region(s, df, dg, lo=0, n=half):
        return xg.at[pl.ds(s * half + lo, n), at.axis_block(order[s], df, dg)]

    def pass_rows(s, df, dg, axis, d, slot, lo=0, n=half):
        r = region(s, df, dg, lo, n)
        send(r, r, (gsem[0].at[s], gsem[1].at[s]), slot, at.step(order[s], axis, d))

    def rows_in(s, df, dg, slot, lo=0, n=half):
        arrived(region(s, df, dg, lo, n), (gsem[0].at[s], gsem[1].at[s]), slot)

    def both_ways(s, df):
        pass_rows(s, df, 0, second_axis, UP, slot_up + df)
        pass_rows(s, df, 0, second_axis, DOWN, slot_down + df)

    for s in halves:
        pass_rows(s, 0, 0, first_axis, UP, 0)
        pass_rows(s, 0, 0, first_axis, DOWN, 1)
        both_ways(s, 0)
    xo[:] = xg[:, at.j]
    narrow[:c_f, :] = wm_ref[:].astype(f32)
    narrow[c_f:, :] = wa_ref[:].astype(f32)
    tall[:k_loc, :] = narrow[:].T
    w2v[at.x, :k_loc] = tall[:k_loc, :].astype(bf16)
    head_dim = k_s.shape[2]
    request = lax.broadcasted_iota(jnp.int32, (dev_rows, head_dim), 0)
    lane = lax.broadcasted_iota(jnp.int32, (dev_rows, head_dim), 1)

    def place(b, p):
        return jnp.where(request == b, len_ref[b].astype(f32), p)

    angles = lax.fori_loop(0, dev_rows, place, jnp.zeros((dev_rows, head_dim), f32), unroll=8) * freq_ref[:]
    cos_s[:] = jnp.cos(angles)
    sin_s[:] = jnp.where(lane < head_dim // 2, -1.0, 1.0) * jnp.sin(angles)
    for s in halves:
        rows_in(s, DOWN, 0, 0)
        pass_rows(s, DOWN, 0, first_axis, UP, FAR, 0, quarter)
        rows_in(s, UP, 0, 1)
        pass_rows(s, UP, 0, first_axis, DOWN, DOWN, quarter, quarter)
        both_ways(s, DOWN)
        both_ways(s, UP)
    for s in halves:
        rows_in(s, FAR, 0, FAR, 0, quarter)
        rows_in(s, FAR, 0, DOWN, quarter, quarter)
        both_ways(s, FAR)
    forward_half(copies, at, w1_at, wsem)
    spread_own(late, at, w2_at, vsem)

    diagonal = lax.broadcasted_iota(jnp.int32, (gp, 128), 0) == lax.broadcasted_iota(jnp.int32, (gp, 128), 1)
    feature = lax.broadcasted_iota(jnp.int32, (gp, 1), 0)

    def add_up(s, dg, sums):
        def body(i, c):
            x, j = s * half + i // RING, at.axis_block(order[s], i % RING, dg)
            raw = xg[x, j].astype(f32)
            col = jnp.sum(jnp.where(diagonal, raw[grp:grp + 1, :128], 0.0), axis=1, keepdims=True)
            gcol[x, j] = jnp.broadcast_to(col, (gp, 128))
            parts = jnp.where(feature < grp, raw, 0.0).reshape(gp // 8, 8, rows)
            return c[0] + jnp.sum(parts, axis=0), c[1] + jnp.sum(parts * parts, axis=0)

        return lax.fori_loop(0, half * RING, body, sums, unroll=4)

    sums = (jnp.zeros((8, rows), f32), jnp.zeros((8, rows), f32))
    for s in halves:
        sums = add_up(s, 0, sums)
    for s in halves:
        for df in (0, DOWN):
            rows_in(s, df, DOWN, slot_up + df)
            pass_rows(s, df, DOWN, second_axis, UP, slot_far + df)
    share_near(copies, at, w1_at, wsem)
    for s in halves:
        for df in (UP, FAR):
            rows_in(s, df, UP, slot_down + df)
            pass_rows(s, df, UP, second_axis, DOWN, slot_far + df)
    for s in halves:
        for df in (UP, FAR):
            rows_in(s, df, DOWN, slot_up + df)
        for df in (0, DOWN):
            rows_in(s, df, UP, slot_down + df)
    for dg in (DOWN, UP):
        for s in halves:
            sums = add_up(s, dg, sums)
    for s in halves:
        for df in range(RING):
            rows_in(s, df, FAR, slot_far + df)
        sums = add_up(s, FAR, sums)

    pairs = yzs // 2
    real = lax.broadcasted_iota(jnp.int32, (2, gp, 1), 1).reshape(2 * gp, 1) < grp
    s1, s2 = sums
    d_model = grp * xs * yzs
    mean = jnp.sum(s1, axis=0, keepdims=True) / d_model
    var = jnp.sum(s2, axis=0, keepdims=True) / d_model - mean * mean
    scale = lax.rsqrt(var + 1e-6)

    def normalize(q, c):
        at_q = q // pairs, pl.ds((q % pairs) * 2, 2)
        gain = jnp.concatenate([gcol[at_q].reshape(2 * gp, 128)] * (rows // 128), axis=1)
        out = jnp.where(real, (xg[at_q].astype(f32).reshape(2 * gp, rows) - mean) * scale * gain, 0.0)
        h[pl.ds(pl.multiple_of(q * 2 * gp, 16), 2 * gp), :] = out.astype(bf16)
        return c

    some = xs * pairs // 2
    lax.fori_loop(0, some, normalize, 0, unroll=2)
    share_far(copies, at, w1_at, wsem)
    lax.fori_loop(some, xs * pairs, normalize, 0, unroll=2)
    all_in(copies, at, w1_at, wsem)

    nt = 256

    def query(n, c):
        q = jnp.dot(w1[:c_q], h[:, pl.ds(pl.multiple_of(n * nt, nt), nt)], preferred_element_type=f32)
        q = q.T
        for i in range(nt // dev_rows):
            to = n * (nt // dev_rows) + i
            for k in range(2):
                piece = q[i * dev_rows + k * part:i * dev_rows + (k + 1) * part]
                qkv_s[k, to, :part] = piece[:, :128].astype(bf16)
                qkv_s[k, to, part:] = jnp.concatenate([piece[:part // 2, 128:], piece[part // 2:, 128:]], axis=1).astype(bf16)
        return c

    def unpacked(k, j):
        piece = qkv_in[k, j].astype(f32)
        rest = piece[part:]
        rest = jnp.concatenate([rest[:, :c_q - 128], rest[:, c_q - 128:]], axis=0)
        return jnp.concatenate([piece[:part], rest], axis=1)

    part = dev_rows // 2
    lax.fori_loop(0, rows // nt, query, 0)
    own_q = []
    for k in range(2):
        own = pltpu.make_async_copy(qkv_s.at[k, at.j], qkv_in.at[k, at.j], loc_sem.at[2 + k])
        own.start()
        own_q.append(own)
        for d in range(1, yzs):
            to = (at.j + d) % yzs
            remote(qkv_s.at[k, to], qkv_in.at[k, at.j], qsem[0].at[k], qsem[1].at[k], at.on_yz(to)).start()

    def mlp(n, c):
        cols = pl.ds(pl.multiple_of(n * nt, nt), nt)
        gate = jnp.dot(w1[c_q:c_q + c_f], h[:, cols], preferred_element_type=f32).astype(bf16).astype(f32)
        up = jnp.dot(w1[c_q + c_f:], h[:, cols], preferred_element_type=f32).astype(bf16).astype(f32)
        act[pl.ds(0, c_f), cols] = (jax.nn.silu(gate) * up).astype(bf16)
        return c

    steps = rows // nt
    lax.fori_loop(0, steps // 2, mlp, 0)
    forward_half(late, at, w2_at, vsem)

    per = 2 * c_q // head_dim

    def rotate(k):
        take = pl.ds(k * part, part)
        for p in range(yzs // 2):
            both = jnp.concatenate([unpacked(k, 2 * p), unpacked(k, 2 * p + 1)], axis=1)
            for i in range(per):
                hd = p * per + i
                u = both[:, i * head_dim:(i + 1) * head_dim]
                if hd <= num_heads:
                    u = u * cos_s[take, :] + pltpu.roll(u, head_dim // 2, 1) * sin_s[take, :]
                    u = u.astype(bf16).astype(f32)
                heads[hd, take, :] = u

    group = 8
    t_len = k_s.shape[1]
    hp = heads.shape[0]
    position = lax.broadcasted_iota(jnp.int32, (t_len, head_dim), 0)
    along = lax.broadcasted_iota(jnp.int32, (hp, t_len), 1)

    def attend(g, c):
        first = pl.multiple_of(g * group, group)
        block = jnp.swapaxes(heads[:, pl.ds(first, group), :], 0, 1)
        scores, keys, values = [], [], []
        for i in range(group):
            b = first + i
            last = len_ref[b]
            mine = block[i]
            slot = position == last
            kb, vb = [
                jnp.where(slot, mine[row:row + 1], old[b].astype(f32)).astype(bf16)
                for row, old in ((num_heads, k_s), (num_heads + 1, v_s))
            ]
            keys.append(kb)
            values.append(vb)
            score = lax.dot_general(mine.astype(bf16), kb, (((1,), (1,)), ((), ())), preferred_element_type=f32) * head_dim ** -0.5
            scores.append(jnp.where(along <= last, score, -1e30))
        for i in range(group):
            k_s[first + i] = keys[i]
            v_s[first + i] = values[i]
        scores = jnp.concatenate(scores, axis=0)
        e = jnp.exp(scores - jnp.max(scores, axis=1, keepdims=True))
        probs = (e / jnp.sum(e, axis=1, keepdims=True)).reshape(group, hp, t_len).astype(bf16)
        outs = [jnp.dot(probs[i], values[i], preferred_element_type=f32) for i in range(group)]
        heads[:, pl.ds(first, group), :] = jnp.swapaxes(jnp.stack(outs, axis=0), 0, 1)
        return c

    read_k.wait()
    read_v.wait()
    for k in range(2):
        arrived(qkv_in.at[k, pl.ds(0, yzs - 1)], qsem, k)
        copies.sent(qkv_s.at[k, pl.ds(0, yzs - 1)], qsem[0].at[k], qsem[1].at[k])
        own_q[k].wait()
        rotate(k)
        lax.fori_loop(k * part // group, (k + 1) * part // group, attend, 0)
        take = pl.ds(k * part, part)
        for jj in range(yzs):
            lo, hi = jj * c_a // head_dim, ((jj + 1) * c_a - 1) // head_dim + 1
            wide = jnp.concatenate([heads[hd, take, :] for hd in range(lo, hi)], axis=1)
            start = jj * c_a - lo * head_dim
            o_send[k, jj] = wide[:, start:start + c_a].astype(bf16)
        o_own(k).start()
        for d in range(1, yzs):
            o_copy(k, d).start()
    for write in cache_writes():
        write.start()
    share_near(late, at, w2_at, vsem)
    lax.fori_loop(steps // 2, steps, mlp, 0)
    copies.finish()


def second_phase(
    xs, yzs, grp, at, any_peer, finish_first, finish_last, w2v, act, xo, y_ref,
    loc_sem, gsem, ysem, ready, zb, r1, r2, r3, r4, yv, ws,
):
    for d in (UP, DOWN):
        for peer in (at.block(d, 0), at.block(0, d)):
            pl.semaphore_signal(ready, inc=1, device_id=at.on_yz(peer), device_id_type=MESH)
    yv[:] = jnp.zeros_like(yv)
    late = finish_first()
    ys, yq = ysem

    def pair1(h, dg):
        return gsem[0].at[h, dg], gsem[1].at[h, dg]

    def pair2(h, s, dg):
        return pair1(h, RING + RING * s + dg)

    def pair3(h, k):
        return pair1(h, 3 * RING + k)

    def pair4(h, s, k):
        return pair1(h, 3 * RING + 2 + 2 * s + k)

    order = ("z", "y")
    hr = zb.shape[2] // 2
    copies = Copies(any_peer)
    send, arrived = copies.send, copies.arrived

    def zat(h, df, dg):
        dz, dy = (df, dg) if order[h] == "z" else (dg, df)
        return zb.at[dz, dy, pl.ds(h * hr, hr)]

    def compute(dz, dy):
        start = at.block(dz, dy) * grp
        base = start // 16 * 16
        span = 48
        for x in range(xs):
            w = w2v[x, pl.ds(pl.multiple_of(base, 16), span), :].astype(jnp.float32)
            ws[pl.ds(x * grp, grp), :] = pltpu.roll(w, span - (start - base), 0)[:grp]
        zb[dz, dy] = jnp.dot(ws[:].astype(jnp.bfloat16), act[:], preferred_element_type=jnp.float32)

    def send1(h, dg):
        d = 1 if dg < 2 else 3
        send(zat(h, 2, dg), r1.at[h, dg], *pair1(h, dg), at.step(order[h], 0, d))

    compute(2, 2)
    pl.semaphore_wait(ready, RING)
    send1(0, 2)
    send1(1, 2)
    for k in (0, 1, 3):
        compute(2, k)
        send1(0, k)
        compute(k, 2)
        send1(1, k)

    def second(i, c):
        k, m = i // 3, i % 3
        compute(k + k // 2, m + m // 2)
        return c

    lax.fori_loop(0, 9, second, 0)

    def send2(h, up, dg):
        df, d, s = (1, 1, 0) if up else (3, 3, 1)
        send(zat(h, df, dg), r2.at[h, s, dg], *pair2(h, s, dg), at.step(order[h], 0, d))

    for h in range(2):
        for dg in (2, 3):
            send2(h, True, dg)
        for dg in (0, 1):
            send2(h, False, dg)
    for k in range(2):
        for h in range(2):
            for up in (True, False):
                dg = 1 - k if up else 2 + k
                arrived(r1.at[h, dg], *pair1(h, dg))
                ref = zat(h, 1 if up else 3, dg)
                ref[:] = ref[:] + r1[h, dg]
                send2(h, up, dg)

    def plane(h, dg):
        for s in range(2):
            arrived(r2.at[h, s, dg], *pair2(h, s, dg))
        ref = zat(h, 0, dg)
        ref[:] = ref[:] + r2[h, 0, dg] + r2[h, 1, dg]

    big = r3.shape[2]
    sizes = (big, hr - big)

    def part(h, dg, k):
        dz, dy = (0, dg) if order[h] == "z" else (dg, 0)
        return zb.at[dz, dy, pl.ds(h * hr + k * big, sizes[k])]

    def r3_at(h, k):
        return r3.at[h, k, pl.ds(0, sizes[k])]

    def r4_at(h, s, k):
        return r4.at[h, s, k, pl.ds(0, sizes[k])]

    def send4(h, up, k):
        dg, d, s = (1, 1, 0) if up else (3, 3, 1)
        send(part(h, dg, k), r4_at(h, s, k), *pair4(h, s, k), at.step(order[h], 1, d))

    for h in range(2):
        plane(h, 2)
        send(part(h, 2, 0), r3_at(h, 0), *pair3(h, 0), at.step(order[h], 1, 1))
        send(part(h, 2, 1), r3_at(h, 1), *pair3(h, 1), at.step(order[h], 1, 3))
    for h in range(2):
        plane(h, 1)
        send4(h, True, 1)
        plane(h, 3)
        send4(h, False, 0)
    for h in range(2):
        plane(h, 0)
    for h in range(2):
        arrived(r3_at(h, 0), *pair3(h, 0))
        ref = part(h, 1, 0)
        ref[:] = ref[:] + r3_at(h, 0)[:]
        send4(h, True, 0)
        arrived(r3_at(h, 1), *pair3(h, 1))
        ref = part(h, 3, 1)
        ref[:] = ref[:] + r3_at(h, 1)[:]
        send4(h, False, 1)
    def y_cols(x):
        rows = yv.shape[2]
        return y_ref.at[:, pl.ds(pl.multiple_of(x * rows, 128), rows)]

    def y_copy(x):
        return pltpu.make_async_remote_copy(
            src_ref=yv.at[x], dst_ref=y_cols(at.x), send_sem=ys.at[0], recv_sem=yq.at[0], device_id=at.on_x(x), device_id_type=MESH
        )

    for h in range(2):
        for k in range(2):
            for s in range(2):
                arrived(r4_at(h, s, k), *pair4(h, s, k))
            ref = part(h, 0, k)
            ref[:] = ref[:] + r4_at(h, 0, k)[:] + r4_at(h, 1, k)[:]
            done = xs // 4
            for x in range((2 * h + k) * done, (2 * h + k + 1) * done):
                z = zb[0, 0, pl.ds(x * grp, grp), :]
                yv[x, :grp, :] = (xo[x, :grp, :].astype(jnp.float32) + z).astype(jnp.bfloat16)
                d = lax.rem(x - at.x + xs, xs)

                @pl.when(d == 0)
                def _():
                    pltpu.make_async_copy(yv.at[x], y_cols(x), loc_sem.at[3]).start()

                @pl.when(d != 0)
                def _():
                    y_copy(x).start()

    arrived(y_ref.at[:, pl.ds(0, (xs - 1) * yv.shape[2])], ys.at[0], yq.at[0])
    pltpu.make_async_copy(yv.at[at.x], y_cols(at.x), loc_sem.at[3]).wait()
    copies.sent(yv.at[pl.ds(0, xs - 1)], ys.at[0], yq.at[0])
    copies.finish()
    finish_last(late)


def layer(x_t, gain, weights, freq, k_cache, v_cache, ctx_len, xs, yzs, gp):
    n_rows = x_t.shape[1]
    rows = n_rows // xs
    dev_rows = k_cache.shape[0]
    c_a, c_f = weights[3].shape[0], weights[4].shape[0]
    n2 = c_a + c_f
    grp = x_t.shape[0]
    dma, vmem = pltpu.SemaphoreType.DMA, pltpu.VMEM
    bf16 = jnp.bfloat16
    aspec = pl.BlockSpec(memory_space=pl.ANY)
    sems = lambda *shape: [dma(shape), dma(shape)]
    cache = jax.ShapeDtypeStruct(k_cache.shape, bf16)
    return pl.pallas_call(
        functools.partial(layer_kernel, xs, yzs, gp),
        out_shape=(jax.ShapeDtypeStruct((gp, n_rows), bf16), cache, cache),
        in_specs=[aspec] * 11,
        out_specs=(aspec, aspec, aspec),
        scratch_shapes=[
            vmem((n2, rows), bf16),
            vmem((xs, yzs * grp + 16, n2), bf16),
            vmem((xs, gp, rows), bf16),
            vmem(k_cache.shape, bf16),
            vmem(k_cache.shape, bf16),
            vmem((2, yzs, dev_rows // 2, c_a), bf16),
            vmem((rows, c_a), bf16),
            dma((8,)),
        ]
        + sems(1) + sems(2, RING * RING + 2) + sems(11) + sems(11) + sems(2) + sems(2) + sems(1)
        + [pltpu.SemaphoreType.REGULAR],
        compiler_params=pltpu.CompilerParams(collective_id=0, has_side_effects=True, vmem_limit_bytes=VMEM_LIMIT),
        name="layer",
    )(ctx_len, x_t, gain, *weights, freq, k_cache, v_cache)


def results_kernel(chunks, y_ref, k_ref, v_ref, yo_ref, ko_ref, vo_ref, y_in, y_out, k_s, v_s, y_sem, in_sem, out_sem):
    n = k_s.shape[0] // chunks
    y_read = pltpu.make_async_copy(y_ref, y_in, y_sem.at[0])
    y_read.start()
    copies = []
    for c in range(chunks):
        for i, (src, buf, dst) in enumerate(((k_ref, k_s, ko_ref), (v_ref, v_s, vo_ref))):
            take = pl.ds(c * n, n)
            read = pltpu.make_async_copy(src.at[take], buf.at[take], in_sem.at[i, c])
            read.start()
            copies.append((read, pltpu.make_async_copy(buf.at[take], dst.at[take], out_sem.at[i, c])))
    y_read.wait()
    y_out[:] = y_in[:y_out.shape[0], :]
    y_write = pltpu.make_async_copy(y_out, yo_ref, y_sem.at[1])
    y_write.start()
    for read, write in copies:
        read.wait()
        write.start()
    y_write.wait()
    for _, write in copies:
        write.wait()


def results(y_t, k_all, v_all, grp):
    chunks = 4
    dma, vmem = pltpu.SemaphoreType.DMA, pltpu.VMEM
    aspec = pl.BlockSpec(memory_space=pl.ANY)
    shapes = ((grp, y_t.shape[1]), k_all.shape, v_all.shape)
    return pl.pallas_call(
        functools.partial(results_kernel, chunks),
        out_shape=tuple(jax.ShapeDtypeStruct(shape, y_t.dtype) for shape in shapes),
        in_specs=[aspec] * 3,
        out_specs=(aspec,) * 3,
        scratch_shapes=[vmem(shape, y_t.dtype) for shape in (y_t.shape,) + shapes] + [dma((2,)), dma((2, chunks)), dma((2, chunks))],
        compiler_params=pltpu.CompilerParams(vmem_limit_bytes=VMEM_LIMIT),
        name="results",
    )(y_t, k_all, v_all)


def solution(mesh):
    xs = mesh.shape["x"]
    yzs = mesh.shape["yz"]
    both_axes = ("x", "yz")
    row_spec = P("dp", both_axes)
    in_w_spec = P("x", "yz")
    out_w_spec = P("yz", "x")
    cache_spec = P(("dp", "x", "yz"), None, None)
    len_spec = P(("dp", "x", "yz"))

    def local_layer(x_loc, gain_loc, wqkv_loc, wgate_loc, wup_loc, wao_loc, wmo_loc, kc_loc, vc_loc, len_loc):
        grp = x_loc.shape[1]
        gp = grp + -grp % 8
        freq = rope_frequencies(kc_loc.shape[2])
        weights = (wqkv_loc.T, wgate_loc, wup_loc, wao_loc, wmo_loc)
        y_t, k_all, v_all = layer(x_loc.T, gain_loc.reshape(1, grp), weights, freq, kc_loc, vc_loc, len_loc, xs, yzs, gp)
        y_t, k_all, v_all = results(y_t, k_all, v_all, grp)
        return y_t.T, k_all, v_all

    in_specs = (row_spec, P(both_axes), in_w_spec, in_w_spec, in_w_spec, out_w_spec, out_w_spec, cache_spec, cache_spec, len_spec)
    out_specs = (row_spec, cache_spec, cache_spec)
    return jax.shard_map(local_layer, mesh=mesh, in_specs=in_specs, out_specs=out_specs, check_vma=False)
```
